16 devices in a mesh: pp: 4 (over z, y), ep: 4 (over x, core).
Axes of the slice: x: 2, y: 2, z: 2, core: 2. Of those that a mesh axis runs over, the one named last changes fastest.
Arguments:
- x_fwd: bfloat16 [4, 16384, 256], P('pp', 'ep')
- ids_fwd: int32 [4, 16384, 4], P('pp', 'ep')
- slots_fwd: int32 [4, 16384, 4], P('pp', 'ep')
- gates_fwd: bfloat16 [4, 16384, 4], P('pp', 'ep')
- x_saved: bfloat16 [4, 16384, 256], P('pp', 'ep')
- grad_in: bfloat16 [4, 16384, 256], P('pp', 'ep')
- ids_bwd: int32 [4, 16384, 4], P('pp', 'ep')
- slots_bwd: int32 [4, 16384, 4], P('pp', 'ep')
- gates_bwd: bfloat16 [4, 16384, 4], P('pp', 'ep')
- w_one: bfloat16 [4, 256, 256], P('pp')
- w_two: bfloat16 [4, 256, 256], P('pp')
- w_gate: bfloat16 [4, 32, 256, 256], P('pp', 'ep')
- w_up: bfloat16 [4, 32, 256, 256], P('pp', 'ep')
- w_down: bfloat16 [4, 32, 256, 256], P('pp', 'ep')
Outputs:
- output 1: bfloat16 [4, 16384, 256], P('pp', 'ep')
- output 2: bfloat16 [4, 16384, 256], P('pp', 'ep')
- output 3: float32 [4, 32, 256, 256], P('pp', 'ep')
- output 4: float32 [4, 32, 256, 256], P('pp', 'ep')
- output 5: float32 [4, 32, 256, 256], P('pp', 'ep')
All inputs are finite; a program needn't handle non-finite values.
Results may differ from the reference program's by a relative error of at most 0.0104285.
Values are sent between devices in bfloat16 or wider.
A program may use at most 1 GiB of HBM per device.

```python
import jax
import jax.numpy as jnp
from jax import lax

STAGES = 4
EP_SIZE = 4
TOKENS_DEV = 4096
HIDDEN = 256
FF_DENSE = 256
FF_EXPERT = 256
EXPERTS = 32
TOP = 4

NORM_EPS = 1e-6
CAP_ROWS = 8 * ((2 * TOKENS_DEV * TOP + 8 * EXPERTS - 1) // (8 * EXPERTS))
TOKENS = EP_SIZE * TOKENS_DEV
BUF_ROWS = EXPERTS * EP_SIZE * CAP_ROWS


def route_ranks(row_ids):
    sort_order = jnp.argsort(row_ids, stable=True)
    sorted_ids = row_ids[sort_order]
    group_start = jnp.searchsorted(sorted_ids, sorted_ids, side="left")
    rank_sorted = (jnp.arange(row_ids.shape[0]) - group_start).astype(jnp.int32)
    return jnp.zeros(row_ids.shape, jnp.int32).at[sort_order].set(rank_sorted)


def draw_routes(route_key):
    key_base, key_mult, key_hot, key_step = jax.random.split(route_key, 4)
    block_shape = (STAGES, EP_SIZE, TOKENS_DEV)
    base_ids = jax.random.randint(key_base, block_shape, 0, EXPERTS, dtype=jnp.int32)
    base_ids = base_ids * jax.random.randint(key_mult, block_shape, 1, 4, dtype=jnp.int32) // 3
    hot_ids = jax.random.randint(key_hot, (STAGES, EP_SIZE, 1), 0, EXPERTS, dtype=jnp.int32)
    base_ids = jnp.where(jnp.arange(TOKENS_DEV) % 2 == 0, hot_ids, base_ids)
    step_ids = jax.random.randint(key_step, (STAGES, EP_SIZE, TOKENS_DEV, TOP), 1, EXPERTS // TOP + 1, dtype=jnp.int32)
    step_ids = jnp.where(jnp.arange(TOP) == 0, 0, step_ids)
    expert_ids = ((base_ids[..., None] + jnp.cumsum(step_ids, axis=-1)) % EXPERTS).astype(jnp.int32)
    route_rank = jax.vmap(route_ranks)(expert_ids.reshape(STAGES * EP_SIZE, TOKENS_DEV * TOP))
    slot_ids = jnp.where(route_rank < CAP_ROWS, route_rank, -1).astype(jnp.int32)
    return expert_ids.reshape(STAGES, TOKENS, TOP), slot_ids.reshape(STAGES, TOKENS, TOP)


def setup_inputs(seed: int = 0) -> dict:
    key_list = jax.random.split(jax.random.key(seed), 14)
    tok_shape = (STAGES, TOKENS, HIDDEN)
    gate_shape = (STAGES, TOKENS, TOP)
    ids_fwd, slots_fwd = draw_routes(key_list[0])
    ids_bwd, slots_bwd = draw_routes(key_list[1])
    return {
        "x_fwd": jax.random.normal(key_list[2], tok_shape, jnp.float32).astype(jnp.bfloat16),
        "ids_fwd": ids_fwd,
        "slots_fwd": slots_fwd,
        "gates_fwd": (jax.random.uniform(key_list[3], gate_shape, jnp.float32, 0.5, 1.5) * TOP ** -0.5).astype(jnp.bfloat16),
        "x_saved": jax.random.normal(key_list[4], tok_shape, jnp.float32).astype(jnp.bfloat16),
        "grad_in": jax.random.normal(key_list[5], tok_shape, jnp.float32).astype(jnp.bfloat16),
        "ids_bwd": ids_bwd,
        "slots_bwd": slots_bwd,
        "gates_bwd": (jax.random.uniform(key_list[6], gate_shape, jnp.float32, 0.5, 1.5) * TOP ** -0.5).astype(jnp.bfloat16),
        "w_one": (jax.random.normal(key_list[7], (STAGES, HIDDEN, FF_DENSE), jnp.float32) * HIDDEN ** -0.5).astype(jnp.bfloat16),
        "w_two": (jax.random.normal(key_list[8], (STAGES, FF_DENSE, HIDDEN), jnp.float32) * FF_DENSE ** -0.5).astype(jnp.bfloat16),
        "w_gate": (jax.random.normal(key_list[9], (STAGES, EXPERTS, HIDDEN, FF_EXPERT), jnp.float32) * HIDDEN ** -0.5).astype(jnp.bfloat16),
        "w_up": (jax.random.normal(key_list[10], (STAGES, EXPERTS, HIDDEN, FF_EXPERT), jnp.float32) * HIDDEN ** -0.5).astype(jnp.bfloat16),
        "w_down": (jax.random.normal(key_list[11], (STAGES, EXPERTS, FF_EXPERT, HIDDEN), jnp.float32) * FF_EXPERT ** -0.5).astype(jnp.bfloat16),
    }


def rms_norm(values):
    return values * lax.rsqrt(jnp.mean(values * values, axis=-1, keepdims=True) + NORM_EPS)


def silu_grad(values):
    sigmoid_vals = jax.nn.sigmoid(values)
    return sigmoid_vals * (1.0 + values * (1.0 - sigmoid_vals))


def dense_forward(x_rows, w_one, w_two):
    normed = rms_norm(x_rows.astype(jnp.float32)).astype(jnp.bfloat16)
    hidden_pre = jnp.dot(normed, w_one, preferred_element_type=jnp.float32)
    dense_act = jax.nn.silu(hidden_pre).astype(jnp.bfloat16)
    dense_out = jnp.dot(dense_act, w_two, preferred_element_type=jnp.float32)
    return (x_rows.astype(jnp.float32) + dense_out).astype(jnp.bfloat16), hidden_pre


def dense_backward(x_rows, hidden_pre, w_one, w_two, grad_h):
    _, norm_vjp = jax.vjp(rms_norm, x_rows.astype(jnp.float32))
    grad_act = jnp.dot(grad_h.astype(jnp.bfloat16), w_two.T, preferred_element_type=jnp.float32)
    grad_pre = (grad_act * silu_grad(hidden_pre)).astype(jnp.bfloat16)
    grad_norm = jnp.dot(grad_pre, w_one.T, preferred_element_type=jnp.float32)
    return grad_h + norm_vjp(grad_norm)[0]


def route_maps(expert_ids, slot_ids):
    source = (jnp.arange(TOKENS, dtype=jnp.int32) // TOKENS_DEV)[:, None]
    row_index = jnp.where(slot_ids >= 0, expert_ids * (EP_SIZE * CAP_ROWS) + source * CAP_ROWS + slot_ids, BUF_ROWS)
    token_ids = jnp.broadcast_to(jnp.arange(TOKENS, dtype=jnp.int32)[:, None], expert_ids.shape)
    token_of_row = jnp.full((BUF_ROWS,), TOKENS, jnp.int32).at[row_index.reshape(-1)].set(token_ids.reshape(-1), mode="drop")
    return row_index, token_of_row


def expert_pass(operands):
    rows_fwd, rows_bwd, grad_out, w_gate, w_up, w_down = operands
    pre_gate = jnp.dot(rows_fwd, w_gate, preferred_element_type=jnp.float32)
    pre_up = jnp.dot(rows_fwd, w_up, preferred_element_type=jnp.float32)
    act_fwd = (jax.nn.silu(pre_gate) * pre_up).astype(jnp.bfloat16)
    out_fwd = jnp.dot(act_fwd, w_down, preferred_element_type=jnp.float32).astype(jnp.bfloat16)
    gate_bwd = jnp.dot(rows_bwd, w_gate, preferred_element_type=jnp.float32)
    up_bwd = jnp.dot(rows_bwd, w_up, preferred_element_type=jnp.float32)
    silu_gate = jax.nn.silu(gate_bwd)
    act_bwd = (silu_gate * up_bwd).astype(jnp.bfloat16)
    dw_down = jnp.dot(act_bwd.T, grad_out, preferred_element_type=jnp.float32)
    grad_act = jnp.dot(grad_out, w_down.T, preferred_element_type=jnp.float32).astype(jnp.bfloat16).astype(jnp.float32)
    grad_gate = (grad_act * up_bwd * silu_grad(gate_bwd)).astype(jnp.bfloat16)
    grad_up = (grad_act * silu_gate).astype(jnp.bfloat16)
    dw_gate = jnp.dot(rows_bwd.T, grad_gate, preferred_element_type=jnp.float32)
    dw_up = jnp.dot(rows_bwd.T, grad_up, preferred_element_type=jnp.float32)
    grad_rows = (jnp.dot(grad_gate, w_gate.T, preferred_element_type=jnp.float32) + jnp.dot(grad_up, w_up.T, preferred_element_type=jnp.float32)).astype(jnp.bfloat16)
    return out_fwd, grad_rows, dw_gate, dw_up, dw_down


def stage_pass(operands):
    (x_fwd, ids_fwd, slots_fwd, gates_fwd, x_saved, grad_in, ids_bwd, slots_bwd, gates_bwd, w_one, w_two, w_gate, w_up, w_down) = operands
    h_fwd, _ = dense_forward(x_fwd, w_one, w_two)
    xn_fwd = rms_norm(h_fwd.astype(jnp.float32)).astype(jnp.bfloat16)
    row_fwd, tok_fwd = route_maps(ids_fwd, slots_fwd)
    rows_fwd = jnp.take(xn_fwd, tok_fwd, axis=0, mode="fill", fill_value=0).reshape(EXPERTS, EP_SIZE * CAP_ROWS, HIDDEN)
    h_bwd, hidden_pre = dense_forward(x_saved, w_one, w_two)
    xn_bwd = rms_norm(h_bwd.astype(jnp.float32)).astype(jnp.bfloat16)
    row_bwd, tok_bwd = route_maps(ids_bwd, slots_bwd)
    rows_bwd = jnp.take(xn_bwd, tok_bwd, axis=0, mode="fill", fill_value=0).reshape(EXPERTS, EP_SIZE * CAP_ROWS, HIDDEN)
    gate_of_row = jnp.zeros((BUF_ROWS,), jnp.float32).at[row_bwd.reshape(-1)].set(gates_bwd.reshape(-1).astype(jnp.float32), mode="drop")
    grad_out = (jnp.take(grad_in, tok_bwd, axis=0, mode="fill", fill_value=0).astype(jnp.float32) * gate_of_row[:, None]).astype(jnp.bfloat16)
    grad_out = grad_out.reshape(EXPERTS, EP_SIZE * CAP_ROWS, HIDDEN)
    out_fwd, grad_rows, dw_gate, dw_up, dw_down = lax.map(expert_pass, (rows_fwd, rows_bwd, grad_out, w_gate, w_up, w_down))
    out_flat = out_fwd.reshape(BUF_ROWS, HIDDEN)
    grad_flat = grad_rows.reshape(BUF_ROWS, HIDDEN)
    mix_sum = jnp.zeros((TOKENS, HIDDEN), jnp.float32)
    grad_xn = jnp.zeros((TOKENS, HIDDEN), jnp.float32)
    for route_idx in range(TOP):
        routed = jnp.take(out_flat, row_fwd[:, route_idx], axis=0, mode="fill", fill_value=0).astype(jnp.float32)
        mix_sum = mix_sum + gates_fwd[:, route_idx].astype(jnp.float32)[:, None] * routed
        grad_xn = grad_xn + jnp.take(grad_flat, row_bwd[:, route_idx], axis=0, mode="fill", fill_value=0).astype(jnp.float32)
    y_out = (h_fwd.astype(jnp.float32) + mix_sum).astype(jnp.bfloat16)
    _, rms_vjp = jax.vjp(rms_norm, h_bwd.astype(jnp.float32))
    grad_h = grad_in.astype(jnp.float32) + rms_vjp(grad_xn)[0]
    grad_x = dense_backward(x_saved, hidden_pre, w_one, w_two, grad_h).astype(jnp.bfloat16)
    return y_out, grad_x, dw_gate, dw_up, dw_down


def reference(x_fwd, ids_fwd, slots_fwd, gates_fwd, x_saved, grad_in, ids_bwd, slots_bwd, gates_bwd, w_one, w_two, w_gate, w_up, w_down):
    y_out, dx_out, dw_gate, dw_up, dw_down = lax.map(stage_pass, (x_fwd, ids_fwd, slots_fwd, gates_fwd, x_saved, grad_in, ids_bwd, slots_bwd, gates_bwd, w_one, w_two, w_gate, w_up, w_down))
    return jnp.roll(y_out, 1, axis=0), jnp.roll(dx_out, -1, axis=0), dw_gate, dw_up, dw_down
```

```python
import functools

import jax
import jax.numpy as jnp
from jax import lax
from jax.experimental import pallas as pl
from jax.experimental.pallas import tpu as pltpu
from jax.sharding import PartitionSpec as P

NORM_EPS = 1e-6
TM = 256
BT = 512
F32 = jnp.float32
BF16 = jnp.bfloat16
VMEM_LIMIT = 60 * 1024 * 1024


def dot(a, b):
    return jnp.dot(a, b, preferred_element_type=F32)


def dot_nt(a, b):
    return lax.dot_general(a, b, (((1,), (1,)), ((), ())), preferred_element_type=F32)


def dot_tn(a, b):
    return lax.dot_general(a, b, (((0,), (0,)), ((), ())), preferred_element_type=F32)


def rms_scale(v):
    return lax.rsqrt(jnp.mean(v * v, axis=-1, keepdims=True) + NORM_EPS)


def rms_back(v, dy):
    r = rms_scale(v)
    return r * dy - v * (r * r * r * jnp.mean(dy * v, axis=-1, keepdims=True))


def dense_forward(xf, w1, w2):
    u = dot((xf * rms_scale(xf)).astype(BF16), w1)
    act = (u * jax.nn.sigmoid(u)).astype(BF16)
    return (xf + dot(act, w2)).astype(BF16)


def rank_kernel(n_exp, dump, ids_ref, slots_ref, pos_ref, tab_ref):
    ids = jnp.where(slots_ref[...] >= 0, ids_ref[...], -1)
    n = ids.shape[1]
    row = lax.broadcasted_iota(jnp.int32, (n, n), 0)
    col = lax.broadcasted_iota(jnp.int32, (n, n), 1)
    ones = jnp.ones((n, n), BF16)
    right = jnp.concatenate([jnp.where(row < col, 1.0, 0.0).astype(BF16), ones], axis=1)
    left = jnp.concatenate([jnp.where(col < row, 1.0, 0.0).astype(BF16), ones], axis=0)
    start = jnp.zeros((8, n), F32)
    pos = jnp.full((n, n), float(dump), F32)
    tab_ref[...] = jnp.zeros_like(tab_ref)
    for e in range(n_exp):
        mask = ids == e
        both = dot(jnp.where(mask, 1.0, 0.0).astype(BF16), right)
        pre = dot(left, both[:, n:].astype(BF16))
        pos = jnp.where(mask, both[:, :n] + pre[:n] + start[0:1], pos)
        tab_ref[e : e + 1, :] = (start[0:1] * (1.0 / TM)).astype(jnp.int32)
        count = pre[n : n + 8]
        start = start + TM * jnp.maximum(jnp.floor((count + (TM - 1.0)) * (1.0 / TM)), 1.0)
    tab_ref[n_exp : n_exp + 1, :] = (start[0:1] * (1.0 / TM)).astype(jnp.int32)
    pos_ref[...] = (pos * 2.0).astype(jnp.int32)


def route_ranks(ids, slots, n_exp, rows):
    n_routes = ids.size
    lanes = 128
    flat = lambda a: a.T.reshape(n_routes // lanes, lanes)
    pos, tab = pl.pallas_call(
        functools.partial(rank_kernel, n_exp, rows),
        out_shape=(
            jax.ShapeDtypeStruct((n_routes // lanes, lanes), jnp.int32),
            jax.ShapeDtypeStruct((n_exp + 8, lanes), jnp.int32),
        ),
        name="rank",
    )(flat(ids), flat(slots))
    return pos.reshape(-1), tab[:, 0]


def put_pairs(ref, rows, vals):
    n = vals.shape[0]
    half = vals.shape[1] // 2
    ref[pl.ds(rows, n, stride=2), :] = vals[:, :half]
    ref[pl.ds(rows + 1, n, stride=2), :] = vals[:, half:]


def get_pairs(ref, rows, n):
    return jnp.concatenate([ref[pl.ds(rows, n, stride=2), :], ref[pl.ds(rows + 1, n, stride=2), :]], axis=1)


def pair(p):
    return pl.ds(pl.multiple_of(p, 2), 2)


def zero_rows(ref):
    step = 512
    n = ref.shape[0]
    whole = n // step

    def body(i, c):
        ref[pl.ds(pl.multiple_of(i * step, step), step), :] = jnp.zeros((step, ref.shape[1]), F32)
        return c

    lax.fori_loop(0, whole, body, 0)
    if n % step:
        ref[whole * step :, :] = jnp.zeros((n % step, ref.shape[1]), F32)


def pre_bwd_kernel(pos_ref, gate_ref, tab_ref, x_ref, g_ref, w1_ref, w2_ref, h_ref, xs_hbm, qs_hbm, xbuf, qbuf, nsc, gsc, xst, qst, sems, *, n_blocks, top_k, n_exp):
    step = pl.program_id(0)
    n_tok = n_blocks * BT

    @pl.when(step == 0)
    def _():
        zero_rows(xbuf)
        zero_rows(qbuf)

    h = dense_forward(x_ref[...].astype(F32), w1_ref[...], w2_ref[...])
    h_ref[...] = h
    hf = h.astype(F32)
    put_pairs(nsc, 0, (hf * rms_scale(hf)).astype(BF16).astype(F32))
    put_pairs(gsc, 0, g_ref[...].astype(F32))
    base = step * BT
    unroll = 8

    def scatter(j, c):
        for k in range(unroll):
            t = j * unroll + k
            nv = nsc[pair(2 * t), :]
            gv = gsc[pair(2 * t), :]
            for r in range(top_k):
                p = pos_ref[r * n_tok + base + t]
                xbuf[pair(p), :] = nv
                qbuf[pair(p), :] = gv * gate_ref[r * n_tok + base + t]
        return c

    lax.fori_loop(0, BT // unroll, scatter, 0)

    @pl.when(step == n_blocks - 1)
    def _():
        n_tiles = tab_ref[n_exp]

        def copies(t, slot):
            rows = pl.ds(pl.multiple_of(t * TM, TM), TM)
            return (
                pltpu.make_async_copy(xst.at[slot], xs_hbm.at[rows], sems.at[0, slot]),
                pltpu.make_async_copy(qst.at[slot], qs_hbm.at[rows], sems.at[1, slot]),
            )

        def convert(t, c):
            slot = lax.rem(t, 2)

            @pl.when(t >= 2)
            def _():
                for cp in copies(t - 2, slot):
                    cp.wait()

            rows = pl.multiple_of(t * (2 * TM), 2 * TM)
            xst[slot] = get_pairs(xbuf, rows, TM).astype(BF16)
            qst[slot] = get_pairs(qbuf, rows, TM).astype(BF16)
            for cp in copies(t, slot):
                cp.start()
            return c

        lax.fori_loop(0, n_tiles, convert, 0)
        for back in (2, 1):
            for cp in copies(n_tiles - back, lax.rem(n_tiles - back, 2)):
                cp.wait()


def pre_bwd(pos, gates, tab, x, g, w1, w2, rows, n_exp, top_k):
    n_tok, hid = x.shape
    n_blocks = n_tok // BT
    smem = pl.BlockSpec(memory_space=pltpu.SMEM)
    blk = pl.BlockSpec((BT, hid), lambda i: (i, 0))
    whole = pl.BlockSpec((hid, hid), lambda i: (0, 0))
    return pl.pallas_call(
        functools.partial(pre_bwd_kernel, n_blocks=n_blocks, top_k=top_k, n_exp=n_exp),
        grid=(n_blocks,),
        in_specs=[smem, smem, smem, blk, blk, whole, whole],
        out_specs=[blk, pl.BlockSpec(memory_space=pl.ANY), pl.BlockSpec(memory_space=pl.ANY)],
        out_shape=(
            jax.ShapeDtypeStruct((n_tok, hid), BF16),
            jax.ShapeDtypeStruct((rows, hid), BF16),
            jax.ShapeDtypeStruct((rows, hid), BF16),
        ),
        scratch_shapes=[
            pltpu.VMEM((2 * rows + 8, hid // 2), F32),
            pltpu.VMEM((2 * rows + 8, hid // 2), F32),
            pltpu.VMEM((2 * BT, hid // 2), F32),
            pltpu.VMEM((2 * BT, hid // 2), F32),
            pltpu.VMEM((2, TM, hid), BF16),
            pltpu.VMEM((2, TM, hid), BF16),
            pltpu.SemaphoreType.DMA((2, 2)),
        ],
        compiler_params=pltpu.CompilerParams(vmem_limit_bytes=VMEM_LIMIT),
        cost_estimate=pl.CostEstimate(flops=30_000_000_000, bytes_accessed=30_000_000, transcendentals=0),
        name="pre_bwd",
    )(pos, gates, tab, x, g, w1, w2)


def exp_bwd_kernel(first_ref, tab_ref, wg_ref, wu_ref, wd_ref, xs_hbm, qs_hbm, rs_hbm, dwg_ref, dwu_ref, dwd_ref, xb, qb, rb, sems, *, n_loc):
    first = first_ref[0]
    begin = tab_ref[first]
    end = tab_ref[first + n_loc]

    def rows_of(t):
        return pl.ds(pl.multiple_of(t * TM, TM), TM)

    def loads(t, slot):
        return (
            pltpu.make_async_copy(xs_hbm.at[rows_of(t)], xb.at[slot], sems.at[0, slot]),
            pltpu.make_async_copy(qs_hbm.at[rows_of(t)], qb.at[slot], sems.at[1, slot]),
        )

    def save(t, slot):
        return pltpu.make_async_copy(rb.at[slot], rs_hbm.at[rows_of(t)], sems.at[2, slot])

    for cp in loads(begin, lax.rem(begin, 2)):
        cp.start()
    dwg_ref[...] = jnp.zeros_like(dwg_ref)
    dwu_ref[...] = jnp.zeros_like(dwu_ref)
    dwd_ref[...] = jnp.zeros_like(dwd_ref)

    def body(t, e):
        slot = lax.rem(t, 2)
        e = jnp.where(t >= tab_ref[first + e + 1], e + 1, e)

        @pl.when(t + 1 < end)
        def _():
            for cp in loads(t + 1, 1 - slot):
                cp.start()

        for cp in loads(t, slot):
            cp.wait()

        @pl.when(t >= begin + 2)
        def _():
            save(t - 2, slot).wait()

        x = xb[slot]
        q = qb[slot]
        wg, wu, wd = wg_ref[e], wu_ref[e], wd_ref[e]
        pre = dot(x, wg)
        up = dot(x, wu)
        sig = jax.nn.sigmoid(pre)
        sil = pre * sig
        act = (sil * up).astype(BF16)
        dwd_ref[e] += dot_tn(act, q)
        da = dot_nt(q, wd).astype(BF16).astype(F32)
        dpre = (da * up * (sig * (1.0 + pre * (1.0 - sig)))).astype(BF16)
        dup = (da * sil).astype(BF16)
        dwg_ref[e] += dot_tn(x, dpre)
        dwu_ref[e] += dot_tn(x, dup)
        rb[slot] = (dot_nt(dpre, wg) + dot_nt(dup, wu)).astype(BF16)
        save(t, slot).start()
        return e

    lax.fori_loop(begin, end, body, 0)
    for back in (2, 1):
        save(end - back, lax.rem(end - back, 2)).wait()


def exp_bwd(first, tab, wg, wu, wd, xs, qs):
    n_loc, hid, ff = wg.shape
    smem = pl.BlockSpec(memory_space=pltpu.SMEM)
    vmem = pl.BlockSpec(memory_space=pltpu.VMEM)
    hbm = pl.BlockSpec(memory_space=pl.ANY)
    dw = jax.ShapeDtypeStruct((n_loc, hid, ff), F32)
    return pl.pallas_call(
        functools.partial(exp_bwd_kernel, n_loc=n_loc),
        in_specs=[smem, smem, vmem, vmem, vmem, hbm, hbm],
        out_specs=[hbm, vmem, vmem, vmem],
        out_shape=(jax.ShapeDtypeStruct(xs.shape, BF16), dw, dw, dw),
        input_output_aliases={5: 0},
        scratch_shapes=[
            pltpu.VMEM((2, TM, hid), BF16),
            pltpu.VMEM((2, TM, hid), BF16),
            pltpu.VMEM((2, TM, hid), BF16),
            pltpu.SemaphoreType.DMA((3, 2)),
        ],
        compiler_params=pltpu.CompilerParams(vmem_limit_bytes=VMEM_LIMIT),
        cost_estimate=pl.CostEstimate(flops=8_000_000_000, bytes_accessed=20_000_000, transcendentals=0),
        name="exp_bwd",
    )(first, tab, wg, wu, wd, xs, qs)


def post_bwd_kernel(pos_ref, tab_ref, x_ref, g_ref, h_ref, w1_ref, w2_ref, rs_hbm, dx_ref, rbuf, acc, st, sems, *, n_blocks, top_k, n_exp, rows):
    step = pl.program_id(0)
    n_tok = n_blocks * BT

    @pl.when(step == 0)
    def _():
        n_tiles = tab_ref[n_exp]

        def load(t, slot):
            return pltpu.make_async_copy(rs_hbm.at[pl.ds(pl.multiple_of(t * TM, TM), TM)], st.at[slot], sems.at[slot])

        load(0, 0).start()
        rbuf[2 * rows : 2 * rows + 8, :] = jnp.zeros((8, rbuf.shape[1]), F32)

        def expand(t, c):
            slot = lax.rem(t, 2)

            @pl.when(t + 1 < n_tiles)
            def _():
                load(t + 1, 1 - slot).start()

            load(t, slot).wait()
            put_pairs(rbuf, pl.multiple_of(t * (2 * TM), 2 * TM), st[slot].astype(F32))
            return c

        lax.fori_loop(0, n_tiles, expand, 0)

    base = step * BT
    unroll = 8

    def gather(j, c):
        for k in range(unroll):
            t = j * unroll + k
            total = rbuf[pair(pos_ref[base + t]), :]
            for r in range(1, top_k):
                total = total + rbuf[pair(pos_ref[r * n_tok + base + t]), :]
            acc[pair(2 * t), :] = total
        return c

    lax.fori_loop(0, BT // unroll, gather, 0)
    dn = get_pairs(acc, 0, BT)
    xf = x_ref[...].astype(F32)
    u = dot((xf * rms_scale(xf)).astype(BF16), w1_ref[...])
    dh = g_ref[...].astype(F32) + rms_back(h_ref[...].astype(F32), dn)
    sig = jax.nn.sigmoid(u)
    du = (dot_nt(dh.astype(BF16), w2_ref[...]) * (sig * (1.0 + u * (1.0 - sig)))).astype(BF16)
    dx_ref[...] = (dh + rms_back(xf, dot_nt(du, w1_ref[...]))).astype(BF16)


def post_bwd(pos, tab, x, g, h, w1, w2, rs, n_exp, top_k):
    n_tok, hid = x.shape
    rows = rs.shape[0]
    n_blocks = n_tok // BT
    smem = pl.BlockSpec(memory_space=pltpu.SMEM)
    blk = pl.BlockSpec((BT, hid), lambda i: (i, 0))
    whole = pl.BlockSpec((hid, hid), lambda i: (0, 0))
    return pl.pallas_call(
        functools.partial(post_bwd_kernel, n_blocks=n_blocks, top_k=top_k, n_exp=n_exp, rows=rows),
        grid=(n_blocks,),
        in_specs=[smem, smem, blk, blk, blk, whole, whole, pl.BlockSpec(memory_space=pl.ANY)],
        out_specs=blk,
        out_shape=jax.ShapeDtypeStruct((n_tok, hid), BF16),
        scratch_shapes=[
            pltpu.VMEM((2 * rows + 8, hid // 2), F32),
            pltpu.VMEM((2 * BT, hid // 2), F32),
            pltpu.VMEM((2, TM, hid), BF16),
            pltpu.SemaphoreType.DMA((2,)),
        ],
        compiler_params=pltpu.CompilerParams(vmem_limit_bytes=VMEM_LIMIT),
        cost_estimate=pl.CostEstimate(flops=30_000_000_000, bytes_accessed=30_000_000, transcendentals=0),
        name="post_bwd",
    )(pos, tab, x, g, h, w1, w2, rs)


def fwd_kernel(firsts_ref, pos_ref, gate_ref, tab_ref, x_ref, w1_ref, w2_ref, *rest, n_blocks, top_k, n_exp, n_groups, rows):
    w_hbm = rest[: 3 * n_groups]
    y_ref, buf, nsc, hsc, wsc, sems = rest[3 * n_groups :]
    step = pl.program_id(0)
    n_tok = n_blocks * BT
    n_loc = n_exp // n_groups
    unroll = 8

    def w_copy(i):
        return pltpu.make_async_copy(w_hbm[i], wsc.at[i], sems.at[i])

    @pl.when(step == 0)
    def _():
        for i in range(3 * n_groups):
            w_copy(i).start()
        zero_rows(buf)

    @pl.when(step < n_blocks)
    def _():
        h = dense_forward(x_ref[...].astype(F32), w1_ref[...], w2_ref[...])
        base = step * BT
        hsc[pl.ds(pl.multiple_of(base, BT), BT), :] = h
        hf = h.astype(F32)
        put_pairs(nsc, 0, (hf * rms_scale(hf)).astype(BF16).astype(F32))

        def scatter(j, c):
            for k in range(unroll):
                t = j * unroll + k
                nv = nsc[pair(2 * t), :]
                for r in range(top_k):
                    buf[pair(pos_ref[r * n_tok + base + t]), :] = nv
            return c

        lax.fori_loop(0, BT // unroll, scatter, 0)

    @pl.when(step == n_blocks)
    def _():
        buf[2 * rows : 2 * rows + 8, :] = jnp.zeros((8, buf.shape[1]), F32)
        for g in range(n_groups):
            for i in range(3):
                w_copy(3 * g + i).wait()
            first = firsts_ref[g]

            def body(t, e):
                e = jnp.where(t >= tab_ref[first + e + 1], e + 1, e)
                at = pl.multiple_of(t * (2 * TM), 2 * TM)
                x = get_pairs(buf, at, TM).astype(BF16)
                pre = dot(x, wsc[3 * g, e])
                up = dot(x, wsc[3 * g + 1, e])
                act = (pre * jax.nn.sigmoid(pre) * up).astype(BF16)
                put_pairs(buf, at, dot(act, wsc[3 * g + 2, e]).astype(BF16).astype(F32))
                return e

            lax.fori_loop(tab_ref[first], tab_ref[first + n_loc], body, 0)

    @pl.when(step > n_blocks)
    def _():
        base = (step - n_blocks - 1) * BT

        def gather(j, c):
            for k in range(unroll):
                t = j * unroll + k
                total = None
                for r in range(top_k):
                    at = r * n_tok + base + t
                    term = buf[pair(pos_ref[at]), :] * gate_ref[at]
                    total = term if total is None else total + term
                nsc[pair(2 * t), :] = total
            return c

        lax.fori_loop(0, BT // unroll, gather, 0)
        h = hsc[pl.ds(pl.multiple_of(base, BT), BT), :]
        y_ref[...] = (h.astype(F32) + get_pairs(nsc, 0, BT)).astype(BF16)


def fwd(firsts, pos, gates, tab, x, w1, w2, weights, rows, n_exp, top_k):
    n_tok, hid = x.shape
    n_blocks = n_tok // BT
    n_groups = len(weights)
    n_loc = n_exp // n_groups
    smem = pl.BlockSpec(memory_space=pltpu.SMEM)
    whole = pl.BlockSpec((hid, hid), lambda i: (0, 0))
    flat = [w for group in weights for w in group]
    return pl.pallas_call(
        functools.partial(fwd_kernel, n_blocks=n_blocks, top_k=top_k, n_exp=n_exp, n_groups=n_groups, rows=rows),
        grid=(2 * n_blocks + 1,),
        in_specs=[smem, smem, smem, smem, pl.BlockSpec((BT, hid), lambda i: (jnp.minimum(i, n_blocks - 1), 0)), whole, whole]
        + [pl.BlockSpec(memory_space=pl.ANY)] * len(flat),
        out_specs=pl.BlockSpec((BT, hid), lambda i: (jnp.maximum(i - n_blocks - 1, 0), 0)),
        out_shape=jax.ShapeDtypeStruct((n_tok, hid), BF16),
        scratch_shapes=[
            pltpu.VMEM((2 * rows + 8, hid // 2), F32),
            pltpu.VMEM((2 * BT, hid // 2), F32),
            pltpu.VMEM((n_tok, hid), BF16),
            pltpu.VMEM((len(flat), n_loc, hid, hid), BF16),
            pltpu.SemaphoreType.DMA((len(flat),)),
        ],
        compiler_params=pltpu.CompilerParams(vmem_limit_bytes=VMEM_LIMIT),
        cost_estimate=pl.CostEstimate(flops=80_000_000_000, bytes_accessed=30_000_000, transcendentals=0),
        name="fwd",
    )(firsts, pos, gates, tab, x, w1, w2, *flat)


def solution(mesh):
    stages = mesh.shape["pp"]
    ep_size = mesh.shape["ep"]
    next_perm = [(i, (i + 1) % stages) for i in range(stages)]
    prev_perm = [(i, (i - 1) % stages) for i in range(stages)]
    mate_perm = [(i, i ^ 1) for i in range(ep_size)]
    chip_perm = [(i, i ^ 2) for i in range(ep_size)]
    tok_spec = P("pp", "ep", None)
    dense_spec = P("pp", None, None)
    expert_spec = P("pp", "ep", None, None)

    def mate(a):
        return lax.ppermute(a, "ep", mate_perm)

    def chip(a):
        return lax.ppermute(a, "ep", chip_perm)

    def device_step(x_fwd, ids_fwd, slots_fwd, gates_fwd, x_saved, grad_in, ids_bwd, slots_bwd, gates_bwd, w_one, w_two, w_gate, w_up, w_down):
        x_fwd, ids_fwd, slots_fwd, gates_fwd = x_fwd[0], ids_fwd[0], slots_fwd[0], gates_fwd[0]
        x_saved, grad_in, ids_bwd, slots_bwd, gates_bwd = x_saved[0], grad_in[0], ids_bwd[0], slots_bwd[0], gates_bwd[0]
        w1, w2, w_gate, w_up, w_down = w_one[0], w_two[0], w_gate[0], w_up[0], w_down[0]
        top_k = ids_fwd.shape[1]
        n_loc = w_gate.shape[0]
        n_exp = n_loc * ep_size
        rows = TM * (ids_fwd.size // TM + n_exp)
        me = lax.axis_index("ep")

        own = (w_gate, w_up, w_down)
        far = tuple(chip(w) for w in own)
        near = tuple(mate(w) for w in own)
        far_near = tuple(mate(w) for w in far)
        weights = (own, near, far, far_near)
        firsts = [(me ^ g) * n_loc for g in range(ep_size)]

        pos_b, tab_b = route_ranks(ids_bwd, slots_bwd, n_exp, rows)
        pos_f, tab_f = route_ranks(ids_fwd, slots_fwd, n_exp, rows)
        gates_b = gates_bwd.T.reshape(-1).astype(F32)
        gates_f = gates_fwd.T.reshape(-1).astype(F32)

        h_bwd, xs, qs = pre_bwd(pos_b, gates_b, tab_b, x_saved, grad_in, w1, w2, rows, n_exp, top_k)
        parts = []
        for g in range(ep_size):
            xs, *dw = exp_bwd(firsts[g].reshape(1), tab_b, *weights[g], xs, qs)
            parts.append(dw)
        grad_x = post_bwd(pos_b, tab_b, x_saved, grad_in, h_bwd, w1, w2, xs, n_exp, top_k)
        dx_prev = lax.ppermute(grad_x, "pp", prev_perm)

        dws = []
        for i in range(3):
            there = chip(parts[2][i] + mate(parts[3][i]))
            dws.append(parts[0][i] + mate(parts[1][i]) + there)

        y_out = fwd(jnp.stack(firsts), pos_f, gates_f, tab_f, x_fwd, w1, w2, weights, rows, n_exp, top_k)
        y_next = lax.ppermute(y_out, "pp", next_perm)
        return y_next[None], dx_prev[None], dws[0][None], dws[1][None], dws[2][None]

    in_specs = (tok_spec,) * 9 + (dense_spec, dense_spec, expert_spec, expert_spec, expert_spec)
    out_specs = (tok_spec, tok_spec, expert_spec, expert_spec, expert_spec)
    return jax.shard_map(device_step, mesh=mesh, in_specs=in_specs, out_specs=out_specs, check_vma=False)
```

```python
import functools

import jax
import jax.numpy as jnp
from jax import lax
from jax.experimental import pallas as pl
from jax.experimental.pallas import tpu as pltpu
from jax.sharding import PartitionSpec as P

NORM_EPS = 1e-6
TM = 256
BT = 512
DEPTH = 4
F32 = jnp.float32
BF16 = jnp.bfloat16
VMEM_LIMIT = 60 * 1024 * 1024


def dot(a, b):
    return jnp.dot(a, b, preferred_element_type=F32)


def dot_nt(a, b):
    return lax.dot_general(a, b, (((1,), (1,)), ((), ())), preferred_element_type=F32)


def dot_tn(a, b):
    return lax.dot_general(a, b, (((0,), (0,)), ((), ())), preferred_element_type=F32)


def rms_scale(v):
    return lax.rsqrt(jnp.mean(v * v, axis=-1, keepdims=True) + NORM_EPS)


def rms_back(v, dy):
    r = rms_scale(v)
    return r * dy - v * (r * r * r * jnp.mean(dy * v, axis=-1, keepdims=True))


def dense_forward(xf, w1, w2):
    u = dot((xf * rms_scale(xf)).astype(BF16), w1)
    act = (u * jax.nn.sigmoid(u)).astype(BF16)
    return (xf + dot(act, w2)).astype(BF16)


def rank_kernel(n_exp, dump, ids_ref, slots_ref, pos_ref, tab_ref):
    ids = jnp.where(slots_ref[...] >= 0, ids_ref[...], -1)
    n = ids.shape[1]
    row = lax.broadcasted_iota(jnp.int32, (n, n), 0)
    col = lax.broadcasted_iota(jnp.int32, (n, n), 1)
    ones = jnp.ones((n, n), BF16)
    right = jnp.concatenate([jnp.where(row < col, 1.0, 0.0).astype(BF16), ones], axis=1)
    left = jnp.concatenate([jnp.where(col < row, 1.0, 0.0).astype(BF16), ones], axis=0)
    start = jnp.zeros((8, n), F32)
    pos = jnp.full((n, n), float(dump), F32)
    tab_ref[...] = jnp.zeros_like(tab_ref)
    for e in range(n_exp):
        mask = ids == e
        both = dot(jnp.where(mask, 1.0, 0.0).astype(BF16), right)
        pre = dot(left, both[:, n:].astype(BF16))
        pos = jnp.where(mask, both[:, :n] + pre[:n] + start[0:1], pos)
        tab_ref[e : e + 1, :] = (start[0:1] * (1.0 / TM)).astype(jnp.int32)
        count = pre[n : n + 8]
        start = start + TM * jnp.maximum(jnp.floor((count + (TM - 1.0)) * (1.0 / TM)), 1.0)
    tab_ref[n_exp : n_exp + 1, :] = (start[0:1] * (1.0 / TM)).astype(jnp.int32)
    pos_ref[...] = pos.astype(jnp.int32)


def route_ranks(ids, slots, n_exp, rows):
    n_routes = ids.size
    lanes = 128
    flat = lambda a: a.T.reshape(n_routes // lanes, lanes)
    pos, tab = pl.pallas_call(
        functools.partial(rank_kernel, n_exp, rows),
        out_shape=(
            jax.ShapeDtypeStruct((n_routes // lanes, lanes), jnp.int32),
            jax.ShapeDtypeStruct((n_exp + 8, lanes), jnp.int32),
        ),
        name="rank",
    )(flat(ids), flat(slots))
    return pos.reshape(-1), tab[:, 0]


def put_rows(ref, at, vals, pitch=2, off=0):
    n = vals.shape[0]
    half = vals.shape[1] // 2
    ref[pl.ds(at + off, n, stride=pitch), :] = vals[:, :half]
    ref[pl.ds(at + off + 1, n, stride=pitch), :] = vals[:, half:]


def get_rows(ref, at, n, pitch=2, off=0):
    return jnp.concatenate([ref[pl.ds(at + off + i, n, stride=pitch), :] for i in range(2)], axis=1)


def pair(p):
    return pl.ds(pl.multiple_of(p * 2, 2), 2)


def gather_sum(buf, acc, pos_ref, gate_ref, first, n_tok, top_k):
    unroll = 8

    def body(j, c):
        base = first + j * unroll
        at = pl.multiple_of(j * (2 * unroll), 2 * unroll)
        for k in range(unroll):
            total = None
            for r in range(top_k):
                i = base + (r * n_tok + k)
                term = buf[pair(pos_ref[i]), :]
                if gate_ref is not None:
                    term = term * gate_ref[i]
                total = term if total is None else total + term
            acc[pl.ds(at + 2 * k, 2), :] = total
        return c

    lax.fori_loop(0, BT // unroll, body, 0)


def zero_rows(ref):
    step = 512
    n = ref.shape[0]
    whole = n // step

    def body(i, c):
        ref[pl.ds(pl.multiple_of(i * step, step), step), :] = jnp.zeros((step, ref.shape[1]), F32)
        return c

    lax.fori_loop(0, whole, body, 0)
    if n % step:
        ref[whole * step :, :] = jnp.zeros((n % step, ref.shape[1]), F32)


def pre_bwd_kernel(pos_ref, gate_ref, tab_ref, x_ref, g_ref, w1_ref, w2_ref, h_ref, xs_hbm, qs_hbm, buf, src, xst, qst, sems, *, n_blocks, top_k, n_exp):
    step = pl.program_id(0)
    n_tok = n_blocks * BT

    @pl.when(step == 0)
    def _():
        zero_rows(buf)

    h = dense_forward(x_ref[...].astype(F32), w1_ref[...], w2_ref[...])
    h_ref[...] = h
    hf = h.astype(F32)
    put_rows(src, 0, (hf * rms_scale(hf)).astype(BF16).astype(F32), 4, 0)
    put_rows(src, 0, g_ref[...].astype(F32), 4, 2)
    unroll = 8
    is_row = lax.broadcasted_iota(jnp.int32, (4, buf.shape[1]), 0) < 2

    def scatter(j, c):
        base = step * BT + j * unroll
        at = pl.multiple_of(j * (4 * unroll), 4 * unroll)
        for k in range(unroll):
            v = src[pl.ds(at + 4 * k, 4), :]
            for r in range(top_k):
                p = pl.multiple_of(pos_ref[base + (r * n_tok + k)] * 4, 4)
                buf[pl.ds(p, 4), :] = v * jnp.where(is_row, 1.0, gate_ref[base + (r * n_tok + k)])
        return c

    lax.fori_loop(0, BT // unroll, scatter, 0)

    @pl.when(step == n_blocks - 1)
    def _():
        n_tiles = tab_ref[n_exp]

        def copies(t, slot):
            rows = pl.ds(pl.multiple_of(t * TM, TM), TM)
            return (
                pltpu.make_async_copy(xst.at[slot], xs_hbm.at[rows], sems.at[0, slot]),
                pltpu.make_async_copy(qst.at[slot], qs_hbm.at[rows], sems.at[1, slot]),
            )

        def convert(t, c):
            slot = lax.rem(t, DEPTH)

            @pl.when(t >= DEPTH)
            def _():
                for cp in copies(t - DEPTH, slot):
                    cp.wait()

            rows = pl.multiple_of(t * (4 * TM), 4 * TM)
            xst[slot] = get_rows(buf, rows, TM, 4, 0).astype(BF16)
            qst[slot] = get_rows(buf, rows, TM, 4, 2).astype(BF16)
            for cp in copies(t, slot):
                cp.start()
            return c

        lax.fori_loop(0, n_tiles, convert, 0)
        for back in range(DEPTH, 0, -1):
            for cp in copies(n_tiles - back, lax.rem(n_tiles - back, DEPTH)):
                cp.wait()


def pre_bwd(pos, gates, tab, x, g, w1, w2, rows, n_exp, top_k):
    n_tok, hid = x.shape
    n_blocks = n_tok // BT
    smem = pl.BlockSpec(memory_space=pltpu.SMEM)
    blk = pl.BlockSpec((BT, hid), lambda i: (i, 0))
    whole = pl.BlockSpec((hid, hid), lambda i: (0, 0))
    return pl.pallas_call(
        functools.partial(pre_bwd_kernel, n_blocks=n_blocks, top_k=top_k, n_exp=n_exp),
        grid=(n_blocks,),
        in_specs=[smem, smem, smem, blk, blk, whole, whole],
        out_specs=[blk, pl.BlockSpec(memory_space=pl.ANY), pl.BlockSpec(memory_space=pl.ANY)],
        out_shape=(
            jax.ShapeDtypeStruct((n_tok, hid), BF16),
            jax.ShapeDtypeStruct((rows, hid), BF16),
            jax.ShapeDtypeStruct((rows, hid), BF16),
        ),
        scratch_shapes=[
            pltpu.VMEM((4 * rows + 8, hid // 2), F32),
            pltpu.VMEM((4 * BT, hid // 2), F32),
            pltpu.VMEM((DEPTH, TM, hid), BF16),
            pltpu.VMEM((DEPTH, TM, hid), BF16),
            pltpu.SemaphoreType.DMA((2, DEPTH)),
        ],
        compiler_params=pltpu.CompilerParams(vmem_limit_bytes=VMEM_LIMIT),
        cost_estimate=pl.CostEstimate(flops=30_000_000_000, bytes_accessed=30_000_000, transcendentals=0),
        name="pre_bwd",
    )(pos, gates, tab, x, g, w1, w2)


def exp_bwd_kernel(first_ref, tab_ref, wg_hbm, wu_hbm, wd_hbm, xs_hbm, qs_hbm, rs_hbm, dwg_hbm, dwu_hbm, dwd_hbm, wb, dwb, xb, qb, rb, sems, wsems, dsems, *, n_loc):
    first = first_ref[0]
    begin = tab_ref[first]
    end = tab_ref[first + n_loc]
    w_hbm = (wg_hbm, wu_hbm, wd_hbm)
    dw_hbm = (dwg_hbm, dwu_hbm, dwd_hbm)

    def rows_of(t):
        return pl.ds(pl.multiple_of(t * TM, TM), TM)

    def loads(t):
        slot = lax.rem(t, DEPTH)
        return (
            pltpu.make_async_copy(xs_hbm.at[rows_of(t)], xb.at[slot], sems.at[0, slot]),
            pltpu.make_async_copy(qs_hbm.at[rows_of(t)], qb.at[slot], sems.at[1, slot]),
        )

    def save(t):
        slot = lax.rem(t, DEPTH)
        return pltpu.make_async_copy(rb.at[slot], rs_hbm.at[rows_of(t)], sems.at[2, slot])

    def w_loads(e):
        slot = lax.rem(e, 2)
        return [pltpu.make_async_copy(w_hbm[i].at[e], wb.at[slot, i], wsems.at[i, slot]) for i in range(3)]

    def dw_saves(e):
        slot = lax.rem(e, 2)
        return [pltpu.make_async_copy(dwb.at[slot, i], dw_hbm[i].at[e], dsems.at[i, slot]) for i in range(3)]

    for cp in w_loads(0):
        cp.start()
    for ahead in range(DEPTH - 1):
        for cp in loads(begin + ahead):
            cp.start()

    def expert(e, c):
        wslot = lax.rem(e, 2)
        for cp in w_loads(e):
            cp.wait()

        @pl.when(e + 1 < n_loc)
        def _():
            for cp in w_loads(e + 1):
                cp.start()

        @pl.when(e >= 2)
        def _():
            for cp in dw_saves(e - 2):
                cp.wait()

        dwb[wslot] = jnp.zeros(dwb.shape[1:], F32)

        def body(t, c):
            slot = lax.rem(t, DEPTH)

            @pl.when(t + (DEPTH - 1) < end)
            def _():
                for cp in loads(t + (DEPTH - 1)):
                    cp.start()

            for cp in loads(t):
                cp.wait()

            @pl.when(t >= begin + DEPTH)
            def _():
                save(t - DEPTH).wait()

            x = xb[slot]
            q = qb[slot]
            wg, wu, wd = wb[wslot, 0], wb[wslot, 1], wb[wslot, 2]
            pre = dot(x, wg)
            up = dot(x, wu)
            sig = jax.nn.sigmoid(pre)
            sil = pre * sig
            act = (sil * up).astype(BF16)
            dwb[wslot, 2] += dot_tn(act, q)
            da = dot_nt(q, wd).astype(BF16).astype(F32)
            dpre = (da * up * (sig * (1.0 + pre * (1.0 - sig)))).astype(BF16)
            dup = (da * sil).astype(BF16)
            dwb[wslot, 0] += dot_tn(x, dpre)
            dwb[wslot, 1] += dot_tn(x, dup)
            rb[slot] = (dot_nt(dpre, wg) + dot_nt(dup, wu)).astype(BF16)
            save(t).start()
            return c

        lax.fori_loop(tab_ref[first + e], tab_ref[first + e + 1], body, 0)
        for cp in dw_saves(e):
            cp.start()
        return c

    lax.fori_loop(0, n_loc, expert, 0)
    for back in range(DEPTH, 0, -1):
        save(end - back).wait()
    for e in (n_loc - 2, n_loc - 1):
        for cp in dw_saves(e):
            cp.wait()


def exp_bwd(first, tab, wg, wu, wd, xs, qs):
    n_loc, hid, ff = wg.shape
    smem = pl.BlockSpec(memory_space=pltpu.SMEM)
    hbm = pl.BlockSpec(memory_space=pl.ANY)
    dw = jax.ShapeDtypeStruct((n_loc, hid, ff), F32)
    return pl.pallas_call(
        functools.partial(exp_bwd_kernel, n_loc=n_loc),
        in_specs=[smem, smem, hbm, hbm, hbm, hbm, hbm],
        out_specs=[hbm, hbm, hbm, hbm],
        out_shape=(jax.ShapeDtypeStruct(xs.shape, BF16), dw, dw, dw),
        input_output_aliases={5: 0},
        scratch_shapes=[
            pltpu.VMEM((2, 3, hid, ff), BF16),
            pltpu.VMEM((2, 3, hid, ff), F32),
            pltpu.VMEM((DEPTH, TM, hid), BF16),
            pltpu.VMEM((DEPTH, TM, hid), BF16),
            pltpu.VMEM((DEPTH, TM, hid), BF16),
            pltpu.SemaphoreType.DMA((3, DEPTH)),
            pltpu.SemaphoreType.DMA((3, 2)),
            pltpu.SemaphoreType.DMA((3, 2)),
        ],
        compiler_params=pltpu.CompilerParams(vmem_limit_bytes=VMEM_LIMIT),
        cost_estimate=pl.CostEstimate(flops=8_000_000_000, bytes_accessed=20_000_000, transcendentals=0),
        name="exp_bwd",
    )(first, tab, wg, wu, wd, xs, qs)


def post_bwd_kernel(pos_ref, tab_ref, x_ref, g_ref, h_ref, w1_ref, w2_ref, rs_hbm, dx_ref, rbuf, acc, st, sems, *, n_blocks, top_k, n_exp, rows):
    step = pl.program_id(0)
    n_tok = n_blocks * BT

    @pl.when(step == 0)
    def _():
        n_tiles = tab_ref[n_exp]

        def load(t):
            slot = lax.rem(t, DEPTH)
            return pltpu.make_async_copy(rs_hbm.at[pl.ds(pl.multiple_of(t * TM, TM), TM)], st.at[slot], sems.at[slot])

        for ahead in range(DEPTH - 1):
            load(ahead).start()
        rbuf[2 * rows : 2 * rows + 8, :] = jnp.zeros((8, rbuf.shape[1]), F32)

        def expand(t, c):
            @pl.when(t + (DEPTH - 1) < n_tiles)
            def _():
                load(t + (DEPTH - 1)).start()

            load(t).wait()
            put_rows(rbuf, pl.multiple_of(t * (2 * TM), 2 * TM), st[lax.rem(t, DEPTH)].astype(F32))
            return c

        lax.fori_loop(0, n_tiles, expand, 0)

    gather_sum(rbuf, acc, pos_ref, None, step * BT, n_tok, top_k)
    dn = get_rows(acc, 0, BT)
    xf = x_ref[...].astype(F32)
    u = dot((xf * rms_scale(xf)).astype(BF16), w1_ref[...])
    dh = g_ref[...].astype(F32) + rms_back(h_ref[...].astype(F32), dn)
    sig = jax.nn.sigmoid(u)
    du = (dot_nt(dh.astype(BF16), w2_ref[...]) * (sig * (1.0 + u * (1.0 - sig)))).astype(BF16)
    dx_ref[...] = (dh + rms_back(xf, dot_nt(du, w1_ref[...]))).astype(BF16)


def post_bwd(pos, tab, x, g, h, w1, w2, rs, n_exp, top_k):
    n_tok, hid = x.shape
    rows = rs.shape[0]
    n_blocks = n_tok // BT
    smem = pl.BlockSpec(memory_space=pltpu.SMEM)
    blk = pl.BlockSpec((BT, hid), lambda i: (i, 0))
    whole = pl.BlockSpec((hid, hid), lambda i: (0, 0))
    return pl.pallas_call(
        functools.partial(post_bwd_kernel, n_blocks=n_blocks, top_k=top_k, n_exp=n_exp, rows=rows),
        grid=(n_blocks,),
        in_specs=[smem, smem, blk, blk, blk, whole, whole, pl.BlockSpec(memory_space=pl.ANY)],
        out_specs=blk,
        out_shape=jax.ShapeDtypeStruct((n_tok, hid), BF16),
        scratch_shapes=[
            pltpu.VMEM((2 * rows + 8, hid // 2), F32),
            pltpu.VMEM((2 * BT, hid // 2), F32),
            pltpu.VMEM((DEPTH, TM, hid), BF16),
            pltpu.SemaphoreType.DMA((DEPTH,)),
        ],
        compiler_params=pltpu.CompilerParams(vmem_limit_bytes=VMEM_LIMIT),
        cost_estimate=pl.CostEstimate(flops=30_000_000_000, bytes_accessed=30_000_000, transcendentals=0),
        name="post_bwd",
    )(pos, tab, x, g, h, w1, w2, rs)


def fwd_kernel(firsts_ref, pos_ref, gate_ref, tab_ref, x_ref, w1_ref, w2_ref, *rest, n_blocks, top_k, n_exp, n_groups, rows):
    w_hbm = rest[: 3 * n_groups]
    y_ref, buf, nsc, hsc, wsc, sems = rest[3 * n_groups :]
    step = pl.program_id(0)
    n_tok = n_blocks * BT
    n_loc = n_exp // n_groups
    unroll = 8

    def w_copy(i):
        return pltpu.make_async_copy(w_hbm[i], wsc.at[i], sems.at[i])

    @pl.when(step == 0)
    def _():
        for i in range(3 * n_groups):
            w_copy(i).start()
        zero_rows(buf)

    @pl.when(step < n_blocks)
    def _():
        h = dense_forward(x_ref[...].astype(F32), w1_ref[...], w2_ref[...])
        base = step * BT
        hsc[pl.ds(pl.multiple_of(base, BT), BT), :] = h
        hf = h.astype(F32)
        put_rows(nsc, 0, (hf * rms_scale(hf)).astype(BF16).astype(F32))

        def scatter(j, c):
            first = base + j * unroll
            at = pl.multiple_of(j * (2 * unroll), 2 * unroll)
            for k in range(unroll):
                nv = nsc[pl.ds(at + 2 * k, 2), :]
                for r in range(top_k):
                    buf[pair(pos_ref[first + (r * n_tok + k)]), :] = nv
            return c

        lax.fori_loop(0, BT // unroll, scatter, 0)

    @pl.when(step == n_blocks)
    def _():
        buf[2 * rows : 2 * rows + 8, :] = jnp.zeros((8, buf.shape[1]), F32)
        for g in range(n_groups):
            for i in range(3):
                w_copy(3 * g + i).wait()
            first = firsts_ref[g]

            def body(t, e):
                e = jnp.where(t >= tab_ref[first + e + 1], e + 1, e)
                at = pl.multiple_of(t * (2 * TM), 2 * TM)
                x = get_rows(buf, at, TM).astype(BF16)
                pre = dot(x, wsc[3 * g, e])
                up = dot(x, wsc[3 * g + 1, e])
                act = (pre * jax.nn.sigmoid(pre) * up).astype(BF16)
                put_rows(buf, at, dot(act, wsc[3 * g + 2, e]).astype(BF16).astype(F32))
                return e

            lax.fori_loop(tab_ref[first], tab_ref[first + n_loc], body, 0)

    @pl.when(step > n_blocks)
    def _():
        base = (step - n_blocks - 1) * BT

        gather_sum(buf, nsc, pos_ref, gate_ref, base, n_tok, top_k)
        h = hsc[pl.ds(pl.multiple_of(base, BT), BT), :]
        y_ref[...] = (h.astype(F32) + get_rows(nsc, 0, BT)).astype(BF16)


def fwd(firsts, pos, gates, tab, x, w1, w2, weights, rows, n_exp, top_k):
    n_tok, hid = x.shape
    n_blocks = n_tok // BT
    n_groups = len(weights)
    n_loc = n_exp // n_groups
    smem = pl.BlockSpec(memory_space=pltpu.SMEM)
    whole = pl.BlockSpec((hid, hid), lambda i: (0, 0))
    flat = [w for group in weights for w in group]
    return pl.pallas_call(
        functools.partial(fwd_kernel, n_blocks=n_blocks, top_k=top_k, n_exp=n_exp, n_groups=n_groups, rows=rows),
        grid=(2 * n_blocks + 1,),
        in_specs=[smem, smem, smem, smem, pl.BlockSpec((BT, hid), lambda i: (jnp.minimum(i, n_blocks - 1), 0)), whole, whole]
        + [pl.BlockSpec(memory_space=pl.ANY)] * len(flat),
        out_specs=pl.BlockSpec((BT, hid), lambda i: (jnp.maximum(i - n_blocks - 1, 0), 0)),
        out_shape=jax.ShapeDtypeStruct((n_tok, hid), BF16),
        scratch_shapes=[
            pltpu.VMEM((2 * rows + 8, hid // 2), F32),
            pltpu.VMEM((2 * BT, hid // 2), F32),
            pltpu.VMEM((n_tok, hid), BF16),
            pltpu.VMEM((len(flat), n_loc, hid, hid), BF16),
            pltpu.SemaphoreType.DMA((len(flat),)),
        ],
        compiler_params=pltpu.CompilerParams(vmem_limit_bytes=VMEM_LIMIT),
        cost_estimate=pl.CostEstimate(flops=80_000_000_000, bytes_accessed=30_000_000, transcendentals=0),
        name="fwd",
    )(firsts, pos, gates, tab, x, w1, w2, *flat)


def solution(mesh):
    stages = mesh.shape["pp"]
    ep_size = mesh.shape["ep"]
    next_perm = [(i, (i + 1) % stages) for i in range(stages)]
    prev_perm = [(i, (i - 1) % stages) for i in range(stages)]
    mate_perm = [(i, i ^ 1) for i in range(ep_size)]
    chip_perm = [(i, i ^ 2) for i in range(ep_size)]
    tok_spec = P("pp", "ep", None)
    dense_spec = P("pp", None, None)
    expert_spec = P("pp", "ep", None, None)

    def mate(a):
        return lax.ppermute(a, "ep", mate_perm)

    def chip(a):
        return lax.ppermute(a, "ep", chip_perm)

    def device_step(x_fwd, ids_fwd, slots_fwd, gates_fwd, x_saved, grad_in, ids_bwd, slots_bwd, gates_bwd, w_one, w_two, w_gate, w_up, w_down):
        x_fwd, ids_fwd, slots_fwd, gates_fwd = x_fwd[0], ids_fwd[0], slots_fwd[0], gates_fwd[0]
        x_saved, grad_in, ids_bwd, slots_bwd, gates_bwd = x_saved[0], grad_in[0], ids_bwd[0], slots_bwd[0], gates_bwd[0]
        w1, w2, w_gate, w_up, w_down = w_one[0], w_two[0], w_gate[0], w_up[0], w_down[0]
        top_k = ids_fwd.shape[1]
        n_loc = w_gate.shape[0]
        n_exp = n_loc * ep_size
        rows = TM * (ids_fwd.size // TM + n_exp)
        me = lax.axis_index("ep")

        own = (w_gate, w_up, w_down)
        far = tuple(chip(w) for w in own)
        near = tuple(mate(w) for w in own)
        far_near = tuple(mate(w) for w in far)
        weights = (own, near, far, far_near)
        firsts = [(me ^ g) * n_loc for g in range(ep_size)]

        pos_b, tab_b = route_ranks(ids_bwd, slots_bwd, n_exp, rows)
        pos_f, tab_f = route_ranks(ids_fwd, slots_fwd, n_exp, rows)
        gates_b = gates_bwd.T.reshape(-1).astype(F32)
        gates_f = gates_fwd.T.reshape(-1).astype(F32)

        h_bwd, xs, qs = pre_bwd(pos_b, gates_b, tab_b, x_saved, grad_in, w1, w2, rows, n_exp, top_k)
        parts = [None] * ep_size
        for g in (0, 3, 2):
            xs, *parts[g] = exp_bwd(firsts[g].reshape(1), tab_b, *weights[g], xs, qs)
        sums = [parts[2][i] + mate(parts[3][i]) for i in range(3)]
        xs, *sums = lax.optimization_barrier((xs, *sums))
        there = [chip(v) for v in sums]
        xs, *parts[1] = exp_bwd(firsts[1].reshape(1), tab_b, *weights[1], xs, qs)
        grad_x = post_bwd(pos_b, tab_b, x_saved, grad_in, h_bwd, w1, w2, xs, n_exp, top_k)
        x_fwd, grad_x = lax.optimization_barrier((x_fwd, grad_x))
        dx_prev = lax.ppermute(grad_x[None], "pp", prev_perm)
        dws = [parts[0][i] + mate(parts[1][i]) + there[i] for i in range(3)]
        y_out = fwd(jnp.stack(firsts), pos_f, gates_f, tab_f, x_fwd, w1, w2, weights, rows, n_exp, top_k)
        y_next = lax.ppermute(y_out[None], "pp", next_perm)
        return y_next, dx_prev, dws[0][None], dws[1][None], dws[2][None]

    in_specs = (tok_spec,) * 9 + (dense_spec, dense_spec, expert_spec, expert_spec, expert_spec)
    out_specs = (tok_spec, tok_spec, expert_spec, expert_spec, expert_spec)
    return jax.shard_map(device_step, mesh=mesh, in_specs=in_specs, out_specs=out_specs, check_vma=False)
```

```python
import functools

import jax
import jax.numpy as jnp
from jax import lax
from jax.experimental import pallas as pl
from jax.experimental.pallas import tpu as pltpu
from jax.sharding import PartitionSpec as P


NORM_EPS = 1e-6
TM = 256
BT = 512
DEPTH = 4
F32 = jnp.float32
BF16 = jnp.bfloat16
VMEM_LIMIT = 60 * 1024 * 1024


def dot(a, b):
    return jnp.dot(a, b, preferred_element_type=F32)


def dot_nt(a, b):
    return lax.dot_general(a, b, (((1,), (1,)), ((), ())), preferred_element_type=F32)


def dot_tn(a, b):
    return lax.dot_general(a, b, (((0,), (0,)), ((), ())), preferred_element_type=F32)


def rms_scale(v):
    return lax.rsqrt(jnp.mean(v * v, axis=-1, keepdims=True) + NORM_EPS)


def rms_back(v, dy):
    r = rms_scale(v)
    return r * dy - v * (r * r * r * jnp.mean(dy * v, axis=-1, keepdims=True))


def dense_forward(xf, w1, w2):
    u = dot((xf * rms_scale(xf)).astype(BF16), w1)
    act = (u * jax.nn.sigmoid(u)).astype(BF16)
    return (xf + dot(act, w2)).astype(BF16)


def rank_kernel(n_exp, dump, scales, ids_ref, slots_ref, tab_ref, *pos_refs):
    ids = jnp.where(slots_ref[...] >= 0, ids_ref[...], -1)
    n = ids.shape[1]
    row = lax.broadcasted_iota(jnp.int32, (n, n), 0)
    col = lax.broadcasted_iota(jnp.int32, (n, n), 1)
    ones = jnp.ones((n, n), BF16)
    right = jnp.concatenate([jnp.where(row < col, 1.0, 0.0).astype(BF16), ones], axis=1)
    left = jnp.concatenate([jnp.where(col < row, 1.0, 0.0).astype(BF16), ones], axis=0)
    start = jnp.zeros((8, n), F32)
    pos = jnp.full((n, n), float(dump), F32)
    tab_ref[...] = jnp.zeros_like(tab_ref)
    for e in range(n_exp):
        mask = ids == e
        both = dot(jnp.where(mask, 1.0, 0.0).astype(BF16), right)
        pre = dot(left, both[:, n:].astype(BF16))
        pos = jnp.where(mask, both[:, :n] + pre[:n] + start[0:1], pos)
        tab_ref[e : e + 1, :] = (start[0:1] * (1.0 / TM)).astype(jnp.int32)
        count = pre[n : n + 8]
        start = start + TM * jnp.maximum(jnp.floor((count + (TM - 1.0)) * (1.0 / TM)), 1.0)
    tab_ref[n_exp : n_exp + 1, :] = (start[0:1] * (1.0 / TM)).astype(jnp.int32)
    for pos_ref, scale in zip(pos_refs, scales):
        pos_ref[...] = (pos * float(scale)).astype(jnp.int32)


def by_block(a):
    n_tok, top_k = a.shape
    return a.T.reshape(top_k, n_tok // BT, BT).swapaxes(0, 1)


def route_ranks(ids, slots, n_exp, rows, scales):
    lanes = 128
    flat = (ids.size // lanes, lanes)
    tab, *pos = pl.pallas_call(
        functools.partial(rank_kernel, n_exp, rows, scales),
        out_shape=(jax.ShapeDtypeStruct((n_exp + 8, lanes), jnp.int32),) + (jax.ShapeDtypeStruct(flat, jnp.int32),) * len(scales),
        name="rank",
    )(by_block(ids).reshape(flat), by_block(slots).reshape(flat))
    return (tab[:, 0], *[p.reshape(-1) for p in pos])


def put_rows(ref, at, vals, pitch=2, off=0):
    n = vals.shape[0]
    half = vals.shape[1] // 2
    ref[pl.ds(at + off, n, stride=pitch), :] = vals[:, :half]
    ref[pl.ds(at + off + 1, n, stride=pitch), :] = vals[:, half:]


def get_rows(ref, at, n, pitch=2, off=0):
    return jnp.concatenate([ref[pl.ds(at + off + i, n, stride=pitch), :] for i in range(2)], axis=1)


def rows_at(p, n):
    return pl.ds(pl.multiple_of(p, n), n)


def gather_rows(buf, acc, pos_ref, top_k):
    unroll = 8

    def body(j, c):
        base = j * unroll
        at = pl.multiple_of(j * (2 * unroll), 2 * unroll)
        for k in range(unroll):
            for r in range(top_k):
                acc[r, pl.ds(at + 2 * k, 2), :] = buf[rows_at(pos_ref[base + (r * BT + k)], 2), :]
        return c

    lax.fori_loop(0, BT // unroll, body, 0)


def scatter_rows(src, buf, pos_ref, top_k, n, shared):
    unroll = 8

    def body(j, c):
        base = j * unroll
        at = pl.multiple_of(j * (n * unroll), n * unroll)
        for k in range(unroll):
            v = src[pl.ds(at + n * k, n), :] if shared else None
            for r in range(top_k):
                row = v if shared else src[r, pl.ds(at + n * k, n), :]
                buf[rows_at(pos_ref[base + (r * BT + k)], n), :] = row
        return c

    lax.fori_loop(0, BT // unroll, body, 0)


def zero_tails(buf, tab_ref, n_exp, pitch):
    def body(e, c):
        at = pl.multiple_of((tab_ref[e + 1] - 1) * (pitch * TM), pitch * TM)
        buf[pl.ds(at, pitch * TM), :] = jnp.zeros((pitch * TM, buf.shape[1]), F32)
        return c

    lax.fori_loop(0, n_exp, body, 0)


def pre_bwd_kernel(pos_ref, tab_ref, gate_ref, x_ref, g_ref, w1_ref, w2_ref, h_ref, xs_hbm, qs_hbm, buf, src, xst, qst, sems, *, n_blocks, top_k, n_exp):
    step = pl.program_id(0)

    @pl.when(step == 0)
    def _():
        zero_tails(buf, tab_ref, n_exp, 4)

    h = dense_forward(x_ref[...].astype(F32), w1_ref[...], w2_ref[...])
    h_ref[...] = h
    hf = h.astype(F32)
    n = (hf * rms_scale(hf)).astype(BF16).astype(F32)
    g = g_ref[...].astype(F32)
    gates = gate_ref[...].T
    for r in range(top_k):
        put_rows(src.at[r], 0, n, 4, 0)
        put_rows(src.at[r], 0, g * gates[:, r : r + 1], 4, 2)
    scatter_rows(src, buf, pos_ref, top_k, 4, False)

    @pl.when(step == n_blocks - 1)
    def _():
        n_tiles = tab_ref[n_exp]

        def copies(t, slot):
            rows = pl.ds(pl.multiple_of(t * TM, TM), TM)
            return (
                pltpu.make_async_copy(xst.at[slot], xs_hbm.at[rows], sems.at[0, slot]),
                pltpu.make_async_copy(qst.at[slot], qs_hbm.at[rows], sems.at[1, slot]),
            )

        def convert(t, c):
            slot = lax.rem(t, DEPTH)

            @pl.when(t >= DEPTH)
            def _():
                for cp in copies(t - DEPTH, slot):
                    cp.wait()

            rows = pl.multiple_of(t * (4 * TM), 4 * TM)
            xst[slot] = get_rows(buf, rows, TM, 4, 0).astype(BF16)
            qst[slot] = get_rows(buf, rows, TM, 4, 2).astype(BF16)
            for cp in copies(t, slot):
                cp.start()
            return c

        lax.fori_loop(0, n_tiles, convert, 0)
        for back in range(DEPTH, 0, -1):
            for cp in copies(n_tiles - back, lax.rem(n_tiles - back, DEPTH)):
                cp.wait()


def route_spec(top_k, n_blocks, first=0):
    return pl.BlockSpec((top_k * BT,), lambda i: (jnp.clip(i - first, 0, n_blocks - 1),), memory_space=pltpu.SMEM)


def gate_spec(top_k, n_blocks, first=0):
    return pl.BlockSpec((top_k, BT), lambda i: (0, jnp.clip(i - first, 0, n_blocks - 1)))


def pre_bwd(pos, tab, gates, x, g, w1, w2, rows, n_exp, top_k):
    n_tok, hid = x.shape
    n_blocks = n_tok // BT
    smem = pl.BlockSpec(memory_space=pltpu.SMEM)
    blk = pl.BlockSpec((BT, hid), lambda i: (i, 0))
    whole = pl.BlockSpec((hid, hid), lambda i: (0, 0))
    return pl.pallas_call(
        functools.partial(pre_bwd_kernel, n_blocks=n_blocks, top_k=top_k, n_exp=n_exp),
        grid=(n_blocks,),
        in_specs=[route_spec(top_k, n_blocks), smem, gate_spec(top_k, n_blocks), blk, blk, whole, whole],
        out_specs=[blk, pl.BlockSpec(memory_space=pl.ANY), pl.BlockSpec(memory_space=pl.ANY)],
        out_shape=(
            jax.ShapeDtypeStruct((n_tok, hid), BF16),
            jax.ShapeDtypeStruct((rows, hid), BF16),
            jax.ShapeDtypeStruct((rows, hid), BF16),
        ),
        scratch_shapes=[
            pltpu.VMEM((4 * rows + 8, hid // 2), F32),
            pltpu.VMEM((top_k, 4 * BT, hid // 2), F32),
            pltpu.VMEM((DEPTH, TM, hid), BF16),
            pltpu.VMEM((DEPTH, TM, hid), BF16),
            pltpu.SemaphoreType.DMA((2, DEPTH)),
        ],
        compiler_params=pltpu.CompilerParams(vmem_limit_bytes=VMEM_LIMIT),
        cost_estimate=pl.CostEstimate(flops=30_000_000_000, bytes_accessed=30_000_000, transcendentals=0),
        name="pre_bwd",
    )(pos, tab, gates, x, g, w1, w2)


def exp_bwd_kernel(first_ref, tab_ref, wg_hbm, wu_hbm, wd_hbm, xs_hbm, qs_hbm, rs_hbm, dwg_hbm, dwu_hbm, dwd_hbm, wb, dwb, xb, qb, rb, sems, wsems, dsems, *, n_loc):
    first = first_ref[0]
    begin = tab_ref[first]
    end = tab_ref[first + n_loc]
    w_hbm = (wg_hbm, wu_hbm, wd_hbm)
    dw_hbm = (dwg_hbm, dwu_hbm, dwd_hbm)

    def rows_of(t):
        return pl.ds(pl.multiple_of(t * TM, TM), TM)

    def loads(t):
        slot = lax.rem(t, DEPTH)
        return (
            pltpu.make_async_copy(xs_hbm.at[rows_of(t)], xb.at[slot], sems.at[0, slot]),
            pltpu.make_async_copy(qs_hbm.at[rows_of(t)], qb.at[slot], sems.at[1, slot]),
        )

    def save(t):
        slot = lax.rem(t, DEPTH)
        return pltpu.make_async_copy(rb.at[slot], rs_hbm.at[rows_of(t)], sems.at[2, slot])

    def w_loads(e):
        slot = lax.rem(e, 2)
        return [pltpu.make_async_copy(w_hbm[i].at[e], wb.at[slot, i], wsems.at[i, slot]) for i in range(3)]

    def dw_saves(e):
        slot = lax.rem(e, 2)
        return [pltpu.make_async_copy(dwb.at[slot, i], dw_hbm[i].at[e], dsems.at[i, slot]) for i in range(3)]

    for cp in w_loads(0):
        cp.start()
    for ahead in range(DEPTH - 1):
        for cp in loads(begin + ahead):
            cp.start()

    def expert(e, c):
        wslot = lax.rem(e, 2)
        for cp in w_loads(e):
            cp.wait()

        @pl.when(e + 1 < n_loc)
        def _():
            for cp in w_loads(e + 1):
                cp.start()

        @pl.when(e >= 2)
        def _():
            for cp in dw_saves(e - 2):
                cp.wait()

        dwb[wslot] = jnp.zeros(dwb.shape[1:], F32)

        def body(t, c):
            slot = lax.rem(t, DEPTH)

            @pl.when(t + (DEPTH - 1) < end)
            def _():
                for cp in loads(t + (DEPTH - 1)):
                    cp.start()

            for cp in loads(t):
                cp.wait()

            @pl.when(t >= begin + DEPTH)
            def _():
                save(t - DEPTH).wait()

            x = xb[slot]
            q = qb[slot]
            wg, wu, wd = wb[wslot, 0], wb[wslot, 1], wb[wslot, 2]
            pre = dot(x, wg)
            up = dot(x, wu)
            sig = jax.nn.sigmoid(pre)
            sil = pre * sig
            act = (sil * up).astype(BF16)
            dwb[wslot, 2] += dot_tn(act, q)
            da = dot_nt(q, wd).astype(BF16).astype(F32)
            dpre = (da * up * (sig * (1.0 + pre * (1.0 - sig)))).astype(BF16)
            dup = (da * sil).astype(BF16)
            dwb[wslot, 0] += dot_tn(x, dpre)
            dwb[wslot, 1] += dot_tn(x, dup)
            rb[slot] = (dot_nt(dpre, wg) + dot_nt(dup, wu)).astype(BF16)
            save(t).start()
            return c

        lax.fori_loop(tab_ref[first + e], tab_ref[first + e + 1], body, 0)
        for cp in dw_saves(e):
            cp.start()
        return c

    lax.fori_loop(0, n_loc, expert, 0)
    for back in range(DEPTH, 0, -1):
        save(end - back).wait()
    for e in (n_loc - 2, n_loc - 1):
        for cp in dw_saves(e):
            cp.wait()


def exp_bwd(first, tab, wg, wu, wd, xs, qs):
    n_loc, hid, ff = wg.shape
    smem = pl.BlockSpec(memory_space=pltpu.SMEM)
    hbm = pl.BlockSpec(memory_space=pl.ANY)
    dw = jax.ShapeDtypeStruct((n_loc, hid, ff), F32)
    return pl.pallas_call(
        functools.partial(exp_bwd_kernel, n_loc=n_loc),
        in_specs=[smem, smem, hbm, hbm, hbm, hbm, hbm],
        out_specs=[hbm, hbm, hbm, hbm],
        out_shape=(jax.ShapeDtypeStruct(xs.shape, BF16), dw, dw, dw),
        input_output_aliases={5: 0},
        scratch_shapes=[
            pltpu.VMEM((2, 3, hid, ff), BF16),
            pltpu.VMEM((2, 3, hid, ff), F32),
            pltpu.VMEM((DEPTH, TM, hid), BF16),
            pltpu.VMEM((DEPTH, TM, hid), BF16),
            pltpu.VMEM((DEPTH, TM, hid), BF16),
            pltpu.SemaphoreType.DMA((3, DEPTH)),
            pltpu.SemaphoreType.DMA((3, 2)),
            pltpu.SemaphoreType.DMA((3, 2)),
        ],
        compiler_params=pltpu.CompilerParams(vmem_limit_bytes=VMEM_LIMIT),
        cost_estimate=pl.CostEstimate(flops=8_000_000_000, bytes_accessed=20_000_000, transcendentals=0),
        name="exp_bwd",
    )(first, tab, wg, wu, wd, xs, qs)


def post_bwd_kernel(pos_ref, tab_ref, x_ref, g_ref, h_ref, w1_ref, w2_ref, rs_hbm, dx_ref, rbuf, acc, st, sems, *, n_blocks, top_k, n_exp, rows):
    @pl.when(pl.program_id(0) == 0)
    def _():
        n_tiles = tab_ref[n_exp]

        def load(t):
            slot = lax.rem(t, DEPTH)
            return pltpu.make_async_copy(rs_hbm.at[pl.ds(pl.multiple_of(t * TM, TM), TM)], st.at[slot], sems.at[slot])

        for ahead in range(DEPTH - 1):
            load(ahead).start()
        rbuf[2 * rows : 2 * rows + 8, :] = jnp.zeros((8, rbuf.shape[1]), F32)

        def expand(t, c):
            @pl.when(t + (DEPTH - 1) < n_tiles)
            def _():
                load(t + (DEPTH - 1)).start()

            load(t).wait()
            put_rows(rbuf, pl.multiple_of(t * (2 * TM), 2 * TM), st[lax.rem(t, DEPTH)].astype(F32))
            return c

        lax.fori_loop(0, n_tiles, expand, 0)

    gather_rows(rbuf, acc, pos_ref, top_k)
    dn = get_rows(acc.at[0], 0, BT)
    for r in range(1, top_k):
        dn = dn + get_rows(acc.at[r], 0, BT)
    xf = x_ref[...].astype(F32)
    u = dot((xf * rms_scale(xf)).astype(BF16), w1_ref[...])
    dh = g_ref[...].astype(F32) + rms_back(h_ref[...].astype(F32), dn)
    sig = jax.nn.sigmoid(u)
    du = (dot_nt(dh.astype(BF16), w2_ref[...]) * (sig * (1.0 + u * (1.0 - sig)))).astype(BF16)
    dx_ref[...] = (dh + rms_back(xf, dot_nt(du, w1_ref[...]))).astype(BF16)


def post_bwd(pos, tab, x, g, h, w1, w2, rs, n_exp, top_k):
    n_tok, hid = x.shape
    rows = rs.shape[0]
    n_blocks = n_tok // BT
    smem = pl.BlockSpec(memory_space=pltpu.SMEM)
    blk = pl.BlockSpec((BT, hid), lambda i: (i, 0))
    whole = pl.BlockSpec((hid, hid), lambda i: (0, 0))
    return pl.pallas_call(
        functools.partial(post_bwd_kernel, n_blocks=n_blocks, top_k=top_k, n_exp=n_exp, rows=rows),
        grid=(n_blocks,),
        in_specs=[route_spec(top_k, n_blocks), smem, blk, blk, blk, whole, whole, pl.BlockSpec(memory_space=pl.ANY)],
        out_specs=blk,
        out_shape=jax.ShapeDtypeStruct((n_tok, hid), BF16),
        scratch_shapes=[
            pltpu.VMEM((2 * rows + 8, hid // 2), F32),
            pltpu.VMEM((top_k, 2 * BT, hid // 2), F32),
            pltpu.VMEM((DEPTH, TM, hid), BF16),
            pltpu.SemaphoreType.DMA((DEPTH,)),
        ],
        compiler_params=pltpu.CompilerParams(vmem_limit_bytes=VMEM_LIMIT),
        cost_estimate=pl.CostEstimate(flops=30_000_000_000, bytes_accessed=30_000_000, transcendentals=0),
        name="post_bwd",
    )(pos, tab, x, g, h, w1, w2, rs)


def fwd_kernel(firsts_ref, tab_ref, pos_ref, pos_out_ref, gate_ref, x_ref, w1_ref, w2_ref, *rest, n_blocks, top_k, n_exp, n_groups, rows):
    w_hbm = rest[: 3 * n_groups]
    y_ref, buf, acc, hsc, wsc, sems = rest[3 * n_groups :]
    nsc = acc.at[0]
    step = pl.program_id(0)
    n_loc = n_exp // n_groups

    def w_copy(i):
        return pltpu.make_async_copy(w_hbm[i], wsc.at[i], sems.at[i])

    @pl.when(step == 0)
    def _():
        for i in range(3 * n_groups):
            w_copy(i).start()
        zero_tails(buf, tab_ref, n_exp, 2)

    @pl.when(step < n_blocks)
    def _():
        h = dense_forward(x_ref[...].astype(F32), w1_ref[...], w2_ref[...])
        base = step * BT
        hsc[pl.ds(pl.multiple_of(base, BT), BT), :] = h
        hf = h.astype(F32)
        put_rows(nsc, 0, (hf * rms_scale(hf)).astype(BF16).astype(F32))

        scatter_rows(nsc, buf, pos_ref, top_k, 2, True)

    @pl.when(step == n_blocks)
    def _():
        buf[2 * rows : 2 * rows + 8, :] = jnp.zeros((8, buf.shape[1]), F32)
        for g in range(n_groups):
            for i in range(3):
                w_copy(3 * g + i).wait()
            first = firsts_ref[g]

            def body(t, e):
                e = jnp.where(t >= tab_ref[first + e + 1], e + 1, e)
                at = pl.multiple_of(t * (2 * TM), 2 * TM)
                x = get_rows(buf, at, TM).astype(BF16)
                pre = dot(x, wsc[3 * g, e])
                up = dot(x, wsc[3 * g + 1, e])
                act = (pre * jax.nn.sigmoid(pre) * up).astype(BF16)
                put_rows(buf, at, dot(act, wsc[3 * g + 2, e]).astype(BF16).astype(F32))
                return e

            lax.fori_loop(tab_ref[first], tab_ref[first + n_loc], body, 0)

    @pl.when(step > n_blocks)
    def _():
        base = (step - n_blocks - 1) * BT

        gather_rows(buf, acc, pos_out_ref, top_k)
        gates = gate_ref[...].T
        h = hsc[pl.ds(pl.multiple_of(base, BT), BT), :]
        mix = get_rows(acc.at[0], 0, BT) * gates[:, 0:1]
        for r in range(1, top_k):
            mix = mix + get_rows(acc.at[r], 0, BT) * gates[:, r : r + 1]
        y_ref[...] = (h.astype(F32) + mix).astype(BF16)


def fwd(firsts, tab, pos, gates, x, w1, w2, weights, rows, n_exp, top_k):
    n_tok, hid = x.shape
    n_blocks = n_tok // BT
    n_groups = len(weights)
    n_loc = n_exp // n_groups
    smem = pl.BlockSpec(memory_space=pltpu.SMEM)
    whole = pl.BlockSpec((hid, hid), lambda i: (0, 0))
    flat = [w for group in weights for w in group]
    return pl.pallas_call(
        functools.partial(fwd_kernel, n_blocks=n_blocks, top_k=top_k, n_exp=n_exp, n_groups=n_groups, rows=rows),
        grid=(2 * n_blocks + 1,),
        in_specs=[smem, smem, route_spec(top_k, n_blocks), route_spec(top_k, n_blocks, n_blocks + 1), gate_spec(top_k, n_blocks, n_blocks + 1)]
        + [pl.BlockSpec((BT, hid), lambda i: (jnp.minimum(i, n_blocks - 1), 0)), whole, whole]
        + [pl.BlockSpec(memory_space=pl.ANY)] * len(flat),
        out_specs=pl.BlockSpec((BT, hid), lambda i: (jnp.maximum(i - n_blocks - 1, 0), 0)),
        out_shape=jax.ShapeDtypeStruct((n_tok, hid), BF16),
        scratch_shapes=[
            pltpu.VMEM((2 * rows + 8, hid // 2), F32),
            pltpu.VMEM((top_k, 2 * BT, hid // 2), F32),
            pltpu.VMEM((n_tok, hid), BF16),
            pltpu.VMEM((len(flat), n_loc, hid, hid), BF16),
            pltpu.SemaphoreType.DMA((len(flat),)),
        ],
        compiler_params=pltpu.CompilerParams(vmem_limit_bytes=VMEM_LIMIT),
        cost_estimate=pl.CostEstimate(flops=80_000_000_000, bytes_accessed=30_000_000, transcendentals=0),
        name="fwd",
    )(firsts, tab, pos, pos, gates, x, w1, w2, *flat)


def solution(mesh):
    stages = mesh.shape["pp"]
    ep_size = mesh.shape["ep"]
    next_perm = [(i, (i + 1) % stages) for i in range(stages)]
    prev_perm = [(i, (i - 1) % stages) for i in range(stages)]
    mate_perm = [(i, i ^ 1) for i in range(ep_size)]
    chip_perm = [(i, i ^ 2) for i in range(ep_size)]
    tok_spec = P("pp", "ep", None)
    dense_spec = P("pp", None, None)
    expert_spec = P("pp", "ep", None, None)

    def mate(a):
        return lax.ppermute(a, "ep", mate_perm)

    def chip(a):
        return lax.ppermute(a, "ep", chip_perm)

    def slot(x_fwd, ids_fwd, slots_fwd, gates_fwd, x_saved, grad_in, ids_bwd, slots_bwd, gates_bwd, w_one, w_two, w_gate, w_up, w_down):
        x_fwd, ids_fwd, slots_fwd, gates_fwd = x_fwd[0], ids_fwd[0], slots_fwd[0], gates_fwd[0]
        x_saved, grad_in, ids_bwd, slots_bwd, gates_bwd = x_saved[0], grad_in[0], ids_bwd[0], slots_bwd[0], gates_bwd[0]
        w1, w2, w_gate, w_up, w_down = w_one[0], w_two[0], w_gate[0], w_up[0], w_down[0]
        top_k = ids_fwd.shape[1]
        n_loc = w_gate.shape[0]
        n_exp = n_loc * ep_size
        rows = TM * (ids_fwd.size // TM + n_exp)
        me = lax.axis_index("ep")

        own = (w_gate, w_up, w_down)
        far = tuple(chip(w) for w in own)
        near = tuple(mate(w) for w in own)
        far_near = tuple(mate(w) for w in far)
        weights = (own, near, far, far_near)
        firsts = [(me ^ g) * n_loc for g in range(ep_size)]

        tab_b, pos4_b, pos2_b = route_ranks(ids_bwd, slots_bwd, n_exp, rows, (4, 2))
        tab_f, pos2_f = route_ranks(ids_fwd, slots_fwd, n_exp, rows, (2,))
        gates_b = gates_bwd.T.astype(F32)
        gates_f = gates_fwd.T.astype(F32)

        h_bwd, xs, qs = pre_bwd(pos4_b, tab_b, gates_b, x_saved, grad_in, w1, w2, rows, n_exp, top_k)
        parts = [None] * ep_size
        for g in (0, 3, 2, 1):
            xs, *parts[g] = exp_bwd(firsts[g].reshape(1), tab_b, *weights[g], xs, qs)
        sums = [parts[2][i] + mate(parts[3][i]) for i in range(3)]
        there = [chip(v) for v in sums]
        grad_x = post_bwd(pos2_b, tab_b, x_saved, grad_in, h_bwd, w1, w2, xs, n_exp, top_k)
        x_fwd, grad_x = lax.optimization_barrier((x_fwd, grad_x))
        dx_prev = lax.ppermute(grad_x[None], "pp", prev_perm)
        dws = [parts[0][i] + mate(parts[1][i]) + there[i] for i in range(3)]

        y_out = fwd(jnp.stack(firsts), tab_f, pos2_f, gates_f, x_fwd, w1, w2, weights, rows, n_exp, top_k)
        y_next = lax.ppermute(y_out[None], "pp", next_perm)
        return y_next, dx_prev, dws[0][None], dws[1][None], dws[2][None]

    in_specs = (tok_spec,) * 9 + (dense_spec, dense_spec, expert_spec, expert_spec, expert_spec)
    out_specs = (tok_spec, tok_spec, expert_spec, expert_spec, expert_spec)
    return jax.shard_map(slot, mesh=mesh, in_specs=in_specs, out_specs=out_specs, check_vma=False)
```

```python
import functools

import jax
import jax.numpy as jnp
from jax import lax
from jax.experimental import pallas as pl
from jax.experimental.pallas import tpu as pltpu
from jax.sharding import PartitionSpec as P


NORM_EPS = 1e-6
TM = 256
BT = 512
DEPTH = 4
HALVES = 2
F32 = jnp.float32
BF16 = jnp.bfloat16
VMEM_LIMIT = 60 * 1024 * 1024


def dot(a, b):
    return jnp.dot(a, b, preferred_element_type=F32)


def dot_nt(a, b):
    return lax.dot_general(a, b, (((1,), (1,)), ((), ())), preferred_element_type=F32)


def dot_tn(a, b):
    return lax.dot_general(a, b, (((0,), (0,)), ((), ())), preferred_element_type=F32)


def rms_scale(v):
    return lax.rsqrt(jnp.mean(v * v, axis=-1, keepdims=True) + NORM_EPS)


def rms_back(v, dy):
    r = rms_scale(v)
    return r * dy - v * (r * r * r * jnp.mean(dy * v, axis=-1, keepdims=True))


def dense_forward(xf, w1, w2):
    u = dot((xf * rms_scale(xf)).astype(BF16), w1)
    act = (u * jax.nn.sigmoid(u)).astype(BF16)
    return (xf + dot(act, w2)).astype(BF16)


def rank_routes(ids, slots, n_exp, dump):
    ids = jnp.where(slots >= 0, ids, -1)
    n, lanes = ids.shape
    row = lax.broadcasted_iota(jnp.int32, (lanes, lanes), 0)
    col = lax.broadcasted_iota(jnp.int32, (lanes, lanes), 1)
    right = jnp.concatenate([jnp.where(row < col, 1.0, 0.0).astype(BF16), jnp.ones((lanes, lanes), BF16)], axis=1)
    row = lax.broadcasted_iota(jnp.int32, (n + 8, n), 0)
    col = lax.broadcasted_iota(jnp.int32, (n + 8, n), 1)
    left = jnp.where((col < row) | (row >= n), 1.0, 0.0).astype(BF16)
    lane = lax.broadcasted_iota(jnp.int32, (8, lanes), 1)
    start = jnp.zeros((8, lanes), F32)
    tab = jnp.zeros((8, lanes), F32)
    pos = jnp.full((n, lanes), float(dump), F32)
    for e in range(n_exp):
        mask = ids == e
        both = dot(jnp.where(mask, 1.0, 0.0).astype(BF16), right)
        pre = dot(left, both[:, lanes:].astype(BF16))
        pos = jnp.where(mask, both[:, :lanes] + pre[:n] + start[0:1], pos)
        tab = jnp.where(lane == e, start, tab)
        start = start + TM * jnp.maximum(jnp.floor((pre[n:] + (TM - 1.0)) * (1.0 / TM)), 1.0)
    tab = jnp.where(lane == n_exp, start, tab) * (1.0 / TM)
    return pos, tab.astype(jnp.int32)


def chunks(ref, first, last):
    return jnp.concatenate([ref[:, c * 128 : (c + 1) * 128] for c in range(first, last)], axis=0)


def rank_kernel(n_exp, rows_b, rows_f, ids_b, slots_b, ids_f, slots_f, tab_b, pos4_b, pos2_b, tab_f, pos2_f):
    n = ids_b.shape[1] // 128
    pos, tab_b[...] = rank_routes(chunks(ids_b, 0, n), chunks(slots_b, 0, n), n_exp, rows_b)
    pos4_b[...] = (pos * 4.0).astype(jnp.int32)
    pos2_b[...] = (pos * 2.0).astype(jnp.int32)
    step = n // HALVES
    for h in range(HALVES):
        at = (h * step, (h + 1) * step)
        pos, tab_f[h] = rank_routes(chunks(ids_f, *at), chunks(slots_f, *at), n_exp, rows_f)
        k = pos.shape[0]
        pos2_f[h * k : (h + 1) * k, :] = (pos * 2.0).astype(jnp.int32)


def route_ranks(ids_b, slots_b, ids_f, slots_f, n_exp, rows_b, rows_f):
    pos = jax.ShapeDtypeStruct((ids_b.size // 128, 128), jnp.int32)
    tab = (8, 128)
    tab_b, pos4_b, pos2_b, tab_f, pos2_f = pl.pallas_call(
        functools.partial(rank_kernel, n_exp, rows_b, rows_f),
        out_shape=(
            jax.ShapeDtypeStruct(tab, jnp.int32),
            pos,
            pos,
            jax.ShapeDtypeStruct((HALVES, *tab), jnp.int32),
            pos,
        ),
        name="rank",
    )(ids_b.T, slots_b.T, ids_f.T, slots_f.T)
    return tab_b, pos4_b.reshape(-1), pos2_b.reshape(-1), tab_f, pos2_f.reshape(-1)


def put_rows(ref, at, vals, pitch=2, off=0):
    n = vals.shape[0]
    half = vals.shape[1] // 2
    ref[pl.ds(at + off, n, stride=pitch), :] = vals[:, :half]
    ref[pl.ds(at + off + 1, n, stride=pitch), :] = vals[:, half:]


def get_rows(ref, at, n, pitch=2, off=0):
    return jnp.concatenate([ref[pl.ds(at + off + i, n, stride=pitch), :] for i in range(2)], axis=1)


def rows_at(p, n):
    return pl.ds(pl.multiple_of(p, n), n)


def table_at(j, unroll, top_k):
    per = 128 // unroll
    return lax.div(j, per) * (128 * top_k) + lax.rem(j, per) * unroll


def gather_rows(buf, acc, pos_ref, top_k):
    unroll = 16

    def body(j, c):
        base = table_at(j, unroll, top_k)
        at = pl.multiple_of(j * (2 * unroll), 2 * unroll)
        for k in range(unroll):
            for r in range(top_k):
                acc[r, pl.ds(at + 2 * k, 2), :] = buf[rows_at(pos_ref[base + (r * 128 + k)], 2), :]
        return c

    lax.fori_loop(0, BT // unroll, body, 0)


def scatter_rows(src, buf, pos_ref, top_k, n, shared):
    unroll = 16

    def body(j, c):
        base = table_at(j, unroll, top_k)
        at = pl.multiple_of(j * (n * unroll), n * unroll)
        for k in range(unroll):
            v = src[pl.ds(at + n * k, n), :] if shared else None
            for r in range(top_k):
                row = v if shared else src[r, pl.ds(at + n * k, n), :]
                buf[rows_at(pos_ref[base + (r * 128 + k)], n), :] = row
        return c

    lax.fori_loop(0, BT // unroll, body, 0)


def zero_tails(buf, tab_ref, n_exp, pitch):
    def body(e, c):
        at = pl.multiple_of((tab_ref[0, e + 1] - 1) * (pitch * TM), pitch * TM)
        buf[pl.ds(at, pitch * TM), :] = jnp.zeros((pitch * TM, buf.shape[1]), F32)
        return c

    lax.fori_loop(0, n_exp, body, 0)


def pre_bwd_kernel(pos_ref, tab_ref, gate_ref, x_ref, g_ref, w1_ref, w2_ref, h_ref, xs_hbm, qs_hbm, buf, src, xst, qst, sems, *, n_blocks, top_k, n_exp):
    step = pl.program_id(0)

    @pl.when(step == 0)
    def _():
        zero_tails(buf, tab_ref, n_exp, 4)

    h = dense_forward(x_ref[...].astype(F32), w1_ref[...], w2_ref[...])
    h_ref[...] = h
    hf = h.astype(F32)
    n = (hf * rms_scale(hf)).astype(BF16).astype(F32)
    g = g_ref[...].astype(F32)
    gates = gate_ref[...].astype(F32).T
    for r in range(top_k):
        put_rows(src.at[r], 0, n, 4, 0)
        put_rows(src.at[r], 0, g * gates[:, r : r + 1], 4, 2)
    scatter_rows(src, buf, pos_ref, top_k, 4, False)

    @pl.when(step == n_blocks - 1)
    def _():
        n_tiles = tab_ref[0, n_exp]

        def copies(t, slot):
            rows = pl.ds(pl.multiple_of(t * TM, TM), TM)
            return (
                pltpu.make_async_copy(xst.at[slot], xs_hbm.at[rows], sems.at[0, slot]),
                pltpu.make_async_copy(qst.at[slot], qs_hbm.at[rows], sems.at[1, slot]),
            )

        def convert(t, c):
            slot = lax.rem(t, DEPTH)

            @pl.when(t >= DEPTH)
            def _():
                for cp in copies(t - DEPTH, slot):
                    cp.wait()

            rows = pl.multiple_of(t * (4 * TM), 4 * TM)
            xst[slot] = get_rows(buf, rows, TM, 4, 0).astype(BF16)
            qst[slot] = get_rows(buf, rows, TM, 4, 2).astype(BF16)
            for cp in copies(t, slot):
                cp.start()
            return c

        lax.fori_loop(0, n_tiles, convert, 0)
        for back in range(DEPTH, 0, -1):
            for cp in copies(n_tiles - back, lax.rem(n_tiles - back, DEPTH)):
                cp.wait()


def route_spec(top_k, n_blocks, first=0, skip=0):
    return pl.BlockSpec((top_k * BT,), lambda i: (skip + jnp.clip(i - first, 0, n_blocks - 1),), memory_space=pltpu.SMEM)


def gate_spec(top_k, n_blocks, first=0, skip=0):
    return pl.BlockSpec((top_k, BT), lambda i: (0, skip + jnp.clip(i - first, 0, n_blocks - 1)))


def pre_bwd(pos, tab, gates, x, g, w1, w2, rows, n_exp, top_k):
    n_tok, hid = x.shape
    n_blocks = n_tok // BT
    smem = pl.BlockSpec(memory_space=pltpu.SMEM)
    blk = pl.BlockSpec((BT, hid), lambda i: (i, 0))
    whole = pl.BlockSpec((hid, hid), lambda i: (0, 0))
    return pl.pallas_call(
        functools.partial(pre_bwd_kernel, n_blocks=n_blocks, top_k=top_k, n_exp=n_exp),
        grid=(n_blocks,),
        in_specs=[route_spec(top_k, n_blocks), smem, gate_spec(top_k, n_blocks), blk, blk, whole, whole],
        out_specs=[blk, pl.BlockSpec(memory_space=pl.ANY), pl.BlockSpec(memory_space=pl.ANY)],
        out_shape=(
            jax.ShapeDtypeStruct((n_tok, hid), BF16),
            jax.ShapeDtypeStruct((rows, hid), BF16),
            jax.ShapeDtypeStruct((rows, hid), BF16),
        ),
        scratch_shapes=[
            pltpu.VMEM((4 * rows + 8, hid // 2), F32),
            pltpu.VMEM((top_k, 4 * BT, hid // 2), F32),
            pltpu.VMEM((DEPTH, TM, hid), BF16),
            pltpu.VMEM((DEPTH, TM, hid), BF16),
            pltpu.SemaphoreType.DMA((2, DEPTH)),
        ],
        compiler_params=pltpu.CompilerParams(vmem_limit_bytes=VMEM_LIMIT),
        cost_estimate=pl.CostEstimate(flops=30_000_000_000, bytes_accessed=30_000_000, transcendentals=0),
        name="pre_bwd",
    )(pos, tab, gates, x, g, w1, w2)


def exp_bwd_kernel(first_ref, tab_ref, *refs, n_loc, has_init):
    w_hbm, (xs_hbm, qs_hbm), refs = refs[:3], refs[3:5], refs[5:]
    init_hbm, refs = (refs[:3], refs[3:]) if has_init else ((), refs)
    rs_hbm, *dw_hbm, wb, dwb, xb, qb, rb, sems, wsems, dsems, isems = refs
    first = first_ref[0]
    begin = tab_ref[0, first]
    end = tab_ref[0, first + n_loc]

    def rows_of(t):
        return pl.ds(pl.multiple_of(t * TM, TM), TM)

    def loads(t):
        slot = lax.rem(t, DEPTH)
        return (
            pltpu.make_async_copy(xs_hbm.at[rows_of(t)], xb.at[slot], sems.at[0, slot]),
            pltpu.make_async_copy(qs_hbm.at[rows_of(t)], qb.at[slot], sems.at[1, slot]),
        )

    def save(t):
        slot = lax.rem(t, DEPTH)
        return pltpu.make_async_copy(rb.at[slot], rs_hbm.at[rows_of(t)], sems.at[2, slot])

    def w_loads(e):
        slot = lax.rem(e, 2)
        return [pltpu.make_async_copy(w_hbm[i].at[e], wb.at[slot, i], wsems.at[i, slot]) for i in range(3)]

    def init_loads(e):
        slot = lax.rem(e, 3)
        return [pltpu.make_async_copy(ref.at[e], dwb.at[slot, i], isems.at[i, slot]) for i, ref in enumerate(init_hbm)]

    def dw_saves(e):
        slot = lax.rem(e, 3)
        return [pltpu.make_async_copy(dwb.at[slot, i], dw_hbm[i].at[e], dsems.at[i, slot]) for i in range(3)]

    for cp in w_loads(0) + init_loads(0):
        cp.start()
    for ahead in range(DEPTH - 1):
        for cp in loads(begin + ahead):
            cp.start()

    def expert(e, c):
        wslot = lax.rem(e, 2)
        dslot = lax.rem(e, 3)
        for cp in w_loads(e) + init_loads(e):
            cp.wait()

        @pl.when(e >= 2)
        def _():
            for cp in dw_saves(e - 2):
                cp.wait()

        @pl.when(e + 1 < n_loc)
        def _():
            for cp in w_loads(e + 1) + init_loads(e + 1):
                cp.start()

        if not has_init:
            dwb[dslot] = jnp.zeros(dwb.shape[1:], F32)

        def body(t, c):
            slot = lax.rem(t, DEPTH)

            @pl.when(t + (DEPTH - 1) < end)
            def _():
                for cp in loads(t + (DEPTH - 1)):
                    cp.start()

            for cp in loads(t):
                cp.wait()

            @pl.when(t >= begin + DEPTH)
            def _():
                save(t - DEPTH).wait()

            x = xb[slot]
            q = qb[slot]
            wg, wu, wd = wb[wslot, 0], wb[wslot, 1], wb[wslot, 2]
            pre = dot(x, wg)
            up = dot(x, wu)
            sig = jax.nn.sigmoid(pre)
            sil = pre * sig
            act = (sil * up).astype(BF16)
            dwb[dslot, 2] += dot_tn(act, q)
            da = dot_nt(q, wd).astype(BF16).astype(F32)
            dpre = (da * up * (sig * (1.0 + pre * (1.0 - sig)))).astype(BF16)
            dup = (da * sil).astype(BF16)
            dwb[dslot, 0] += dot_tn(x, dpre)
            dwb[dslot, 1] += dot_tn(x, dup)
            rb[slot] = (dot_nt(dpre, wg) + dot_nt(dup, wu)).astype(BF16)
            save(t).start()
            return c

        lax.fori_loop(tab_ref[0, first + e], tab_ref[0, first + e + 1], body, 0)
        for cp in dw_saves(e):
            cp.start()
        return c

    lax.fori_loop(0, n_loc, expert, 0)
    for back in range(DEPTH, 0, -1):
        save(end - back).wait()
    for e in (n_loc - 2, n_loc - 1):
        for cp in dw_saves(e):
            cp.wait()


def exp_bwd(first, tab, wg, wu, wd, xs, qs, init=()):
    n_loc, hid, ff = wg.shape
    smem = pl.BlockSpec(memory_space=pltpu.SMEM)
    hbm = pl.BlockSpec(memory_space=pl.ANY)
    dw = jax.ShapeDtypeStruct((n_loc, hid, ff), F32)
    return pl.pallas_call(
        functools.partial(exp_bwd_kernel, n_loc=n_loc, has_init=bool(init)),
        in_specs=[smem, smem] + [hbm] * (5 + len(init)),
        out_specs=[hbm, hbm, hbm, hbm],
        out_shape=(jax.ShapeDtypeStruct(xs.shape, BF16), dw, dw, dw),
        input_output_aliases={5: 0},
        scratch_shapes=[
            pltpu.VMEM((2, 3, hid, ff), BF16),
            pltpu.VMEM((3, 3, hid, ff), F32),
            pltpu.VMEM((DEPTH, TM, hid), BF16),
            pltpu.VMEM((DEPTH, TM, hid), BF16),
            pltpu.VMEM((DEPTH, TM, hid), BF16),
            pltpu.SemaphoreType.DMA((3, DEPTH)),
            pltpu.SemaphoreType.DMA((3, 2)),
            pltpu.SemaphoreType.DMA((3, 3)),
            pltpu.SemaphoreType.DMA((3, 3)),
        ],
        compiler_params=pltpu.CompilerParams(vmem_limit_bytes=VMEM_LIMIT),
        cost_estimate=pl.CostEstimate(flops=8_000_000_000, bytes_accessed=20_000_000, transcendentals=0),
        name="exp_bwd",
    )(first, tab, wg, wu, wd, xs, qs, *init)


def post_bwd_kernel(pos_ref, tab_ref, x_ref, g_ref, h_ref, w1_ref, w2_ref, rs_hbm, dx_ref, rbuf, acc, st, sems, *, n_blocks, top_k, n_exp, rows):
    @pl.when(pl.program_id(0) == 0)
    def _():
        n_tiles = tab_ref[0, n_exp]

        def load(t):
            slot = lax.rem(t, DEPTH)
            return pltpu.make_async_copy(rs_hbm.at[pl.ds(pl.multiple_of(t * TM, TM), TM)], st.at[slot], sems.at[slot])

        for ahead in range(DEPTH - 1):
            load(ahead).start()
        rbuf[2 * rows : 2 * rows + 8, :] = jnp.zeros((8, rbuf.shape[1]), F32)

        def expand(t, c):
            @pl.when(t + (DEPTH - 1) < n_tiles)
            def _():
                load(t + (DEPTH - 1)).start()

            load(t).wait()
            put_rows(rbuf, pl.multiple_of(t * (2 * TM), 2 * TM), st[lax.rem(t, DEPTH)].astype(F32))
            return c

        lax.fori_loop(0, n_tiles, expand, 0)

    gather_rows(rbuf, acc, pos_ref, top_k)
    dn = get_rows(acc.at[0], 0, BT)
    for r in range(1, top_k):
        dn = dn + get_rows(acc.at[r], 0, BT)
    xf = x_ref[...].astype(F32)
    u = dot((xf * rms_scale(xf)).astype(BF16), w1_ref[...])
    dh = g_ref[...].astype(F32) + rms_back(h_ref[...].astype(F32), dn)
    sig = jax.nn.sigmoid(u)
    du = (dot_nt(dh.astype(BF16), w2_ref[...]) * (sig * (1.0 + u * (1.0 - sig)))).astype(BF16)
    dx_ref[...] = (dh + rms_back(xf, dot_nt(du, w1_ref[...]))).astype(BF16)


def post_bwd(pos, tab, x, g, h, w1, w2, rs, n_exp, top_k):
    n_tok, hid = x.shape
    rows = rs.shape[0]
    n_blocks = n_tok // BT
    smem = pl.BlockSpec(memory_space=pltpu.SMEM)
    blk = pl.BlockSpec((BT, hid), lambda i: (i, 0))
    whole = pl.BlockSpec((hid, hid), lambda i: (0, 0))
    return pl.pallas_call(
        functools.partial(post_bwd_kernel, n_blocks=n_blocks, top_k=top_k, n_exp=n_exp, rows=rows),
        grid=(n_blocks,),
        in_specs=[route_spec(top_k, n_blocks), smem, blk, blk, blk, whole, whole, pl.BlockSpec(memory_space=pl.ANY)],
        out_specs=blk,
        out_shape=jax.ShapeDtypeStruct((n_tok, hid), BF16),
        scratch_shapes=[
            pltpu.VMEM((2 * rows + 8, hid // 2), F32),
            pltpu.VMEM((top_k, 2 * BT, hid // 2), F32),
            pltpu.VMEM((DEPTH, TM, hid), BF16),
            pltpu.SemaphoreType.DMA((DEPTH,)),
        ],
        compiler_params=pltpu.CompilerParams(vmem_limit_bytes=VMEM_LIMIT),
        cost_estimate=pl.CostEstimate(flops=30_000_000_000, bytes_accessed=30_000_000, transcendentals=0),
        name="post_bwd",
    )(pos, tab, x, g, h, w1, w2, rs)


def fwd_kernel(firsts_ref, tab_ref, pos_ref, pos_out_ref, gate_ref, x_ref, w1_ref, w2_ref, *rest, n_blocks, top_k, n_exp, n_groups, rows):
    w_hbm = rest[: 3 * n_groups]
    y_ref, buf, acc, hsc, wsc, sems = rest[3 * n_groups :]
    nsc = acc.at[0]
    step = pl.program_id(0)
    n_loc = n_exp // n_groups

    def w_copy(i):
        return pltpu.make_async_copy(w_hbm[i], wsc.at[i], sems.at[i])

    @pl.when(step == 0)
    def _():
        for i in range(3 * n_groups):
            w_copy(i).start()
        zero_tails(buf, tab_ref, n_exp, 2)

    @pl.when(step < n_blocks)
    def _():
        h = dense_forward(x_ref[...].astype(F32), w1_ref[...], w2_ref[...])
        base = step * BT
        hsc[pl.ds(pl.multiple_of(base, BT), BT), :] = h
        hf = h.astype(F32)
        put_rows(nsc, 0, (hf * rms_scale(hf)).astype(BF16).astype(F32))

        scatter_rows(nsc, buf, pos_ref, top_k, 2, True)

    @pl.when(step == n_blocks)
    def _():
        buf[2 * rows : 2 * rows + 8, :] = jnp.zeros((8, buf.shape[1]), F32)
        for g in range(n_groups):
            for i in range(3):
                w_copy(3 * g + i).wait()
            first = firsts_ref[g]

            def body(t, e):
                e = jnp.where(t >= tab_ref[0, first + e + 1], e + 1, e)
                at = pl.multiple_of(t * (2 * TM), 2 * TM)
                x = get_rows(buf, at, TM).astype(BF16)
                pre = dot(x, wsc[3 * g, e])
                up = dot(x, wsc[3 * g + 1, e])
                act = (pre * jax.nn.sigmoid(pre) * up).astype(BF16)
                put_rows(buf, at, dot(act, wsc[3 * g + 2, e]).astype(BF16).astype(F32))
                return e

            lax.fori_loop(tab_ref[0, first], tab_ref[0, first + n_loc], body, 0)

    @pl.when(step > n_blocks)
    def _():
        base = (step - n_blocks - 1) * BT

        gather_rows(buf, acc, pos_out_ref, top_k)
        gates = gate_ref[...].astype(F32).T
        h = hsc[pl.ds(pl.multiple_of(base, BT), BT), :]
        mix = get_rows(acc.at[0], 0, BT) * gates[:, 0:1]
        for r in range(1, top_k):
            mix = mix + get_rows(acc.at[r], 0, BT) * gates[:, r : r + 1]
        y_ref[...] = (h.astype(F32) + mix).astype(BF16)


def fwd(half, firsts, tab, pos, gates, x, w1, w2, weights, rows, n_exp, top_k):
    n_tok, hid = x.shape[0] // HALVES, x.shape[1]
    n_blocks = n_tok // BT
    skip = half * n_blocks
    n_groups = len(weights)
    n_loc = n_exp // n_groups
    smem = pl.BlockSpec(memory_space=pltpu.SMEM)
    whole = pl.BlockSpec((hid, hid), lambda i: (0, 0))
    flat = [w for group in weights for w in group]
    return pl.pallas_call(
        functools.partial(fwd_kernel, n_blocks=n_blocks, top_k=top_k, n_exp=n_exp, n_groups=n_groups, rows=rows),
        grid=(2 * n_blocks + 1,),
        in_specs=[smem, smem, route_spec(top_k, n_blocks, 0, skip), route_spec(top_k, n_blocks, n_blocks + 1, skip), gate_spec(top_k, n_blocks, n_blocks + 1, skip)]
        + [pl.BlockSpec((BT, hid), lambda i: (skip + jnp.minimum(i, n_blocks - 1), 0)), whole, whole]
        + [pl.BlockSpec(memory_space=pl.ANY)] * len(flat),
        out_specs=pl.BlockSpec((BT, hid), lambda i: (jnp.maximum(i - n_blocks - 1, 0), 0)),
        out_shape=jax.ShapeDtypeStruct((n_tok, hid), BF16),
        scratch_shapes=[
            pltpu.VMEM((2 * rows + 8, hid // 2), F32),
            pltpu.VMEM((top_k, 2 * BT, hid // 2), F32),
            pltpu.VMEM((n_tok, hid), BF16),
            pltpu.VMEM((len(flat), n_loc, hid, hid), BF16),
            pltpu.SemaphoreType.DMA((len(flat),)),
        ],
        compiler_params=pltpu.CompilerParams(vmem_limit_bytes=VMEM_LIMIT),
        cost_estimate=pl.CostEstimate(flops=80_000_000_000, bytes_accessed=30_000_000, transcendentals=0),
        name="fwd",
    )(firsts, tab, pos, pos, gates, x, w1, w2, *flat)


def solution(mesh):
    stages = mesh.shape["pp"]
    ep_size = mesh.shape["ep"]
    next_perm = [(i, (i + 1) % stages) for i in range(stages)]
    prev_perm = [(i, (i - 1) % stages) for i in range(stages)]
    mate_perm = [(i, i ^ 1) for i in range(ep_size)]
    chip_perm = [(i, i ^ 2) for i in range(ep_size)]
    tok_spec = P("pp", "ep", None)
    dense_spec = P("pp", None, None)
    expert_spec = P("pp", "ep", None, None)

    def mate(a):
        return lax.ppermute(a, "ep", mate_perm)

    def chip(a):
        return lax.ppermute(a, "ep", chip_perm)

    def slot(x_fwd, ids_fwd, slots_fwd, gates_fwd, x_saved, grad_in, ids_bwd, slots_bwd, gates_bwd, w_one, w_two, w_gate, w_up, w_down):
        x_fwd, ids_fwd, slots_fwd, gates_fwd = x_fwd[0], ids_fwd[0], slots_fwd[0], gates_fwd[0]
        x_saved, grad_in, ids_bwd, slots_bwd, gates_bwd = x_saved[0], grad_in[0], ids_bwd[0], slots_bwd[0], gates_bwd[0]
        w1, w2, w_gate, w_up, w_down = w_one[0], w_two[0], w_gate[0], w_up[0], w_down[0]
        top_k = ids_fwd.shape[1]
        n_loc = w_gate.shape[0]
        n_exp = n_loc * ep_size
        rows = TM * (ids_fwd.size // TM + n_exp)
        rows_f = TM * (ids_fwd.size // HALVES // TM + n_exp)
        me = lax.axis_index("ep")

        own = (w_gate, w_up, w_down)
        far = tuple(chip(w) for w in own)
        near = tuple(mate(w) for w in own)
        far_near = tuple(mate(w) for w in far)
        weights = (own, near, far, far_near)
        firsts = [(me ^ g) * n_loc for g in range(ep_size)]

        tab_b, pos4_b, pos2_b, tab_f, pos2_f = route_ranks(ids_bwd, slots_bwd, ids_fwd, slots_fwd, n_exp, rows, rows_f)
        gates_b = gates_bwd.T
        gates_f = gates_fwd.T

        h_bwd, xs, qs = pre_bwd(pos4_b, tab_b, gates_b, x_saved, grad_in, w1, w2, rows, n_exp, top_k)

        def experts(g, xs, init=()):
            return exp_bwd(firsts[g].reshape(1), tab_b, *weights[g], xs, qs, init)

        xs, *part = experts(1, xs)
        near_sum = [mate(v) for v in part]
        xs, *part = experts(3, xs)
        far_sum = [mate(v) for v in part]
        xs, *dw_own = experts(0, xs, near_sum)
        xs, *part = experts(2, xs, far_sum)
        there = [chip(v) for v in part]
        grad_x = post_bwd(pos2_b, tab_b, x_saved, grad_in, h_bwd, w1, w2, xs, n_exp, top_k)
        x_fwd, grad_x = lax.optimization_barrier((x_fwd, grad_x))
        dx_prev = lax.ppermute(grad_x[None], "pp", prev_perm)

        halves = []
        first_stack = jnp.stack(firsts)
        for h in range(HALVES):
            y_half = fwd(h, first_stack, tab_f[h], pos2_f, gates_f, x_fwd, w1, w2, weights, rows_f, n_exp, top_k)
            if h + 1 < HALVES:
                x_fwd, y_half = lax.optimization_barrier((x_fwd, y_half))
            halves.append(lax.ppermute(y_half, "pp", next_perm))
        y_next = jnp.concatenate(halves, axis=0)[None]
        dws = [(a + b)[None] for a, b in zip(dw_own, there)]
        return y_next, dx_prev, *dws

    in_specs = (tok_spec,) * 9 + (dense_spec, dense_spec, expert_spec, expert_spec, expert_spec)
    out_specs = (tok_spec, tok_spec, expert_spec, expert_spec, expert_spec)
    return jax.shard_map(slot, mesh=mesh, in_specs=in_specs, out_specs=out_specs, check_vma=False)
```

```python
import functools

import jax
import jax.numpy as jnp
from jax import lax
from jax.experimental import pallas as pl
from jax.experimental.pallas import tpu as pltpu
from jax.sharding import PartitionSpec as P


NORM_EPS = 1e-6
TM = 256
BT = 512
DEPTH = 4
QUEUE = 8
HALVES = 2
F32 = jnp.float32
BF16 = jnp.bfloat16
VMEM_LIMIT = 60 * 1024 * 1024


def dot(a, b):
    return jnp.dot(a, b, preferred_element_type=F32)


def dot_nt(a, b):
    return lax.dot_general(a, b, (((1,), (1,)), ((), ())), preferred_element_type=F32)


def dot_tn(a, b):
    return lax.dot_general(a, b, (((0,), (0,)), ((), ())), preferred_element_type=F32)


def rms_scale(v):
    return lax.rsqrt(jnp.mean(v * v, axis=-1, keepdims=True) + NORM_EPS)


def rms_back(v, dy):
    r = rms_scale(v)
    return r * dy - v * (r * r * r * jnp.mean(dy * v, axis=-1, keepdims=True))


def dense_forward(xf, w1, w2):
    u = dot((xf * rms_scale(xf)).astype(BF16), w1)
    act = (u * jax.nn.sigmoid(u)).astype(BF16)
    return (xf + dot(act, w2)).astype(BF16)


def rank_routes(ids, slots, n_exp, dump):
    ids = jnp.where(slots >= 0, ids, -1)
    n, lanes = ids.shape
    row = lax.broadcasted_iota(jnp.int32, (lanes, lanes), 0)
    col = lax.broadcasted_iota(jnp.int32, (lanes, lanes), 1)
    upper = jnp.where(row < col, 1.0, 0.0).astype(BF16)
    right = jnp.concatenate([upper, jnp.ones((lanes, lanes), BF16)], axis=1)
    row = lax.broadcasted_iota(jnp.int32, (n + 8, n), 0)
    col = lax.broadcasted_iota(jnp.int32, (n + 8, n), 1)
    left = jnp.where((col < row) | (row >= n), 1.0, 0.0).astype(BF16)
    lane = lax.broadcasted_iota(jnp.int32, (n, lanes), 1)
    both = dot(jnp.concatenate([jnp.where(ids == e, 1.0, 0.0).astype(BF16) for e in range(n_exp)], axis=0), right)
    totals = jnp.zeros((n, lanes), F32)
    for e in range(n_exp):
        totals = jnp.where(lane == e, both[e * n : (e + 1) * n, lanes:], totals)
    pre = dot(left, totals.astype(BF16))
    tiles = jnp.maximum(jnp.floor((pre[n:] + (TM - 1.0)) * (1.0 / TM)), 1.0)
    tab = dot(tiles.astype(BF16), upper)
    base = pre[:n] + TM * tab[0:1]
    pos = jnp.full((n, lanes), float(dump), F32)
    for e in range(n_exp):
        pos = jnp.where(ids == e, both[e * n : (e + 1) * n, :lanes] + base[:, e : e + 1], pos)
    return pos, tab.astype(jnp.int32)


def chunks(ref, first, last):
    return jnp.concatenate([ref[:, c * 128 : (c + 1) * 128] for c in range(first, last)], axis=0)


def rank_kernel(n_exp, rows_b, rows_f, ids_b, slots_b, ids_f, slots_f, tab_b, pos4_b, pos2_b, tab_f, pos2_f):
    n = ids_b.shape[1] // 128
    pos, tab_b[...] = rank_routes(chunks(ids_b, 0, n), chunks(slots_b, 0, n), n_exp, rows_b)
    pos4_b[...] = (pos * 4.0).astype(jnp.int32)
    pos2_b[...] = (pos * 2.0).astype(jnp.int32)
    step = n // HALVES
    for h in range(HALVES):
        at = (h * step, (h + 1) * step)
        pos, tab_f[h] = rank_routes(chunks(ids_f, *at), chunks(slots_f, *at), n_exp, rows_f)
        k = pos.shape[0]
        pos2_f[h * k : (h + 1) * k, :] = (pos * 2.0).astype(jnp.int32)


def route_ranks(ids_b, slots_b, ids_f, slots_f, n_exp, rows_b, rows_f):
    pos = jax.ShapeDtypeStruct((ids_b.size // 128, 128), jnp.int32)
    tab = (8, 128)
    tab_b, pos4_b, pos2_b, tab_f, pos2_f = pl.pallas_call(
        functools.partial(rank_kernel, n_exp, rows_b, rows_f),
        out_shape=(
            jax.ShapeDtypeStruct(tab, jnp.int32),
            pos,
            pos,
            jax.ShapeDtypeStruct((HALVES, *tab), jnp.int32),
            pos,
        ),
        name="rank",
    )(ids_b.T, slots_b.T, ids_f.T, slots_f.T)
    return tab_b, pos4_b.reshape(-1), pos2_b.reshape(-1), tab_f, pos2_f.reshape(-1)


def put_rows(ref, at, vals, pitch=2, off=0):
    n = vals.shape[0]
    half = vals.shape[1] // 2
    ref[pl.ds(at + off, n, stride=pitch), :] = vals[:, :half]
    ref[pl.ds(at + off + 1, n, stride=pitch), :] = vals[:, half:]


def get_rows(ref, at, n, pitch=2, off=0):
    return jnp.concatenate([ref[pl.ds(at + off + i, n, stride=pitch), :] for i in range(2)], axis=1)


def rows_at(p, n):
    return pl.ds(pl.multiple_of(p, n), n)


def table_at(j, unroll, top_k):
    per = 128 // unroll
    return lax.div(j, per) * (128 * top_k) + lax.rem(j, per) * unroll


def gather_rows(buf, acc, pos_ref, top_k):
    unroll = 16

    def body(j, c):
        base = table_at(j, unroll, top_k)
        at = pl.multiple_of(j * (2 * unroll), 2 * unroll)
        for k in range(unroll):
            for r in range(top_k):
                acc[r, pl.ds(at + 2 * k, 2), :] = buf[rows_at(pos_ref[base + (r * 128 + k)], 2), :]
        return c

    lax.fori_loop(0, BT // unroll, body, 0)


def scatter_rows(src, buf, pos_ref, top_k, n, shared):
    unroll = 16

    def body(j, c):
        base = table_at(j, unroll, top_k)
        at = pl.multiple_of(j * (n * unroll), n * unroll)
        for k in range(unroll):
            v = src[pl.ds(at + n * k, n), :] if shared else None
            for r in range(top_k):
                row = v if shared else src[r, pl.ds(at + n * k, n), :]
                buf[rows_at(pos_ref[base + (r * 128 + k)], n), :] = row
        return c

    lax.fori_loop(0, BT // unroll, body, 0)


def zero_tails(buf, tab_ref, n_exp, pitch):
    def body(e, c):
        at = pl.multiple_of((tab_ref[0, e + 1] - 1) * (pitch * TM), pitch * TM)
        buf[pl.ds(at, pitch * TM), :] = jnp.zeros((pitch * TM, buf.shape[1]), F32)
        return c

    lax.fori_loop(0, n_exp, body, 0)


def pre_bwd_kernel(pos_ref, tab_ref, gate_ref, x_ref, g_ref, w1_ref, w2_ref, h_ref, xs_hbm, qs_hbm, buf, src, xst, qst, sems, *, n_blocks, top_k, n_exp):
    step = pl.program_id(0)

    @pl.when(step == 0)
    def _():
        zero_tails(buf, tab_ref, n_exp, 4)

    h = dense_forward(x_ref[...].astype(F32), w1_ref[...], w2_ref[...])
    h_ref[...] = h
    hf = h.astype(F32)
    n = (hf * rms_scale(hf)).astype(BF16).astype(F32)
    g = g_ref[...].astype(F32)
    gates = gate_ref[...].astype(F32).T
    for r in range(top_k):
        put_rows(src.at[r], 0, n, 4, 0)
        put_rows(src.at[r], 0, g * gates[:, r : r + 1], 4, 2)
    scatter_rows(src, buf, pos_ref, top_k, 4, False)

    @pl.when(step == n_blocks - 1)
    def _():
        n_tiles = tab_ref[0, n_exp]

        def copies(t, slot):
            rows = pl.ds(pl.multiple_of(t * TM, TM), TM)
            return (
                pltpu.make_async_copy(xst.at[slot], xs_hbm.at[rows], sems.at[0, slot]),
                pltpu.make_async_copy(qst.at[slot], qs_hbm.at[rows], sems.at[1, slot]),
            )

        def convert(t, c):
            slot = lax.rem(t, QUEUE)

            @pl.when(t >= QUEUE)
            def _():
                for cp in copies(t - QUEUE, slot):
                    cp.wait()

            rows = pl.multiple_of(t * (4 * TM), 4 * TM)
            xst[slot] = get_rows(buf, rows, TM, 4, 0).astype(BF16)
            qst[slot] = get_rows(buf, rows, TM, 4, 2).astype(BF16)
            for cp in copies(t, slot):
                cp.start()
            return c

        lax.fori_loop(0, n_tiles, convert, 0)
        for back in range(QUEUE, 0, -1):
            for cp in copies(n_tiles - back, lax.rem(n_tiles - back, QUEUE)):
                cp.wait()


def route_spec(top_k, n_blocks, first=0, skip=0):
    return pl.BlockSpec((top_k * BT,), lambda i: (skip + jnp.clip(i - first, 0, n_blocks - 1),), memory_space=pltpu.SMEM)


def gate_spec(top_k, n_blocks, first=0, skip=0):
    return pl.BlockSpec((top_k, BT), lambda i: (0, skip + jnp.clip(i - first, 0, n_blocks - 1)))


def pre_bwd(pos, tab, gates, x, g, w1, w2, rows, n_exp, top_k):
    n_tok, hid = x.shape
    n_blocks = n_tok // BT
    smem = pl.BlockSpec(memory_space=pltpu.SMEM)
    blk = pl.BlockSpec((BT, hid), lambda i: (i, 0))
    whole = pl.BlockSpec((hid, hid), lambda i: (0, 0))
    return pl.pallas_call(
        functools.partial(pre_bwd_kernel, n_blocks=n_blocks, top_k=top_k, n_exp=n_exp),
        grid=(n_blocks,),
        in_specs=[route_spec(top_k, n_blocks), smem, gate_spec(top_k, n_blocks), blk, blk, whole, whole],
        out_specs=[blk, pl.BlockSpec(memory_space=pl.ANY), pl.BlockSpec(memory_space=pl.ANY)],
        out_shape=(
            jax.ShapeDtypeStruct((n_tok, hid), BF16),
            jax.ShapeDtypeStruct((rows, hid), BF16),
            jax.ShapeDtypeStruct((rows, hid), BF16),
        ),
        scratch_shapes=[
            pltpu.VMEM((4 * rows + 8, hid // 2), F32),
            pltpu.VMEM((top_k, 4 * BT, hid // 2), F32),
            pltpu.VMEM((QUEUE, TM, hid), BF16),
            pltpu.VMEM((QUEUE, TM, hid), BF16),
            pltpu.SemaphoreType.DMA((2, QUEUE)),
        ],
        compiler_params=pltpu.CompilerParams(vmem_limit_bytes=VMEM_LIMIT),
        cost_estimate=pl.CostEstimate(flops=30_000_000_000, bytes_accessed=30_000_000, transcendentals=0),
        name="pre_bwd",
    )(pos, tab, gates, x, g, w1, w2)


def exp_bwd_kernel(first_ref, tab_ref, *refs, n_loc, has_init):
    w_hbm, (xs_hbm, qs_hbm), refs = refs[:3], refs[3:5], refs[5:]
    init_hbm, refs = (refs[:3], refs[3:]) if has_init else ((), refs)
    rs_hbm, *dw_hbm, wb, dwb, xb, qb, rb, mid, sems, wsems, dsems, isems = refs
    first = first_ref[0]
    begin = tab_ref[0, first]
    end = tab_ref[0, first + n_loc]

    def rows_of(t):
        return pl.ds(pl.multiple_of(t * TM, TM), TM)

    def loads(t):
        slot = lax.rem(t, DEPTH)
        return (
            pltpu.make_async_copy(xs_hbm.at[rows_of(t)], xb.at[slot], sems.at[0, slot]),
            pltpu.make_async_copy(qs_hbm.at[rows_of(t)], qb.at[slot], sems.at[1, slot]),
        )

    def save(t):
        slot = lax.rem(t, DEPTH)
        return pltpu.make_async_copy(rb.at[slot], rs_hbm.at[rows_of(t)], sems.at[2, slot])

    def w_loads(e):
        copies = [pltpu.make_async_copy(w_hbm[i].at[e], wb.at[i, e], wsems.at[i, e]) for i in range(3)]
        return copies + [pltpu.make_async_copy(ref.at[e], dwb.at[i, e], isems.at[i, e]) for i, ref in enumerate(init_hbm)]

    def dw_saves(e):
        return [pltpu.make_async_copy(dwb.at[i, e], dw_hbm[i].at[e], dsems.at[i, e]) for i in range(3)]

    def first_half(t, e):
        slot = lax.rem(t, DEPTH)
        x = xb[slot]
        pre = dot(x, wb[0, e])
        up = dot(x, wb[1, e])
        da = dot_nt(qb[slot], wb[2, e]).astype(BF16).astype(F32)
        sig = jax.nn.sigmoid(pre)
        sil = pre * sig
        return (
            (sil * up).astype(BF16),
            (da * up * (sig * (1.0 + pre * (1.0 - sig)))).astype(BF16),
            (da * sil).astype(BF16),
        )

    def keep(t, vals):
        for i, v in enumerate(vals):
            mid[lax.rem(t, 2), i] = v

    for cp in w_loads(0):
        cp.start()
    for ahead in range(DEPTH - 1):
        for cp in loads(begin + ahead):
            cp.start()
    for e in range(1, n_loc):
        for cp in w_loads(e):
            cp.start()
    if not has_init:
        def clear(e, c):
            for i in range(3):
                dwb[i, e] = jnp.zeros(dwb.shape[2:], F32)
            return c

        lax.fori_loop(0, n_loc, clear, 0)
    for cp in w_loads(0):
        cp.wait()
    for cp in loads(begin):
        cp.wait()
    keep(begin, first_half(begin, 0))

    def body(t, e):
        slot = lax.rem(t, DEPTH)
        more = t + 1 < end
        changes = t + 1 >= tab_ref[0, first + e + 1]
        then = jnp.where(changes & more, e + 1, e)

        @pl.when(changes & more)
        def _():
            for cp in w_loads(then):
                cp.wait()

        @pl.when(t + (DEPTH - 1) < end)
        def _():
            for cp in loads(t + (DEPTH - 1)):
                cp.start()

        @pl.when(more)
        def _():
            for cp in loads(t + 1):
                cp.wait()

        @pl.when(t >= begin + DEPTH)
        def _():
            save(t - DEPTH).wait()

        act, dpre, dup = mid[lax.rem(t, 2), 0], mid[lax.rem(t, 2), 1], mid[lax.rem(t, 2), 2]
        x = xb[slot]
        rows = (dot_nt(dpre, wb[0, e]) + dot_nt(dup, wb[1, e])).astype(BF16)
        upcoming = first_half(jnp.minimum(t + 1, end - 1), then)
        grads = (dot_tn(x, dpre), dot_tn(x, dup), dot_tn(act, qb[slot]))
        rb[slot] = rows
        for i, grad in enumerate(grads):
            dwb[i, e] += grad
        keep(t + 1, upcoming)
        save(t).start()

        @pl.when(changes)
        def _():
            for cp in dw_saves(e):
                cp.start()

        return then

    lax.fori_loop(begin, end, body, 0)
    for back in range(DEPTH, 0, -1):
        save(end - back).wait()
    for e in range(n_loc):
        for cp in dw_saves(e):
            cp.wait()


def exp_bwd(first, tab, wg, wu, wd, xs, qs, init=()):
    n_loc, hid, ff = wg.shape
    smem = pl.BlockSpec(memory_space=pltpu.SMEM)
    hbm = pl.BlockSpec(memory_space=pl.ANY)
    dw = jax.ShapeDtypeStruct((n_loc, hid, ff), F32)
    return pl.pallas_call(
        functools.partial(exp_bwd_kernel, n_loc=n_loc, has_init=bool(init)),
        in_specs=[smem, smem] + [hbm] * (5 + len(init)),
        out_specs=[hbm, hbm, hbm, hbm],
        out_shape=(jax.ShapeDtypeStruct(xs.shape, BF16), dw, dw, dw),
        input_output_aliases={5: 0},
        scratch_shapes=[
            pltpu.VMEM((3, n_loc, hid, ff), BF16),
            pltpu.VMEM((3, n_loc, hid, ff), F32),
            pltpu.VMEM((DEPTH, TM, hid), BF16),
            pltpu.VMEM((DEPTH, TM, hid), BF16),
            pltpu.VMEM((DEPTH, TM, hid), BF16),
            pltpu.VMEM((2, 3, TM, ff), BF16),
            pltpu.SemaphoreType.DMA((3, DEPTH)),
            pltpu.SemaphoreType.DMA((3, n_loc)),
            pltpu.SemaphoreType.DMA((3, n_loc)),
            pltpu.SemaphoreType.DMA((3, n_loc)),
        ],
        compiler_params=pltpu.CompilerParams(vmem_limit_bytes=VMEM_LIMIT),
        cost_estimate=pl.CostEstimate(flops=8_000_000_000, bytes_accessed=20_000_000, transcendentals=0),
        name="exp_bwd",
    )(first, tab, wg, wu, wd, xs, qs, *init)


def post_bwd_kernel(pos_ref, tab_ref, x_ref, g_ref, h_ref, w1_ref, w2_ref, rs_hbm, dx_ref, rbuf, acc, st, sems, *, n_blocks, top_k, n_exp, rows):
    @pl.when(pl.program_id(0) == 0)
    def _():
        n_tiles = tab_ref[0, n_exp]

        def load(t):
            slot = lax.rem(t, (2 * QUEUE))
            return pltpu.make_async_copy(rs_hbm.at[pl.ds(pl.multiple_of(t * TM, TM), TM)], st.at[slot], sems.at[slot])

        for ahead in range((2 * QUEUE) - 1):
            load(ahead).start()
        rbuf[2 * rows : 2 * rows + 8, :] = jnp.zeros((8, rbuf.shape[1]), F32)

        def expand(t, c):
            @pl.when(t + ((2 * QUEUE) - 1) < n_tiles)
            def _():
                load(t + ((2 * QUEUE) - 1)).start()

            load(t).wait()
            put_rows(rbuf, pl.multiple_of(t * (2 * TM), 2 * TM), st[lax.rem(t, (2 * QUEUE))].astype(F32))
            return c

        lax.fori_loop(0, n_tiles, expand, 0)

    gather_rows(rbuf, acc, pos_ref, top_k)
    dn = get_rows(acc.at[0], 0, BT)
    for r in range(1, top_k):
        dn = dn + get_rows(acc.at[r], 0, BT)
    xf = x_ref[...].astype(F32)
    u = dot((xf * rms_scale(xf)).astype(BF16), w1_ref[...])
    dh = g_ref[...].astype(F32) + rms_back(h_ref[...].astype(F32), dn)
    sig = jax.nn.sigmoid(u)
    du = (dot_nt(dh.astype(BF16), w2_ref[...]) * (sig * (1.0 + u * (1.0 - sig)))).astype(BF16)
    dx_ref[...] = (dh + rms_back(xf, dot_nt(du, w1_ref[...]))).astype(BF16)


def post_bwd(pos, tab, x, g, h, w1, w2, rs, n_exp, top_k):
    n_tok, hid = x.shape
    rows = rs.shape[0]
    n_blocks = n_tok // BT
    smem = pl.BlockSpec(memory_space=pltpu.SMEM)
    blk = pl.BlockSpec((BT, hid), lambda i: (i, 0))
    whole = pl.BlockSpec((hid, hid), lambda i: (0, 0))
    return pl.pallas_call(
        functools.partial(post_bwd_kernel, n_blocks=n_blocks, top_k=top_k, n_exp=n_exp, rows=rows),
        grid=(n_blocks,),
        in_specs=[route_spec(top_k, n_blocks), smem, blk, blk, blk, whole, whole, pl.BlockSpec(memory_space=pl.ANY)],
        out_specs=blk,
        out_shape=jax.ShapeDtypeStruct((n_tok, hid), BF16),
        scratch_shapes=[
            pltpu.VMEM((2 * rows + 8, hid // 2), F32),
            pltpu.VMEM((top_k, 2 * BT, hid // 2), F32),
            pltpu.VMEM(((2 * QUEUE), TM, hid), BF16),
            pltpu.SemaphoreType.DMA(((2 * QUEUE),)),
        ],
        compiler_params=pltpu.CompilerParams(vmem_limit_bytes=VMEM_LIMIT),
        cost_estimate=pl.CostEstimate(flops=30_000_000_000, bytes_accessed=30_000_000, transcendentals=0),
        name="post_bwd",
    )(pos, tab, x, g, h, w1, w2, rs)


def fwd_kernel(firsts_ref, tab_ref, pos_ref, pos_out_ref, gate_ref, x_ref, w1_ref, w2_ref, *rest, n_blocks, top_k, n_exp, n_groups, rows):
    w_hbm = rest[: 3 * n_groups]
    y_ref, buf, acc, hsc, wsc, mid, sems = rest[3 * n_groups :]
    nsc = acc.at[0]
    step = pl.program_id(0)
    n_loc = n_exp // n_groups

    def w_copy(i):
        return pltpu.make_async_copy(w_hbm[i], wsc.at[i % 3, pl.ds(firsts_ref[i // 3], n_loc)], sems.at[i])

    @pl.when(step == 0)
    def _():
        for i in range(3 * n_groups):
            w_copy(i).start()
        zero_tails(buf, tab_ref, n_exp, 2)

    @pl.when(step < n_blocks)
    def _():
        h = dense_forward(x_ref[...].astype(F32), w1_ref[...], w2_ref[...])
        base = step * BT
        hsc[pl.ds(pl.multiple_of(base, BT), BT), :] = h
        hf = h.astype(F32)
        put_rows(nsc, 0, (hf * rms_scale(hf)).astype(BF16).astype(F32))

        scatter_rows(nsc, buf, pos_ref, top_k, 2, True)

    @pl.when(step == n_blocks)
    def _():
        buf[2 * rows : 2 * rows + 8, :] = jnp.zeros((8, buf.shape[1]), F32)
        for i in range(3 * n_groups):
            w_copy(i).wait()
        end = tab_ref[0, n_exp]

        def rows_of(t):
            return get_rows(buf, pl.multiple_of(t * (2 * TM), 2 * TM), TM).astype(BF16)

        def first_half(x, e):
            pre = dot(x, wsc[0, e])
            up = dot(x, wsc[1, e])
            return (pre * jax.nn.sigmoid(pre) * up).astype(BF16)

        mid[0] = first_half(rows_of(0), 0)

        def body(t, e):
            then = jnp.where((t + 1 >= tab_ref[0, e + 1]) & (t + 1 < end), e + 1, e)
            x = rows_of(jnp.minimum(t + 1, end - 1))
            out = dot(mid[lax.rem(t, 2)], wsc[2, e]).astype(BF16).astype(F32)
            upcoming = first_half(x, then)
            put_rows(buf, pl.multiple_of(t * (2 * TM), 2 * TM), out)
            mid[lax.rem(t + 1, 2)] = upcoming
            return then

        lax.fori_loop(0, end, body, 0)

    @pl.when(step > n_blocks)
    def _():
        base = (step - n_blocks - 1) * BT

        gather_rows(buf, acc, pos_out_ref, top_k)
        gates = gate_ref[...].astype(F32).T
        h = hsc[pl.ds(pl.multiple_of(base, BT), BT), :]
        mix = get_rows(acc.at[0], 0, BT) * gates[:, 0:1]
        for r in range(1, top_k):
            mix = mix + get_rows(acc.at[r], 0, BT) * gates[:, r : r + 1]
        y_ref[...] = (h.astype(F32) + mix).astype(BF16)


def fwd(half, firsts, tab, pos, gates, x, w1, w2, weights, rows, n_exp, top_k):
    n_tok, hid = x.shape[0] // HALVES, x.shape[1]
    n_blocks = n_tok // BT
    skip = half * n_blocks
    n_groups = len(weights)
    smem = pl.BlockSpec(memory_space=pltpu.SMEM)
    whole = pl.BlockSpec((hid, hid), lambda i: (0, 0))
    flat = [w for group in weights for w in group]
    return pl.pallas_call(
        functools.partial(fwd_kernel, n_blocks=n_blocks, top_k=top_k, n_exp=n_exp, n_groups=n_groups, rows=rows),
        grid=(2 * n_blocks + 1,),
        in_specs=[smem, smem, route_spec(top_k, n_blocks, 0, skip), route_spec(top_k, n_blocks, n_blocks + 1, skip), gate_spec(top_k, n_blocks, n_blocks + 1, skip)]
        + [pl.BlockSpec((BT, hid), lambda i: (skip + jnp.minimum(i, n_blocks - 1), 0)), whole, whole]
        + [pl.BlockSpec(memory_space=pl.ANY)] * len(flat),
        out_specs=pl.BlockSpec((BT, hid), lambda i: (jnp.maximum(i - n_blocks - 1, 0), 0)),
        out_shape=jax.ShapeDtypeStruct((n_tok, hid), BF16),
        scratch_shapes=[
            pltpu.VMEM((2 * rows + 8, hid // 2), F32),
            pltpu.VMEM((top_k, 2 * BT, hid // 2), F32),
            pltpu.VMEM((n_tok, hid), BF16),
            pltpu.VMEM((3, n_exp, hid, hid), BF16),
            pltpu.VMEM((2, TM, hid), BF16),
            pltpu.SemaphoreType.DMA((len(flat),)),
        ],
        compiler_params=pltpu.CompilerParams(vmem_limit_bytes=VMEM_LIMIT),
        cost_estimate=pl.CostEstimate(flops=80_000_000_000, bytes_accessed=30_000_000, transcendentals=0),
        name="fwd",
    )(firsts, tab, pos, pos, gates, x, w1, w2, *flat)


def solution(mesh):
    stages = mesh.shape["pp"]
    ep_size = mesh.shape["ep"]
    next_perm = [(i, (i + 1) % stages) for i in range(stages)]
    prev_perm = [(i, (i - 1) % stages) for i in range(stages)]
    mate_perm = [(i, i ^ 1) for i in range(ep_size)]
    chip_perm = [(i, i ^ 2) for i in range(ep_size)]
    tok_spec = P("pp", "ep", None)
    dense_spec = P("pp", None, None)
    expert_spec = P("pp", "ep", None, None)

    def mate(a):
        return lax.ppermute(a, "ep", mate_perm)

    def chip(a):
        return lax.ppermute(a, "ep", chip_perm)

    def slot(x_fwd, ids_fwd, slots_fwd, gates_fwd, x_saved, grad_in, ids_bwd, slots_bwd, gates_bwd, w_one, w_two, w_gate, w_up, w_down):
        x_fwd, ids_fwd, slots_fwd, gates_fwd = x_fwd[0], ids_fwd[0], slots_fwd[0], gates_fwd[0]
        x_saved, grad_in, ids_bwd, slots_bwd, gates_bwd = x_saved[0], grad_in[0], ids_bwd[0], slots_bwd[0], gates_bwd[0]
        w1, w2, w_gate, w_up, w_down = w_one[0], w_two[0], w_gate[0], w_up[0], w_down[0]
        top_k = ids_fwd.shape[1]
        n_loc = w_gate.shape[0]
        n_exp = n_loc * ep_size
        rows = TM * (ids_fwd.size // TM + n_exp)
        rows_f = TM * (ids_fwd.size // HALVES // TM + n_exp)
        me = lax.axis_index("ep")

        own = (w_gate, w_up, w_down)
        far = tuple(chip(w) for w in own)
        near = tuple(mate(w) for w in own)
        far_near = tuple(mate(w) for w in far)
        weights = (own, near, far, far_near)
        firsts = [(me ^ g) * n_loc for g in range(ep_size)]

        tab_b, pos4_b, pos2_b, tab_f, pos2_f = route_ranks(ids_bwd, slots_bwd, ids_fwd, slots_fwd, n_exp, rows, rows_f)
        gates_b = gates_bwd.T
        gates_f = gates_fwd.T

        h_bwd, xs, qs = pre_bwd(pos4_b, tab_b, gates_b, x_saved, grad_in, w1, w2, rows, n_exp, top_k)

        def experts(g, xs, init=()):
            return exp_bwd(firsts[g].reshape(1), tab_b, *weights[g], xs, qs, init)

        xs, *part = experts(1, xs)
        near_sum = [mate(v) for v in part]
        xs, *part = experts(3, xs)
        far_sum = [mate(v) for v in part]
        xs, *dw_own = experts(0, xs, near_sum)
        xs, *part = experts(2, xs, far_sum)
        there = [chip(v) for v in part]
        grad_x = post_bwd(pos2_b, tab_b, x_saved, grad_in, h_bwd, w1, w2, xs, n_exp, top_k)
        x_fwd, grad_x = lax.optimization_barrier((x_fwd, grad_x))
        dx_prev = lax.ppermute(grad_x[None], "pp", prev_perm)

        halves = []
        first_stack = jnp.stack(firsts)
        for h in range(HALVES):
            y_half = fwd(h, first_stack, tab_f[h], pos2_f, gates_f, x_fwd, w1, w2, weights, rows_f, n_exp, top_k)
            if h + 1 < HALVES:
                x_fwd, y_half = lax.optimization_barrier((x_fwd, y_half))
            halves.append(lax.ppermute(y_half, "pp", next_perm))
        y_next = jnp.concatenate(halves, axis=0)[None]
        dws = [(a + b)[None] for a, b in zip(dw_own, there)]
        return y_next, dx_prev, *dws

    in_specs = (tok_spec,) * 9 + (dense_spec, dense_spec, expert_spec, expert_spec, expert_spec)
    out_specs = (tok_spec, tok_spec, expert_spec, expert_spec, expert_spec)
    return jax.shard_map(slot, mesh=mesh, in_specs=in_specs, out_specs=out_specs, check_vma=False)
```

```python
import functools

import jax
import jax.numpy as jnp
from jax import lax
from jax.experimental import pallas as pl
from jax.experimental.pallas import tpu as pltpu
from jax.sharding import PartitionSpec as P


NORM_EPS = 1e-6
TM = 256
BT = 512
DEPTH = 4
QUEUE = 8
FWD_BLOCKS = (5, 3)
F32 = jnp.float32
BF16 = jnp.bfloat16
VMEM_LIMIT = 60 * 1024 * 1024


def dot(a, b):
    return jnp.dot(a, b, preferred_element_type=F32)


def dot_nt(a, b):
    return lax.dot_general(a, b, (((1,), (1,)), ((), ())), preferred_element_type=F32)


def dot_tn(a, b):
    return lax.dot_general(a, b, (((0,), (0,)), ((), ())), preferred_element_type=F32)


def rms_scale(v):
    return lax.rsqrt(jnp.mean(v * v, axis=-1, keepdims=True) + NORM_EPS)


def rms_back(v, dy):
    r = rms_scale(v)
    return r * dy - v * (r * r * r * jnp.mean(dy * v, axis=-1, keepdims=True))


def dense_forward(xf, w1, w2):
    u = dot((xf * rms_scale(xf)).astype(BF16), w1)
    act = (u * jax.nn.sigmoid(u)).astype(BF16)
    return (xf + dot(act, w2)).astype(BF16)


def rank_routes(ids, slots, n_exp, dump):
    ids = jnp.where(slots >= 0, ids, -1)
    n, lanes = ids.shape
    row = lax.broadcasted_iota(jnp.int32, (lanes, lanes), 0)
    col = lax.broadcasted_iota(jnp.int32, (lanes, lanes), 1)
    upper = jnp.where(row < col, 1.0, 0.0).astype(BF16)
    right = jnp.concatenate([upper, jnp.ones((lanes, lanes), BF16)], axis=1)
    row = lax.broadcasted_iota(jnp.int32, (n + 8, n), 0)
    col = lax.broadcasted_iota(jnp.int32, (n + 8, n), 1)
    left = jnp.where((col < row) | (row >= n), 1.0, 0.0).astype(BF16)
    lane = lax.broadcasted_iota(jnp.int32, (n, lanes), 1)
    both = dot(jnp.concatenate([jnp.where(ids == e, 1.0, 0.0).astype(BF16) for e in range(n_exp)], axis=0), right)
    totals = jnp.zeros((n, lanes), F32)
    for e in range(n_exp):
        totals = jnp.where(lane == e, both[e * n : (e + 1) * n, lanes:], totals)
    pre = dot(left, totals.astype(BF16))
    tiles = jnp.maximum(jnp.floor((pre[n:] + (TM - 1.0)) * (1.0 / TM)), 1.0)
    tab = dot(tiles.astype(BF16), upper)
    base = pre[:n] + TM * tab[0:1]
    pos = jnp.full((n, lanes), float(dump), F32)
    for e in range(n_exp):
        pos = jnp.where(ids == e, both[e * n : (e + 1) * n, :lanes] + base[:, e : e + 1], pos)
    return pos, tab.astype(jnp.int32)


def chunks(ref, first, last):
    return jnp.concatenate([ref[:, c * 128 : (c + 1) * 128] for c in range(first, last)], axis=0)


def rank_kernel(n_exp, rows_b, rows_f, ids_b, slots_b, ids_f, slots_f, tab_b, pos4_b, pos2_b, tab_f, pos2_f):
    n = ids_b.shape[1] // 128
    pos, tab_b[...] = rank_routes(chunks(ids_b, 0, n), chunks(slots_b, 0, n), n_exp, rows_b)
    pos4_b[...] = (pos * 4.0).astype(jnp.int32)
    pos2_b[...] = (pos * 2.0).astype(jnp.int32)
    first = 0
    for h, (blocks, dump) in enumerate(zip(FWD_BLOCKS, rows_f)):
        last = first + blocks * (BT // 128)
        pos, tab_f[h] = rank_routes(chunks(ids_f, first, last), chunks(slots_f, first, last), n_exp, dump)
        k = ids_f.shape[0]
        pos2_f[first * k : last * k, :] = (pos * 2.0).astype(jnp.int32)
        first = last


def route_ranks(ids_b, slots_b, ids_f, slots_f, n_exp, rows_b, rows_f):
    pos = jax.ShapeDtypeStruct((ids_b.size // 128, 128), jnp.int32)
    tab = (8, 128)
    tab_b, pos4_b, pos2_b, tab_f, pos2_f = pl.pallas_call(
        functools.partial(rank_kernel, n_exp, rows_b, rows_f),
        out_shape=(
            jax.ShapeDtypeStruct(tab, jnp.int32),
            pos,
            pos,
            jax.ShapeDtypeStruct((len(FWD_BLOCKS), *tab), jnp.int32),
            pos,
        ),
        name="rank",
    )(ids_b.T, slots_b.T, ids_f.T, slots_f.T)
    return tab_b, pos4_b.reshape(-1), pos2_b.reshape(-1), tab_f, pos2_f.reshape(-1)


def put_rows(ref, at, vals, pitch=2, off=0):
    n = vals.shape[0]
    half = vals.shape[1] // 2
    ref[pl.ds(at + off, n, stride=pitch), :] = vals[:, :half]
    ref[pl.ds(at + off + 1, n, stride=pitch), :] = vals[:, half:]


def get_rows(ref, at, n, pitch=2, off=0):
    return jnp.concatenate([ref[pl.ds(at + off + i, n, stride=pitch), :] for i in range(2)], axis=1)


def rows_at(p, n):
    return pl.ds(pl.multiple_of(p, n), n)


def table_at(j, unroll, top_k):
    per = 128 // unroll
    return lax.div(j, per) * (128 * top_k) + lax.rem(j, per) * unroll


def gather_rows(buf, acc, pos_ref, top_k):
    unroll = 16

    def body(j, c):
        base = table_at(j, unroll, top_k)
        at = pl.multiple_of(j * (2 * unroll), 2 * unroll)
        for k in range(unroll):
            for r in range(top_k):
                acc[r, pl.ds(at + 2 * k, 2), :] = buf[rows_at(pos_ref[base + (r * 128 + k)], 2), :]
        return c

    lax.fori_loop(0, BT // unroll, body, 0)


def scatter_rows(src, buf, pos_ref, top_k, n, shared):
    unroll = 16

    def body(j, c):
        base = table_at(j, unroll, top_k)
        at = pl.multiple_of(j * (n * unroll), n * unroll)
        for k in range(unroll):
            v = src[pl.ds(at + n * k, n), :] if shared else None
            for r in range(top_k):
                row = v if shared else src[r, pl.ds(at + n * k, n), :]
                buf[rows_at(pos_ref[base + (r * 128 + k)], n), :] = row
        return c

    lax.fori_loop(0, BT // unroll, body, 0)


def zero_tails(buf, tab_ref, n_exp, pitch):
    def body(e, c):
        at = pl.multiple_of((tab_ref[0, e + 1] - 1) * (pitch * TM), pitch * TM)
        buf[pl.ds(at, pitch * TM), :] = jnp.zeros((pitch * TM, buf.shape[1]), F32)
        return c

    lax.fori_loop(0, n_exp, body, 0)


def pre_bwd_kernel(pos_ref, tab_ref, gate_ref, x_ref, g_ref, w1_ref, w2_ref, h_ref, xs_hbm, qs_hbm, buf, src, xst, qst, sems, *, n_blocks, top_k, n_exp):
    step = pl.program_id(0)

    @pl.when(step == 0)
    def _():
        zero_tails(buf, tab_ref, n_exp, 4)

    h = dense_forward(x_ref[...].astype(F32), w1_ref[...], w2_ref[...])
    h_ref[...] = h
    hf = h.astype(F32)
    n = (hf * rms_scale(hf)).astype(BF16).astype(F32)
    g = g_ref[...].astype(F32)
    gates = gate_ref[...].astype(F32).T
    for r in range(top_k):
        put_rows(src.at[r], 0, n, 4, 0)
        put_rows(src.at[r], 0, g * gates[:, r : r + 1], 4, 2)
    scatter_rows(src, buf, pos_ref, top_k, 4, False)

    @pl.when(step == n_blocks - 1)
    def _():
        n_tiles = tab_ref[0, n_exp]

        def copies(t, slot):
            rows = pl.ds(pl.multiple_of(t * TM, TM), TM)
            return (
                pltpu.make_async_copy(xst.at[slot], xs_hbm.at[rows], sems.at[0, slot]),
                pltpu.make_async_copy(qst.at[slot], qs_hbm.at[rows], sems.at[1, slot]),
            )

        def convert(t, c):
            slot = lax.rem(t, QUEUE)

            @pl.when(t >= QUEUE)
            def _():
                for cp in copies(t - QUEUE, slot):
                    cp.wait()

            rows = pl.multiple_of(t * (4 * TM), 4 * TM)
            xst[slot] = get_rows(buf, rows, TM, 4, 0).astype(BF16)
            qst[slot] = get_rows(buf, rows, TM, 4, 2).astype(BF16)
            for cp in copies(t, slot):
                cp.start()
            return c

        lax.fori_loop(0, n_tiles, convert, 0)
        for back in range(QUEUE, 0, -1):
            for cp in copies(n_tiles - back, lax.rem(n_tiles - back, QUEUE)):
                cp.wait()


def route_spec(top_k, n_blocks, first=0, skip=0):
    return pl.BlockSpec((top_k * BT,), lambda i: (skip + jnp.clip(i - first, 0, n_blocks - 1),), memory_space=pltpu.SMEM)


def gate_spec(top_k, n_blocks, first=0, skip=0):
    return pl.BlockSpec((top_k, BT), lambda i: (0, skip + jnp.clip(i - first, 0, n_blocks - 1)))


def pre_bwd(pos, tab, gates, x, g, w1, w2, rows, n_exp, top_k):
    n_tok, hid = x.shape
    n_blocks = n_tok // BT
    smem = pl.BlockSpec(memory_space=pltpu.SMEM)
    blk = pl.BlockSpec((BT, hid), lambda i: (i, 0))
    whole = pl.BlockSpec((hid, hid), lambda i: (0, 0))
    return pl.pallas_call(
        functools.partial(pre_bwd_kernel, n_blocks=n_blocks, top_k=top_k, n_exp=n_exp),
        grid=(n_blocks,),
        in_specs=[route_spec(top_k, n_blocks), smem, gate_spec(top_k, n_blocks), blk, blk, whole, whole],
        out_specs=[blk, pl.BlockSpec(memory_space=pl.ANY), pl.BlockSpec(memory_space=pl.ANY)],
        out_shape=(
            jax.ShapeDtypeStruct((n_tok, hid), BF16),
            jax.ShapeDtypeStruct((rows, hid), BF16),
            jax.ShapeDtypeStruct((rows, hid), BF16),
        ),
        scratch_shapes=[
            pltpu.VMEM((4 * rows + 8, hid // 2), F32),
            pltpu.VMEM((top_k, 4 * BT, hid // 2), F32),
            pltpu.VMEM((QUEUE, TM, hid), BF16),
            pltpu.VMEM((QUEUE, TM, hid), BF16),
            pltpu.SemaphoreType.DMA((2, QUEUE)),
        ],
        compiler_params=pltpu.CompilerParams(vmem_limit_bytes=VMEM_LIMIT),
        cost_estimate=pl.CostEstimate(flops=30_000_000_000, bytes_accessed=30_000_000, transcendentals=0),
        name="pre_bwd",
    )(pos, tab, gates, x, g, w1, w2)


def exp_bwd_kernel(first_ref, tab_ref, *refs, n_loc, has_init):
    w_hbm, (xs_hbm, qs_hbm), refs = refs[:3], refs[3:5], refs[5:]
    init_hbm, refs = (refs[:3], refs[3:]) if has_init else ((), refs)
    rs_hbm, *dw_hbm, wb, dwb, xb, qb, rb, mid, sems, wsems, dsems, isems = refs
    first = first_ref[0]
    begin = tab_ref[0, first]
    end = tab_ref[0, first + n_loc]

    def rows_of(t):
        return pl.ds(pl.multiple_of(t * TM, TM), TM)

    def loads(t):
        slot = lax.rem(t, DEPTH)
        return (
            pltpu.make_async_copy(xs_hbm.at[rows_of(t)], xb.at[slot], sems.at[0, slot]),
            pltpu.make_async_copy(qs_hbm.at[rows_of(t)], qb.at[slot], sems.at[1, slot]),
        )

    def save(t):
        slot = lax.rem(t, DEPTH)
        return pltpu.make_async_copy(rb.at[slot], rs_hbm.at[rows_of(t)], sems.at[2, slot])

    def w_loads(e):
        copies = [pltpu.make_async_copy(w_hbm[i].at[e], wb.at[i, e], wsems.at[i, e]) for i in range(3)]
        return copies + [pltpu.make_async_copy(ref.at[e], dwb.at[i, e], isems.at[i, e]) for i, ref in enumerate(init_hbm)]

    def dw_saves(e):
        return [pltpu.make_async_copy(dwb.at[i, e], dw_hbm[i].at[e], dsems.at[i, e]) for i in range(3)]

    def first_half(t, e):
        slot = lax.rem(t, DEPTH)
        x = xb[slot]
        pre = dot(x, wb[0, e])
        up = dot(x, wb[1, e])
        da = dot_nt(qb[slot], wb[2, e]).astype(BF16).astype(F32)
        sig = jax.nn.sigmoid(pre)
        sil = pre * sig
        return (
            (sil * up).astype(BF16),
            (da * up * (sig * (1.0 + pre * (1.0 - sig)))).astype(BF16),
            (da * sil).astype(BF16),
        )

    def keep(t, vals):
        for i, v in enumerate(vals):
            mid[lax.rem(t, 2), i] = v

    for cp in w_loads(0):
        cp.start()
    for ahead in range(DEPTH - 1):
        for cp in loads(begin + ahead):
            cp.start()
    for e in range(1, n_loc):
        for cp in w_loads(e):
            cp.start()
    if not has_init:
        def clear(e, c):
            for i in range(3):
                dwb[i, e] = jnp.zeros(dwb.shape[2:], F32)
            return c

        lax.fori_loop(0, n_loc, clear, 0)
    for cp in w_loads(0):
        cp.wait()
    for cp in loads(begin):
        cp.wait()
    keep(begin, first_half(begin, 0))

    def body(t, e):
        slot = lax.rem(t, DEPTH)
        more = t + 1 < end
        changes = t + 1 >= tab_ref[0, first + e + 1]
        then = jnp.where(changes & more, e + 1, e)

        @pl.when(changes & more)
        def _():
            for cp in w_loads(then):
                cp.wait()

        @pl.when(t + (DEPTH - 1) < end)
        def _():
            for cp in loads(t + (DEPTH - 1)):
                cp.start()

        @pl.when(more)
        def _():
            for cp in loads(t + 1):
                cp.wait()

        @pl.when(t >= begin + DEPTH)
        def _():
            save(t - DEPTH).wait()

        act, dpre, dup = mid[lax.rem(t, 2), 0], mid[lax.rem(t, 2), 1], mid[lax.rem(t, 2), 2]
        x = xb[slot]
        rows = (dot_nt(dpre, wb[0, e]) + dot_nt(dup, wb[1, e])).astype(BF16)
        upcoming = first_half(jnp.minimum(t + 1, end - 1), then)
        grads = (dot_tn(x, dpre), dot_tn(x, dup), dot_tn(act, qb[slot]))
        rb[slot] = rows
        for i, grad in enumerate(grads):
            dwb[i, e] += grad
        keep(t + 1, upcoming)
        save(t).start()

        @pl.when(changes)
        def _():
            for cp in dw_saves(e):
                cp.start()

        return then

    lax.fori_loop(begin, end, body, 0)
    for back in range(DEPTH, 0, -1):
        save(end - back).wait()
    for e in range(n_loc):
        for cp in dw_saves(e):
            cp.wait()


def exp_bwd(first, tab, wg, wu, wd, xs, qs, init=()):
    n_loc, hid, ff = wg.shape
    smem = pl.BlockSpec(memory_space=pltpu.SMEM)
    hbm = pl.BlockSpec(memory_space=pl.ANY)
    dw = jax.ShapeDtypeStruct((n_loc, hid, ff), F32)
    return pl.pallas_call(
        functools.partial(exp_bwd_kernel, n_loc=n_loc, has_init=bool(init)),
        in_specs=[smem, smem] + [hbm] * (5 + len(init)),
        out_specs=[hbm, hbm, hbm, hbm],
        out_shape=(jax.ShapeDtypeStruct(xs.shape, BF16), dw, dw, dw),
        input_output_aliases={5: 0},
        scratch_shapes=[
            pltpu.VMEM((3, n_loc, hid, ff), BF16),
            pltpu.VMEM((3, n_loc, hid, ff), F32),
            pltpu.VMEM((DEPTH, TM, hid), BF16),
            pltpu.VMEM((DEPTH, TM, hid), BF16),
            pltpu.VMEM((DEPTH, TM, hid), BF16),
            pltpu.VMEM((2, 3, TM, ff), BF16),
            pltpu.SemaphoreType.DMA((3, DEPTH)),
            pltpu.SemaphoreType.DMA((3, n_loc)),
            pltpu.SemaphoreType.DMA((3, n_loc)),
            pltpu.SemaphoreType.DMA((3, n_loc)),
        ],
        compiler_params=pltpu.CompilerParams(vmem_limit_bytes=VMEM_LIMIT),
        cost_estimate=pl.CostEstimate(flops=8_000_000_000, bytes_accessed=20_000_000, transcendentals=0),
        name="exp_bwd",
    )(first, tab, wg, wu, wd, xs, qs, *init)


def post_bwd_kernel(pos_ref, tab_ref, x_ref, g_ref, h_ref, w1_ref, w2_ref, rs_hbm, dx_ref, rbuf, acc, st, sems, *, n_blocks, top_k, n_exp, rows):
    @pl.when(pl.program_id(0) == 0)
    def _():
        n_tiles = tab_ref[0, n_exp]

        def load(t):
            slot = lax.rem(t, (2 * QUEUE))
            return pltpu.make_async_copy(rs_hbm.at[pl.ds(pl.multiple_of(t * TM, TM), TM)], st.at[slot], sems.at[slot])

        for ahead in range((2 * QUEUE) - 1):
            load(ahead).start()
        rbuf[2 * rows : 2 * rows + 8, :] = jnp.zeros((8, rbuf.shape[1]), F32)

        def expand(t, c):
            @pl.when(t + ((2 * QUEUE) - 1) < n_tiles)
            def _():
                load(t + ((2 * QUEUE) - 1)).start()

            load(t).wait()
            put_rows(rbuf, pl.multiple_of(t * (2 * TM), 2 * TM), st[lax.rem(t, (2 * QUEUE))].astype(F32))
            return c

        lax.fori_loop(0, n_tiles, expand, 0)

    gather_rows(rbuf, acc, pos_ref, top_k)
    dn = get_rows(acc.at[0], 0, BT)
    for r in range(1, top_k):
        dn = dn + get_rows(acc.at[r], 0, BT)
    xf = x_ref[...].astype(F32)
    u = dot((xf * rms_scale(xf)).astype(BF16), w1_ref[...])
    dh = g_ref[...].astype(F32) + rms_back(h_ref[...].astype(F32), dn)
    sig = jax.nn.sigmoid(u)
    du = (dot_nt(dh.astype(BF16), w2_ref[...]) * (sig * (1.0 + u * (1.0 - sig)))).astype(BF16)
    dx_ref[...] = (dh + rms_back(xf, dot_nt(du, w1_ref[...]))).astype(BF16)


def post_bwd(pos, tab, x, g, h, w1, w2, rs, n_exp, top_k):
    n_tok, hid = x.shape
    rows = rs.shape[0]
    n_blocks = n_tok // BT
    smem = pl.BlockSpec(memory_space=pltpu.SMEM)
    blk = pl.BlockSpec((BT, hid), lambda i: (i, 0))
    whole = pl.BlockSpec((hid, hid), lambda i: (0, 0))
    return pl.pallas_call(
        functools.partial(post_bwd_kernel, n_blocks=n_blocks, top_k=top_k, n_exp=n_exp, rows=rows),
        grid=(n_blocks,),
        in_specs=[route_spec(top_k, n_blocks), smem, blk, blk, blk, whole, whole, pl.BlockSpec(memory_space=pl.ANY)],
        out_specs=blk,
        out_shape=jax.ShapeDtypeStruct((n_tok, hid), BF16),
        scratch_shapes=[
            pltpu.VMEM((2 * rows + 8, hid // 2), F32),
            pltpu.VMEM((top_k, 2 * BT, hid // 2), F32),
            pltpu.VMEM(((2 * QUEUE), TM, hid), BF16),
            pltpu.SemaphoreType.DMA(((2 * QUEUE),)),
        ],
        compiler_params=pltpu.CompilerParams(vmem_limit_bytes=VMEM_LIMIT),
        cost_estimate=pl.CostEstimate(flops=30_000_000_000, bytes_accessed=30_000_000, transcendentals=0),
        name="post_bwd",
    )(pos, tab, x, g, h, w1, w2, rs)


def fwd_kernel(firsts_ref, tab_ref, pos_ref, pos_out_ref, gate_ref, x_ref, w1_ref, w2_ref, *rest, n_blocks, top_k, n_exp, n_groups, rows):
    w_hbm = rest[: 3 * n_groups]
    y_ref, buf, acc, hsc, wsc, mid, sems = rest[3 * n_groups :]
    nsc = acc.at[0]
    step = pl.program_id(0)

    def w_copy(i):
        return pltpu.make_async_copy(w_hbm[i], wsc.at[i % 3, pl.ds(firsts_ref[i // 3], w_hbm[i].shape[0])], sems.at[i])

    @pl.when(step == 0)
    def _():
        for i in range(3 * n_groups):
            w_copy(i).start()
        zero_tails(buf, tab_ref, n_exp, 2)

    @pl.when(step < n_blocks)
    def _():
        h = dense_forward(x_ref[...].astype(F32), w1_ref[...], w2_ref[...])
        base = step * BT
        hsc[pl.ds(pl.multiple_of(base, BT), BT), :] = h
        hf = h.astype(F32)
        put_rows(nsc, 0, (hf * rms_scale(hf)).astype(BF16).astype(F32))

        scatter_rows(nsc, buf, pos_ref, top_k, 2, True)

    @pl.when(step == n_blocks)
    def _():
        buf[2 * rows : 2 * rows + 8, :] = jnp.zeros((8, buf.shape[1]), F32)
        for i in range(3 * n_groups):
            w_copy(i).wait()
        end = tab_ref[0, n_exp]

        def rows_of(t):
            return get_rows(buf, pl.multiple_of(t * (2 * TM), 2 * TM), TM).astype(BF16)

        def first_half(x, e):
            pre = dot(x, wsc[0, e])
            up = dot(x, wsc[1, e])
            return (pre * jax.nn.sigmoid(pre) * up).astype(BF16)

        mid[0] = first_half(rows_of(0), 0)

        def body(t, e):
            then = jnp.where((t + 1 >= tab_ref[0, e + 1]) & (t + 1 < end), e + 1, e)
            x = rows_of(jnp.minimum(t + 1, end - 1))
            out = dot(mid[lax.rem(t, 2)], wsc[2, e]).astype(BF16).astype(F32)
            upcoming = first_half(x, then)
            put_rows(buf, pl.multiple_of(t * (2 * TM), 2 * TM), out)
            mid[lax.rem(t + 1, 2)] = upcoming
            return then

        lax.fori_loop(0, end, body, 0)

    @pl.when(step > n_blocks)
    def _():
        base = (step - n_blocks - 1) * BT

        gather_rows(buf, acc, pos_out_ref, top_k)
        gates = gate_ref[...].astype(F32).T
        h = hsc[pl.ds(pl.multiple_of(base, BT), BT), :]
        mix = get_rows(acc.at[0], 0, BT) * gates[:, 0:1]
        for r in range(1, top_k):
            mix = mix + get_rows(acc.at[r], 0, BT) * gates[:, r : r + 1]
        y_ref[...] = (h.astype(F32) + mix).astype(BF16)


def fwd(n_blocks, skip, firsts, tab, pos, gates, x, w1, w2, weights, rows, n_exp, top_k):
    n_tok, hid = n_blocks * BT, x.shape[1]
    n_groups = len(weights)
    smem = pl.BlockSpec(memory_space=pltpu.SMEM)
    whole = pl.BlockSpec((hid, hid), lambda i: (0, 0))
    flat = [w for group in weights for w in group]
    return pl.pallas_call(
        functools.partial(fwd_kernel, n_blocks=n_blocks, top_k=top_k, n_exp=n_exp, n_groups=n_groups, rows=rows),
        grid=(2 * n_blocks + 1,),
        in_specs=[smem, smem, route_spec(top_k, n_blocks, 0, skip), route_spec(top_k, n_blocks, n_blocks + 1, skip), gate_spec(top_k, n_blocks, n_blocks + 1, skip)]
        + [pl.BlockSpec((BT, hid), lambda i: (skip + jnp.minimum(i, n_blocks - 1), 0)), whole, whole]
        + [pl.BlockSpec(memory_space=pl.ANY)] * len(flat),
        out_specs=pl.BlockSpec((BT, hid), lambda i: (jnp.maximum(i - n_blocks - 1, 0), 0)),
        out_shape=jax.ShapeDtypeStruct((n_tok, hid), BF16),
        scratch_shapes=[
            pltpu.VMEM((2 * rows + 8, hid // 2), F32),
            pltpu.VMEM((top_k, 2 * BT, hid // 2), F32),
            pltpu.VMEM((n_tok, hid), BF16),
            pltpu.VMEM((3, n_exp, hid, hid), BF16),
            pltpu.VMEM((2, TM, hid), BF16),
            pltpu.SemaphoreType.DMA((len(flat),)),
        ],
        compiler_params=pltpu.CompilerParams(vmem_limit_bytes=VMEM_LIMIT),
        cost_estimate=pl.CostEstimate(flops=80_000_000_000, bytes_accessed=30_000_000, transcendentals=0),
        name="fwd",
    )(firsts, tab, pos, pos, gates, x, w1, w2, *flat)


def solution(mesh):
    stages = mesh.shape["pp"]
    ep_size = mesh.shape["ep"]
    next_perm = [(i, (i + 1) % stages) for i in range(stages)]
    prev_perm = [(i, (i - 1) % stages) for i in range(stages)]
    mate_perm = [(i, i ^ 1) for i in range(ep_size)]
    chip_perm = [(i, i ^ 2) for i in range(ep_size)]
    tok_spec = P("pp", "ep", None)
    dense_spec = P("pp", None, None)
    expert_spec = P("pp", "ep", None, None)

    def mate(a):
        return lax.ppermute(a, "ep", mate_perm)

    def chip(a):
        return lax.ppermute(a, "ep", chip_perm)

    def slot(x_fwd, ids_fwd, slots_fwd, gates_fwd, x_saved, grad_in, ids_bwd, slots_bwd, gates_bwd, w_one, w_two, w_gate, w_up, w_down):
        x_fwd, ids_fwd, slots_fwd, gates_fwd = x_fwd[0], ids_fwd[0], slots_fwd[0], gates_fwd[0]
        x_saved, grad_in, ids_bwd, slots_bwd, gates_bwd = x_saved[0], grad_in[0], ids_bwd[0], slots_bwd[0], gates_bwd[0]
        w1, w2, w_gate, w_up, w_down = w_one[0], w_two[0], w_gate[0], w_up[0], w_down[0]
        top_k = ids_fwd.shape[1]
        n_loc = w_gate.shape[0]
        n_exp = n_loc * ep_size
        rows = TM * (ids_fwd.size // TM + n_exp)
        rows_f = [TM * (blocks * BT * top_k // TM + n_exp) for blocks in FWD_BLOCKS]
        me = lax.axis_index("ep")

        own = (w_gate, w_up, w_down)
        half = n_loc // 2
        far = [[chip(w[h * half : (h + 1) * half]) for w in own] for h in range(2)]
        near = [mate(w) for w in own]
        relay = [[mate(w) for w in far[h]] for h in range(2)]
        groups = {
            "own": (me * n_loc, own),
            "near": ((me ^ 1) * n_loc, near),
            "far0": ((me ^ 2) * n_loc, far[0]),
            "far1": ((me ^ 2) * n_loc + half, far[1]),
            "relay0": ((me ^ 3) * n_loc, relay[0]),
            "relay1": ((me ^ 3) * n_loc + half, relay[1]),
        }

        tab_b, pos4_b, pos2_b, tab_f, pos2_f = route_ranks(ids_bwd, slots_bwd, ids_fwd, slots_fwd, n_exp, rows, rows_f)
        gates_b = gates_bwd.T
        gates_f = gates_fwd.T

        h_bwd, xs, qs = pre_bwd(pos4_b, tab_b, gates_b, x_saved, grad_in, w1, w2, rows, n_exp, top_k)

        def experts(name, xs, init=()):
            first, weights = groups[name]
            return exp_bwd(first.reshape(1), tab_b, *weights, xs, qs, init)

        def to_mate(parts):
            return [mate(v) for v in parts]

        there = []
        xs, *part = experts("relay0", xs)
        far_sum = to_mate(part)
        xs, *part = experts("near", xs)
        near_sum = to_mate(part)
        xs, *part = experts("far0", xs, far_sum)
        there.append([chip(v) for v in part])
        xs, *part = experts("relay1", xs)
        far_sum = to_mate(part)
        xs, *dw_own = experts("own", xs, near_sum)
        xs, *part = experts("far1", xs, far_sum)
        there.append([chip(v) for v in part])
        grad_x = post_bwd(pos2_b, tab_b, x_saved, grad_in, h_bwd, w1, w2, xs, n_exp, top_k)
        x_fwd, grad_x = lax.optimization_barrier((x_fwd, grad_x))
        dx_prev = lax.ppermute(grad_x[None], "pp", prev_perm)

        halves = []
        firsts = jnp.stack([first for first, _ in groups.values()])
        weights = [w for _, w in groups.values()]
        skip = 0
        for h, blocks in enumerate(FWD_BLOCKS):
            y_half = fwd(blocks, skip, firsts, tab_f[h], pos2_f, gates_f, x_fwd, w1, w2, weights, rows_f[h], n_exp, top_k)
            skip += blocks
            if h + 1 < len(FWD_BLOCKS):
                x_fwd, y_half = lax.optimization_barrier((x_fwd, y_half))
            halves.append(lax.ppermute(y_half, "pp", next_perm))
        y_next = jnp.concatenate(halves, axis=0)[None]
        dws = [jnp.concatenate([a[:half] + b, a[half:] + c], axis=0)[None] for a, b, c in zip(dw_own, *there)]
        return y_next, dx_prev, *dws

    in_specs = (tok_spec,) * 9 + (dense_spec, dense_spec, expert_spec, expert_spec, expert_spec)
    out_specs = (tok_spec, tok_spec, expert_spec, expert_spec, expert_spec)
    return jax.shard_map(slot, mesh=mesh, in_specs=in_specs, out_specs=out_specs, check_vma=False)
```

```python
import functools

import jax
import jax.numpy as jnp
from jax import lax
from jax.experimental import pallas as pl
from jax.experimental.pallas import tpu as pltpu
from jax.sharding import PartitionSpec as P


NORM_EPS = 1e-6
TM = 256
BT = 512
DEPTH = 4
QUEUE = 8
FWD_BLOCKS = (5, 3)
F32 = jnp.float32
BF16 = jnp.bfloat16
VMEM_LIMIT = 60 * 1024 * 1024


def dot(a, b):
    return jnp.dot(a, b, preferred_element_type=F32)


def dot_nt(a, b):
    return lax.dot_general(a, b, (((1,), (1,)), ((), ())), preferred_element_type=F32)


def dot_tn(a, b):
    return lax.dot_general(a, b, (((0,), (0,)), ((), ())), preferred_element_type=F32)


def rms_scale(v):
    return lax.rsqrt(jnp.mean(v * v, axis=-1, keepdims=True) + NORM_EPS)


def rms_back(v, dy):
    r = rms_scale(v)
    return r * dy - v * (r * r * r * jnp.mean(dy * v, axis=-1, keepdims=True))


def dense_forward(xf, w1, w2):
    u = dot((xf * rms_scale(xf)).astype(BF16), w1)
    act = (u * jax.nn.sigmoid(u)).astype(BF16)
    return (xf + dot(act, w2)).astype(BF16)


def rank_routes(ids, slots, n_exp, dump):
    ids = jnp.where(slots >= 0, ids, -1)
    n, lanes = ids.shape
    row = lax.broadcasted_iota(jnp.int32, (lanes, lanes), 0)
    col = lax.broadcasted_iota(jnp.int32, (lanes, lanes), 1)
    upper = jnp.where(row < col, 1.0, 0.0).astype(BF16)
    right = jnp.concatenate([upper, jnp.ones((lanes, lanes), BF16)], axis=1)
    row = lax.broadcasted_iota(jnp.int32, (n + 8, n), 0)
    col = lax.broadcasted_iota(jnp.int32, (n + 8, n), 1)
    left = jnp.where((col < row) | (row >= n), 1.0, 0.0).astype(BF16)
    lane = lax.broadcasted_iota(jnp.int32, (n, lanes), 1)
    both = dot(jnp.concatenate([jnp.where(ids == e, 1.0, 0.0).astype(BF16) for e in range(n_exp)], axis=0), right)
    totals = jnp.zeros((n, lanes), F32)
    for e in range(n_exp):
        totals = jnp.where(lane == e, both[e * n : (e + 1) * n, lanes:], totals)
    pre = dot(left, totals.astype(BF16))
    tiles = jnp.maximum(jnp.floor((pre[n:] + (TM - 1.0)) * (1.0 / TM)), 1.0)
    tab = dot(tiles.astype(BF16), upper)
    base = pre[:n] + TM * tab[0:1]
    pos = jnp.full((n, lanes), float(dump), F32)
    for e in range(n_exp):
        pos = jnp.where(ids == e, both[e * n : (e + 1) * n, :lanes] + base[:, e : e + 1], pos)
    return pos, tab.astype(jnp.int32)


def chunks(ref, first, last):
    return jnp.concatenate([ref[:, c * 128 : (c + 1) * 128] for c in range(first, last)], axis=0)


def rank_kernel(n_exp, rows_b, rows_f, ids_b, slots_b, ids_f, slots_f, tab_b, pos4_b, pos2_b, tab_f, pos2_f):
    n = ids_b.shape[1] // 128
    pos, tab_b[...] = rank_routes(chunks(ids_b, 0, n), chunks(slots_b, 0, n), n_exp, rows_b)
    pos4_b[...] = (pos * 4.0).astype(jnp.int32)
    pos2_b[...] = (pos * 2.0).astype(jnp.int32)
    first = 0
    for h, (blocks, dump) in enumerate(zip(FWD_BLOCKS, rows_f)):
        last = first + blocks * (BT // 128)
        pos, tab_f[h] = rank_routes(chunks(ids_f, first, last), chunks(slots_f, first, last), n_exp, dump)
        k = ids_f.shape[0]
        pos2_f[first * k : last * k, :] = (pos * 2.0).astype(jnp.int32)
        first = last


def route_ranks(ids_b, slots_b, ids_f, slots_f, n_exp, rows_b, rows_f):
    pos = jax.ShapeDtypeStruct((ids_b.size // 128, 128), jnp.int32)
    tab = (8, 128)
    tab_b, pos4_b, pos2_b, tab_f, pos2_f = pl.pallas_call(
        functools.partial(rank_kernel, n_exp, rows_b, rows_f),
        out_shape=(
            jax.ShapeDtypeStruct(tab, jnp.int32),
            pos,
            pos,
            jax.ShapeDtypeStruct((len(FWD_BLOCKS), *tab), jnp.int32),
            pos,
        ),
        name="rank",
    )(ids_b.T, slots_b.T, ids_f.T, slots_f.T)
    return tab_b, pos4_b.reshape(-1), pos2_b.reshape(-1), tab_f, pos2_f.reshape(-1)


def put_rows(ref, at, vals, pitch=2, off=0):
    n = vals.shape[0]
    half = vals.shape[1] // 2
    ref[pl.ds(at + off, n, stride=pitch), :] = vals[:, :half]
    ref[pl.ds(at + off + 1, n, stride=pitch), :] = vals[:, half:]


def get_rows(ref, at, n, pitch=2, off=0):
    return jnp.concatenate([ref[pl.ds(at + off + i, n, stride=pitch), :] for i in range(2)], axis=1)


def rows_at(p, n):
    return pl.ds(pl.multiple_of(p, n), n)


def table_at(j, unroll, top_k):
    per = 128 // unroll
    return lax.div(j, per) * (128 * top_k) + lax.rem(j, per) * unroll


def gather_rows(buf, acc, pos_ref, top_k):
    unroll = 32

    def body(j, c):
        base = table_at(j, unroll, top_k)
        at = pl.multiple_of(j * (2 * unroll), 2 * unroll)
        for k in range(unroll):
            for r in range(top_k):
                acc[r, pl.ds(at + 2 * k, 2), :] = buf[rows_at(pos_ref[base + (r * 128 + k)], 2), :]
        return c

    lax.fori_loop(0, BT // unroll, body, 0)


def scatter_rows(src, buf, pos_ref, top_k, n, shared):
    unroll = 32

    def body(j, c):
        base = table_at(j, unroll, top_k)
        at = pl.multiple_of(j * (n * unroll), n * unroll)
        for k in range(unroll):
            v = src[pl.ds(at + n * k, n), :] if shared else None
            for r in range(top_k):
                row = v if shared else src[r, pl.ds(at + n * k, n), :]
                buf[rows_at(pos_ref[base + (r * 128 + k)], n), :] = row
        return c

    lax.fori_loop(0, BT // unroll, body, 0)


def zero_tails(buf, tab_ref, n_exp, pitch):
    def body(e, c):
        at = pl.multiple_of((tab_ref[0, e + 1] - 1) * (pitch * TM), pitch * TM)
        buf[pl.ds(at, pitch * TM), :] = jnp.zeros((pitch * TM, buf.shape[1]), F32)
        return c

    lax.fori_loop(0, n_exp, body, 0)


def pre_bwd_kernel(pos_ref, tab_ref, gate_ref, x_ref, g_ref, w1_ref, w2_ref, h_ref, xs_hbm, qs_hbm, buf, src, xst, qst, sems, *, n_blocks, top_k, n_exp):
    step = pl.program_id(0)

    @pl.when(step == 0)
    def _():
        zero_tails(buf, tab_ref, n_exp, 4)

    h = dense_forward(x_ref[...].astype(F32), w1_ref[...], w2_ref[...])
    h_ref[...] = h
    hf = h.astype(F32)
    n = (hf * rms_scale(hf)).astype(BF16).astype(F32)
    g = g_ref[...].astype(F32)
    gates = gate_ref[...].astype(F32).T
    for r in range(top_k):
        put_rows(src.at[r], 0, n, 4, 0)
        put_rows(src.at[r], 0, g * gates[:, r : r + 1], 4, 2)
    scatter_rows(src, buf, pos_ref, top_k, 4, False)

    @pl.when(step == n_blocks - 1)
    def _():
        n_tiles = tab_ref[0, n_exp]

        def copies(t, slot):
            rows = pl.ds(pl.multiple_of(t * TM, TM), TM)
            return (
                pltpu.make_async_copy(xst.at[slot], xs_hbm.at[rows], sems.at[0, slot]),
                pltpu.make_async_copy(qst.at[slot], qs_hbm.at[rows], sems.at[1, slot]),
            )

        def convert(t, c):
            slot = lax.rem(t, QUEUE)

            @pl.when(t >= QUEUE)
            def _():
                for cp in copies(t - QUEUE, slot):
                    cp.wait()

            rows = pl.multiple_of(t * (4 * TM), 4 * TM)
            xst[slot] = get_rows(buf, rows, TM, 4, 0).astype(BF16)
            qst[slot] = get_rows(buf, rows, TM, 4, 2).astype(BF16)
            for cp in copies(t, slot):
                cp.start()
            return c

        lax.fori_loop(0, n_tiles, convert, 0)
        for back in range(QUEUE, 0, -1):
            for cp in copies(n_tiles - back, lax.rem(n_tiles - back, QUEUE)):
                cp.wait()


def route_spec(top_k, n_blocks, first=0, skip=0):
    return pl.BlockSpec((top_k * BT,), lambda i: (skip + jnp.clip(i - first, 0, n_blocks - 1),), memory_space=pltpu.SMEM)


def gate_spec(top_k, n_blocks, first=0, skip=0):
    return pl.BlockSpec((top_k, BT), lambda i: (0, skip + jnp.clip(i - first, 0, n_blocks - 1)))


def pre_bwd(pos, tab, gates, x, g, w1, w2, rows, n_exp, top_k):
    n_tok, hid = x.shape
    n_blocks = n_tok // BT
    smem = pl.BlockSpec(memory_space=pltpu.SMEM)
    blk = pl.BlockSpec((BT, hid), lambda i: (i, 0))
    whole = pl.BlockSpec((hid, hid), lambda i: (0, 0))
    return pl.pallas_call(
        functools.partial(pre_bwd_kernel, n_blocks=n_blocks, top_k=top_k, n_exp=n_exp),
        grid=(n_blocks,),
        in_specs=[route_spec(top_k, n_blocks), smem, gate_spec(top_k, n_blocks), blk, blk, whole, whole],
        out_specs=[blk, pl.BlockSpec(memory_space=pl.ANY), pl.BlockSpec(memory_space=pl.ANY)],
        out_shape=(
            jax.ShapeDtypeStruct((n_tok, hid), BF16),
            jax.ShapeDtypeStruct((rows, hid), BF16),
            jax.ShapeDtypeStruct((rows, hid), BF16),
        ),
        scratch_shapes=[
            pltpu.VMEM((4 * rows + 8, hid // 2), F32),
            pltpu.VMEM((top_k, 4 * BT, hid // 2), F32),
            pltpu.VMEM((QUEUE, TM, hid), BF16),
            pltpu.VMEM((QUEUE, TM, hid), BF16),
            pltpu.SemaphoreType.DMA((2, QUEUE)),
        ],
        compiler_params=pltpu.CompilerParams(vmem_limit_bytes=VMEM_LIMIT),
        cost_estimate=pl.CostEstimate(flops=30_000_000_000, bytes_accessed=30_000_000, transcendentals=0),
        name="pre_bwd",
    )(pos, tab, gates, x, g, w1, w2)


def exp_bwd_kernel(first_ref, tab_ref, xs_hbm, qs_hbm, *refs, n_parts, has_init):
    w_hbm, refs = refs[:n_parts], refs[n_parts:]
    init_hbm, refs = (refs[:1], refs[1:]) if has_init else ((), refs)
    per = w_hbm[0].shape[0]
    n_loc = n_parts * per
    rs_hbm, dw_hbm, wb, dwb, xb, qb, rb, mid, sems, wsems, dsems, isems = refs
    first = first_ref[0]
    begin = tab_ref[0, first]
    end = tab_ref[0, first + n_loc]

    def rows_of(t):
        return pl.ds(pl.multiple_of(t * TM, TM), TM)

    def loads(t):
        slot = lax.rem(t, DEPTH)
        return (
            pltpu.make_async_copy(xs_hbm.at[rows_of(t)], xb.at[slot], sems.at[0, slot]),
            pltpu.make_async_copy(qs_hbm.at[rows_of(t)], qb.at[slot], sems.at[1, slot]),
        )

    def save(t):
        slot = lax.rem(t, DEPTH)
        return pltpu.make_async_copy(rb.at[slot], rs_hbm.at[rows_of(t)], sems.at[2, slot])

    def w_loads(e, part=0, at=0):
        copies = [pltpu.make_async_copy(w_hbm[part].at[at], wb.at[e], wsems.at[e])]
        return copies + [pltpu.make_async_copy(ref.at[e], dwb.at[e], isems.at[e]) for ref in init_hbm]

    def dw_save(e):
        return pltpu.make_async_copy(dwb.at[e], dw_hbm.at[e], dsems.at[e])

    def first_half(t, e):
        slot = lax.rem(t, DEPTH)
        x = xb[slot]
        pre = dot(x, wb[e, 0])
        up = dot(x, wb[e, 1])
        da = dot_nt(qb[slot], wb[e, 2]).astype(BF16).astype(F32)
        sig = jax.nn.sigmoid(pre)
        sil = pre * sig
        return (
            (sil * up).astype(BF16),
            (da * up * (sig * (1.0 + pre * (1.0 - sig)))).astype(BF16),
            (da * sil).astype(BF16),
        )

    def keep(t, vals):
        for i, v in enumerate(vals):
            mid[lax.rem(t, 2), i] = v

    for cp in w_loads(0):
        cp.start()
    for ahead in range(DEPTH - 1):
        for cp in loads(begin + ahead):
            cp.start()
    for e in range(1, n_loc):
        for cp in w_loads(e, e // per, e % per):
            cp.start()
    if not has_init:
        def clear(e, c):
            dwb[e] = jnp.zeros(dwb.shape[1:], F32)
            return c

        lax.fori_loop(0, n_loc, clear, 0)
    for cp in w_loads(0):
        cp.wait()
    for cp in loads(begin):
        cp.wait()
    keep(begin, first_half(begin, 0))

    def body(t, e):
        slot = lax.rem(t, DEPTH)
        more = t + 1 < end
        changes = t + 1 >= tab_ref[0, first + e + 1]
        then = jnp.where(changes & more, e + 1, e)

        @pl.when(changes & more)
        def _():
            for cp in w_loads(then):
                cp.wait()

        @pl.when(t + (DEPTH - 1) < end)
        def _():
            for cp in loads(t + (DEPTH - 1)):
                cp.start()

        @pl.when(more)
        def _():
            for cp in loads(t + 1):
                cp.wait()

        @pl.when(t >= begin + DEPTH)
        def _():
            save(t - DEPTH).wait()

        act, dpre, dup = mid[lax.rem(t, 2), 0], mid[lax.rem(t, 2), 1], mid[lax.rem(t, 2), 2]
        x = xb[slot]
        rows = (dot_nt(dpre, wb[e, 0]) + dot_nt(dup, wb[e, 1])).astype(BF16)
        upcoming = first_half(jnp.minimum(t + 1, end - 1), then)
        grads = (dot_tn(x, dpre), dot_tn(x, dup), dot_tn(act, qb[slot]))
        rb[slot] = rows
        for i, grad in enumerate(grads):
            dwb[e, i] += grad
        keep(t + 1, upcoming)
        save(t).start()

        @pl.when(changes)
        def _():
            dw_save(e).start()

        return then

    lax.fori_loop(begin, end, body, 0)
    for back in range(DEPTH, 0, -1):
        save(end - back).wait()
    for e in range(n_loc):
        dw_save(e).wait()


def exp_bwd(first, tab, weights, xs, qs, init=()):
    per, _, hid, ff = weights[0].shape
    n_loc = per * len(weights)
    smem = pl.BlockSpec(memory_space=pltpu.SMEM)
    hbm = pl.BlockSpec(memory_space=pl.ANY)
    return pl.pallas_call(
        functools.partial(exp_bwd_kernel, n_parts=len(weights), has_init=bool(init)),
        in_specs=[smem, smem] + [hbm] * (2 + len(weights) + len(init)),
        out_specs=[hbm, hbm],
        out_shape=(jax.ShapeDtypeStruct(xs.shape, BF16), jax.ShapeDtypeStruct((n_loc, 3, hid, ff), F32)),
        input_output_aliases={2: 0},
        scratch_shapes=[
            pltpu.VMEM((n_loc, 3, hid, ff), BF16),
            pltpu.VMEM((n_loc, 3, hid, ff), F32),
            pltpu.VMEM((DEPTH, TM, hid), BF16),
            pltpu.VMEM((DEPTH, TM, hid), BF16),
            pltpu.VMEM((DEPTH, TM, hid), BF16),
            pltpu.VMEM((2, 3, TM, ff), BF16),
            pltpu.SemaphoreType.DMA((3, DEPTH)),
            pltpu.SemaphoreType.DMA((n_loc,)),
            pltpu.SemaphoreType.DMA((n_loc,)),
            pltpu.SemaphoreType.DMA((n_loc,)),
        ],
        compiler_params=pltpu.CompilerParams(vmem_limit_bytes=VMEM_LIMIT),
        cost_estimate=pl.CostEstimate(flops=8_000_000_000, bytes_accessed=20_000_000, transcendentals=0),
        name="exp_bwd",
    )(first, tab, xs, qs, *weights, *init)


def post_bwd_kernel(pos_ref, tab_ref, x_ref, g_ref, h_ref, w1_ref, w2_ref, rs_hbm, dx_ref, rbuf, acc, st, sems, *, n_blocks, top_k, n_exp, rows):
    @pl.when(pl.program_id(0) == 0)
    def _():
        n_tiles = tab_ref[0, n_exp]

        def load(t):
            slot = lax.rem(t, (2 * QUEUE))
            return pltpu.make_async_copy(rs_hbm.at[pl.ds(pl.multiple_of(t * TM, TM), TM)], st.at[slot], sems.at[slot])

        for ahead in range((2 * QUEUE) - 1):
            load(ahead).start()
        rbuf[2 * rows : 2 * rows + 8, :] = jnp.zeros((8, rbuf.shape[1]), F32)

        def expand(t, c):
            @pl.when(t + ((2 * QUEUE) - 1) < n_tiles)
            def _():
                load(t + ((2 * QUEUE) - 1)).start()

            load(t).wait()
            put_rows(rbuf, pl.multiple_of(t * (2 * TM), 2 * TM), st[lax.rem(t, (2 * QUEUE))].astype(F32))
            return c

        lax.fori_loop(0, n_tiles, expand, 0)

    gather_rows(rbuf, acc, pos_ref, top_k)
    dn = get_rows(acc.at[0], 0, BT)
    for r in range(1, top_k):
        dn = dn + get_rows(acc.at[r], 0, BT)
    xf = x_ref[...].astype(F32)
    u = dot((xf * rms_scale(xf)).astype(BF16), w1_ref[...])
    dh = g_ref[...].astype(F32) + rms_back(h_ref[...].astype(F32), dn)
    sig = jax.nn.sigmoid(u)
    du = (dot_nt(dh.astype(BF16), w2_ref[...]) * (sig * (1.0 + u * (1.0 - sig)))).astype(BF16)
    dx_ref[...] = (dh + rms_back(xf, dot_nt(du, w1_ref[...]))).astype(BF16)


def post_bwd(pos, tab, x, g, h, w1, w2, rs, n_exp, top_k):
    n_tok, hid = x.shape
    rows = rs.shape[0]
    n_blocks = n_tok // BT
    smem = pl.BlockSpec(memory_space=pltpu.SMEM)
    blk = pl.BlockSpec((BT, hid), lambda i: (i, 0))
    whole = pl.BlockSpec((hid, hid), lambda i: (0, 0))
    return pl.pallas_call(
        functools.partial(post_bwd_kernel, n_blocks=n_blocks, top_k=top_k, n_exp=n_exp, rows=rows),
        grid=(n_blocks,),
        in_specs=[route_spec(top_k, n_blocks), smem, blk, blk, blk, whole, whole, pl.BlockSpec(memory_space=pl.ANY)],
        out_specs=blk,
        out_shape=jax.ShapeDtypeStruct((n_tok, hid), BF16),
        scratch_shapes=[
            pltpu.VMEM((2 * rows + 8, hid // 2), F32),
            pltpu.VMEM((top_k, 2 * BT, hid // 2), F32),
            pltpu.VMEM(((2 * QUEUE), TM, hid), BF16),
            pltpu.SemaphoreType.DMA(((2 * QUEUE),)),
        ],
        compiler_params=pltpu.CompilerParams(vmem_limit_bytes=VMEM_LIMIT),
        cost_estimate=pl.CostEstimate(flops=30_000_000_000, bytes_accessed=30_000_000, transcendentals=0),
        name="post_bwd",
    )(pos, tab, x, g, h, w1, w2, rs)


def fwd_kernel(firsts_ref, tab_ref, pos_ref, pos_out_ref, gate_ref, x_ref, w1_ref, w2_ref, *rest, n_blocks, top_k, n_exp, n_groups, rows):
    w_hbm = rest[:n_groups]
    y_ref, buf, acc, hsc, wsc, mid, sems = rest[n_groups:]
    nsc = acc.at[0]
    step = pl.program_id(0)

    def w_copy(i):
        return pltpu.make_async_copy(w_hbm[i], wsc.at[pl.ds(firsts_ref[i], w_hbm[i].shape[0])], sems.at[i])

    @pl.when(step == 0)
    def _():
        for i in range(n_groups):
            w_copy(i).start()
        zero_tails(buf, tab_ref, n_exp, 2)

    @pl.when(step < n_blocks)
    def _():
        h = dense_forward(x_ref[...].astype(F32), w1_ref[...], w2_ref[...])
        base = step * BT
        hsc[pl.ds(pl.multiple_of(base, BT), BT), :] = h
        hf = h.astype(F32)
        put_rows(nsc, 0, (hf * rms_scale(hf)).astype(BF16).astype(F32))

        scatter_rows(nsc, buf, pos_ref, top_k, 2, True)

    @pl.when(step == n_blocks)
    def _():
        buf[2 * rows : 2 * rows + 8, :] = jnp.zeros((8, buf.shape[1]), F32)
        for i in range(n_groups):
            w_copy(i).wait()
        end = tab_ref[0, n_exp]

        def rows_of(t):
            return get_rows(buf, pl.multiple_of(t * (2 * TM), 2 * TM), TM).astype(BF16)

        def first_half(x, e):
            pre = dot(x, wsc[e, 0])
            up = dot(x, wsc[e, 1])
            return (pre * jax.nn.sigmoid(pre) * up).astype(BF16)

        mid[0] = first_half(rows_of(0), 0)

        def body(t, e):
            then = jnp.where((t + 1 >= tab_ref[0, e + 1]) & (t + 1 < end), e + 1, e)
            x = rows_of(jnp.minimum(t + 1, end - 1))
            out = dot(mid[lax.rem(t, 2)], wsc[e, 2]).astype(BF16).astype(F32)
            upcoming = first_half(x, then)
            put_rows(buf, pl.multiple_of(t * (2 * TM), 2 * TM), out)
            mid[lax.rem(t + 1, 2)] = upcoming
            return then

        lax.fori_loop(0, end, body, 0)

    @pl.when(step > n_blocks)
    def _():
        base = (step - n_blocks - 1) * BT

        gather_rows(buf, acc, pos_out_ref, top_k)
        gates = gate_ref[...].astype(F32).T
        h = hsc[pl.ds(pl.multiple_of(base, BT), BT), :]
        mix = get_rows(acc.at[0], 0, BT) * gates[:, 0:1]
        for r in range(1, top_k):
            mix = mix + get_rows(acc.at[r], 0, BT) * gates[:, r : r + 1]
        y_ref[...] = (h.astype(F32) + mix).astype(BF16)


def fwd(n_blocks, skip, firsts, tab, pos, gates, x, w1, w2, weights, rows, n_exp, top_k):
    n_tok, hid = n_blocks * BT, x.shape[1]
    n_groups = len(weights)
    smem = pl.BlockSpec(memory_space=pltpu.SMEM)
    whole = pl.BlockSpec((hid, hid), lambda i: (0, 0))
    return pl.pallas_call(
        functools.partial(fwd_kernel, n_blocks=n_blocks, top_k=top_k, n_exp=n_exp, n_groups=n_groups, rows=rows),
        grid=(2 * n_blocks + 1,),
        in_specs=[smem, smem, route_spec(top_k, n_blocks, 0, skip), route_spec(top_k, n_blocks, n_blocks + 1, skip), gate_spec(top_k, n_blocks, n_blocks + 1, skip)]
        + [pl.BlockSpec((BT, hid), lambda i: (skip + jnp.minimum(i, n_blocks - 1), 0)), whole, whole]
        + [pl.BlockSpec(memory_space=pl.ANY)] * n_groups,
        out_specs=pl.BlockSpec((BT, hid), lambda i: (jnp.maximum(i - n_blocks - 1, 0), 0)),
        out_shape=jax.ShapeDtypeStruct((n_tok, hid), BF16),
        scratch_shapes=[
            pltpu.VMEM((2 * rows + 8, hid // 2), F32),
            pltpu.VMEM((top_k, 2 * BT, hid // 2), F32),
            pltpu.VMEM((n_tok, hid), BF16),
            pltpu.VMEM((n_exp, 3, hid, hid), BF16),
            pltpu.VMEM((2, TM, hid), BF16),
            pltpu.SemaphoreType.DMA((n_groups,)),
        ],
        compiler_params=pltpu.CompilerParams(vmem_limit_bytes=VMEM_LIMIT),
        cost_estimate=pl.CostEstimate(flops=80_000_000_000, bytes_accessed=30_000_000, transcendentals=0),
        name="fwd",
    )(firsts, tab, pos, pos, gates, x, w1, w2, *weights)


def solution(mesh):
    stages = mesh.shape["pp"]
    ep_size = mesh.shape["ep"]
    next_perm = [(i, (i + 1) % stages) for i in range(stages)]
    prev_perm = [(i, (i - 1) % stages) for i in range(stages)]
    mate_perm = [(i, i ^ 1) for i in range(ep_size)]
    chip_perm = [(i, i ^ 2) for i in range(ep_size)]
    tok_spec = P("pp", "ep", None)
    dense_spec = P("pp", None, None)
    expert_spec = P("pp", "ep", None, None)

    def mate(a):
        return lax.ppermute(a, "ep", mate_perm)

    def chip(a):
        return lax.ppermute(a, "ep", chip_perm)

    def slot(x_fwd, ids_fwd, slots_fwd, gates_fwd, x_saved, grad_in, ids_bwd, slots_bwd, gates_bwd, w_one, w_two, w_gate, w_up, w_down):
        x_fwd, ids_fwd, slots_fwd, gates_fwd = x_fwd[0], ids_fwd[0], slots_fwd[0], gates_fwd[0]
        x_saved, grad_in, ids_bwd, slots_bwd, gates_bwd = x_saved[0], grad_in[0], ids_bwd[0], slots_bwd[0], gates_bwd[0]
        w1, w2, w_gate, w_up, w_down = w_one[0], w_two[0], w_gate[0], w_up[0], w_down[0]
        top_k = ids_fwd.shape[1]
        n_loc = w_gate.shape[0]
        n_exp = n_loc * ep_size
        rows = TM * (ids_fwd.size // TM + n_exp)
        rows_f = [TM * (blocks * BT * top_k // TM + n_exp) for blocks in FWD_BLOCKS]
        me = lax.axis_index("ep")

        half = n_loc // 2
        halves = [slice(0, half), slice(half, n_loc)]
        own = [jnp.stack([w[at] for w in (w_gate, w_up, w_down)], axis=1) for at in halves]
        far = [chip(w) for w in own]
        near = [mate(w) for w in own]
        relay = [mate(w) for w in far]
        groups = {
            "own": (me * n_loc, own),
            "near": ((me ^ 1) * n_loc, near),
            "far0": ((me ^ 2) * n_loc, far[:1]),
            "far1": ((me ^ 2) * n_loc + half, far[1:]),
            "relay0": ((me ^ 3) * n_loc, relay[:1]),
            "relay1": ((me ^ 3) * n_loc + half, relay[1:]),
        }

        tab_b, pos4_b, pos2_b, tab_f, pos2_f = route_ranks(ids_bwd, slots_bwd, ids_fwd, slots_fwd, n_exp, rows, rows_f)
        gates_b = gates_bwd.T
        gates_f = gates_fwd.T

        h_bwd, xs, qs = pre_bwd(pos4_b, tab_b, gates_b, x_saved, grad_in, w1, w2, rows, n_exp, top_k)

        def experts(name, xs, init=()):
            first, weights = groups[name]
            return exp_bwd(first.reshape(1), tab_b, weights, xs, qs, init)

        xs, part = experts("relay0", xs)
        far_sum = mate(part)
        xs, part = experts("near", xs)
        near_sum = mate(part)
        xs, part = experts("far0", xs, (far_sum,))
        there = [chip(part)]
        xs, part = experts("relay1", xs)
        far_sum = mate(part)
        xs, dw_own = experts("own", xs, (near_sum,))
        xs, part = experts("far1", xs, (far_sum,))
        there.append(chip(part))
        grad_x = post_bwd(pos2_b, tab_b, x_saved, grad_in, h_bwd, w1, w2, xs, n_exp, top_k)
        x_fwd, grad_x = lax.optimization_barrier((x_fwd, grad_x))
        dx_prev = lax.ppermute(grad_x[None], "pp", prev_perm)

        parts = []
        firsts = jnp.stack([first + i * half for first, ws in groups.values() for i in range(len(ws))])
        weights = [w for _, ws in groups.values() for w in ws]
        skip = 0
        for h, blocks in enumerate(FWD_BLOCKS):
            y_half = fwd(blocks, skip, firsts, tab_f[h], pos2_f, gates_f, x_fwd, w1, w2, weights, rows_f[h], n_exp, top_k)
            skip += blocks
            if h + 1 < len(FWD_BLOCKS):
                x_fwd, y_half = lax.optimization_barrier((x_fwd, y_half))
            parts.append(lax.ppermute(y_half, "pp", next_perm))
        y_next = jnp.concatenate(parts, axis=0)[None]
        dws = [jnp.concatenate([dw_own[at, i] + sums[:, i] for at, sums in zip(halves, there)], axis=0)[None] for i in range(3)]
        dx_prev = jnp.where(me >= 0, dx_prev, jnp.zeros_like(dx_prev))
        return y_next, dx_prev, *dws

    in_specs = (tok_spec,) * 9 + (dense_spec, dense_spec, expert_spec, expert_spec, expert_spec)
    out_specs = (tok_spec, tok_spec, expert_spec, expert_spec, expert_spec)
    return jax.shard_map(slot, mesh=mesh, in_specs=in_specs, out_specs=out_specs, check_vma=False)
```

```python
import functools

import jax
import jax.numpy as jnp
from jax import lax
from jax.experimental import pallas as pl
from jax.experimental.pallas import tpu as pltpu
from jax.sharding import PartitionSpec as P


NORM_EPS = 1e-6
TM = 256
BT = 512
DEPTH = 4
QUEUE = 8
FWD_BLOCKS = (5, 3)
F32 = jnp.float32
BF16 = jnp.bfloat16
VMEM_LIMIT = 60 * 1024 * 1024


def dot(a, b):
    return jnp.dot(a, b, preferred_element_type=F32)


def dot_nt(a, b):
    return lax.dot_general(a, b, (((1,), (1,)), ((), ())), preferred_element_type=F32)


def dot_tn(a, b):
    return lax.dot_general(a, b, (((0,), (0,)), ((), ())), preferred_element_type=F32)


def rms_scale(v):
    return lax.rsqrt(jnp.mean(v * v, axis=-1, keepdims=True) + NORM_EPS)


def rms_back(v, dy):
    r = rms_scale(v)
    return r * dy - v * (r * r * r * jnp.mean(dy * v, axis=-1, keepdims=True))


def dense_forward(xf, w1, w2):
    u = dot((xf * rms_scale(xf)).astype(BF16), w1)
    act = (u * jax.nn.sigmoid(u)).astype(BF16)
    return (xf + dot(act, w2)).astype(BF16)


def rank_routes(ids, slots, n_exp, dump):
    ids = jnp.where(slots >= 0, ids, -1)
    n, lanes = ids.shape
    row = lax.broadcasted_iota(jnp.int32, (lanes, lanes), 0)
    col = lax.broadcasted_iota(jnp.int32, (lanes, lanes), 1)
    upper = jnp.where(row < col, 1.0, 0.0).astype(BF16)
    right = jnp.concatenate([upper, jnp.ones((lanes, lanes), BF16)], axis=1)
    row = lax.broadcasted_iota(jnp.int32, (n + 8, n), 0)
    col = lax.broadcasted_iota(jnp.int32, (n + 8, n), 1)
    left = jnp.where((col < row) | (row >= n), 1.0, 0.0).astype(BF16)
    lane = lax.broadcasted_iota(jnp.int32, (n, lanes), 1)
    both = dot(jnp.concatenate([jnp.where(ids == e, 1.0, 0.0).astype(BF16) for e in range(n_exp)], axis=0), right)
    totals = jnp.zeros((n, lanes), F32)
    for e in range(n_exp):
        totals = jnp.where(lane == e, both[e * n : (e + 1) * n, lanes:], totals)
    pre = dot(left, totals.astype(BF16))
    tiles = jnp.maximum(jnp.floor((pre[n:] + (TM - 1.0)) * (1.0 / TM)), 1.0)
    tab = dot(tiles.astype(BF16), upper)
    base = pre[:n] + TM * tab[0:1]
    pos = jnp.full((n, lanes), float(dump), F32)
    for e in range(n_exp):
        pos = jnp.where(ids == e, both[e * n : (e + 1) * n, :lanes] + base[:, e : e + 1], pos)
    return pos, tab.astype(jnp.int32)


def chunks(ref, first, last):
    return jnp.concatenate([ref[r : r + 1, c * 128 : (c + 1) * 128] for r in range(ref.shape[0]) for c in range(first, last)], axis=0)


def rank_kernel(n_exp, rows_b, rows_f, ids_b, slots_b, ids_f, slots_f, tab_b, pos4_b, pos2_b, tab_f, *pos2_f):
    n = ids_b.shape[1] // 128
    pos, tab_b[...] = rank_routes(chunks(ids_b, 0, n), chunks(slots_b, 0, n), n_exp, rows_b)
    pos4_b[...] = (pos * 4.0).astype(jnp.int32)
    pos2_b[...] = (pos * 2.0).astype(jnp.int32)
    first = 0
    for h, (blocks, dump) in enumerate(zip(FWD_BLOCKS, rows_f)):
        last = first + blocks * (BT // 128)
        pos, tab_f[h] = rank_routes(chunks(ids_f, first, last), chunks(slots_f, first, last), n_exp, dump)
        pos2_f[h][...] = (pos * 2.0).astype(jnp.int32)
        first = last


def route_ranks(ids_b, slots_b, ids_f, slots_f, n_exp, rows_b, rows_f):
    def table(n_tok):
        return jax.ShapeDtypeStruct((n_tok * ids_b.shape[1] // 128, 128), jnp.int32)

    n_tok = ids_b.shape[0]
    tab_b, pos4_b, pos2_b, tab_f, *pos2_f = pl.pallas_call(
        functools.partial(rank_kernel, n_exp, rows_b, rows_f),
        out_shape=(
            jax.ShapeDtypeStruct((8, 128), jnp.int32),
            table(n_tok),
            table(n_tok),
            jax.ShapeDtypeStruct((len(FWD_BLOCKS), 8, 128), jnp.int32),
            *[table(blocks * BT) for blocks in FWD_BLOCKS],
        ),
        name="rank",
    )(ids_b.T, slots_b.T, ids_f.T, slots_f.T)
    return tab_b, pos4_b.reshape(-1), pos2_b.reshape(-1), tab_f, [p.reshape(-1) for p in pos2_f]


def put_rows(ref, at, vals, pitch=2, off=0):
    n = vals.shape[0]
    half = vals.shape[1] // 2
    ref[pl.ds(at + off, n, stride=pitch), :] = vals[:, :half]
    ref[pl.ds(at + off + 1, n, stride=pitch), :] = vals[:, half:]


def get_rows(ref, at, n, pitch=2, off=0):
    return jnp.concatenate([ref[pl.ds(at + off + i, n, stride=pitch), :] for i in range(2)], axis=1)


def rows_at(p, n):
    return pl.ds(pl.multiple_of(p, n), n)


def gather_rows(buf, acc, pos_refs):
    unroll = 32

    def body(j, c):
        base = j * unroll
        at = pl.multiple_of(j * (2 * unroll), 2 * unroll)
        for k in range(unroll):
            i = base + k
            for r, pos_ref in enumerate(pos_refs):
                acc[r, pl.ds(at + 2 * k, 2), :] = buf[rows_at(pos_ref[i], 2), :]
        return c

    lax.fori_loop(0, BT // unroll, body, 0)


def scatter_rows(src, buf, pos_refs, n, shared):
    unroll = 32

    def body(j, c):
        base = j * unroll
        at = pl.multiple_of(j * (n * unroll), n * unroll)
        for k in range(unroll):
            i = base + k
            v = src[pl.ds(at + n * k, n), :] if shared else None
            for r, pos_ref in enumerate(pos_refs):
                buf[rows_at(pos_ref[i], n), :] = v if shared else src[r, pl.ds(at + n * k, n), :]
        return c

    lax.fori_loop(0, BT // unroll, body, 0)


def zero_tails(buf, tab_ref, n_exp, pitch):
    def body(e, c):
        at = pl.multiple_of((tab_ref[0, e + 1] - 1) * (pitch * TM), pitch * TM)
        buf[pl.ds(at, pitch * TM), :] = jnp.zeros((pitch * TM, buf.shape[1]), F32)
        return c

    lax.fori_loop(0, n_exp, body, 0)


def pre_bwd_kernel(*refs, n_blocks, top_k, n_exp):
    pos_refs, refs = refs[:top_k], refs[top_k:]
    tab_ref, gate_ref, x_ref, g_ref, w1_ref, w2_ref, h_ref, xs_hbm, qs_hbm, buf, src, xst, qst, sems = refs
    step = pl.program_id(0)

    @pl.when(step == 0)
    def _():
        zero_tails(buf, tab_ref, n_exp, 4)

    h = dense_forward(x_ref[...].astype(F32), w1_ref[...], w2_ref[...])
    h_ref[...] = h
    hf = h.astype(F32)
    n = (hf * rms_scale(hf)).astype(BF16).astype(F32)
    g = g_ref[...].astype(F32)
    gates = gate_ref[...].astype(F32).T
    for r in range(top_k):
        put_rows(src.at[r], 0, n, 4, 0)
        put_rows(src.at[r], 0, g * gates[:, r : r + 1], 4, 2)
    scatter_rows(src, buf, pos_refs, 4, False)

    @pl.when(step == n_blocks - 1)
    def _():
        n_tiles = tab_ref[0, n_exp]

        def copies(t, slot):
            rows = pl.ds(pl.multiple_of(t * TM, TM), TM)
            return (
                pltpu.make_async_copy(xst.at[slot], xs_hbm.at[rows], sems.at[0, slot]),
                pltpu.make_async_copy(qst.at[slot], qs_hbm.at[rows], sems.at[1, slot]),
            )

        def convert(t, c):
            slot = lax.rem(t, QUEUE)

            @pl.when(t >= QUEUE)
            def _():
                for cp in copies(t - QUEUE, slot):
                    cp.wait()

            rows = pl.multiple_of(t * (4 * TM), 4 * TM)
            xst[slot] = get_rows(buf, rows, TM, 4, 0).astype(BF16)
            qst[slot] = get_rows(buf, rows, TM, 4, 2).astype(BF16)
            for cp in copies(t, slot):
                cp.start()
            return c

        lax.fori_loop(0, n_tiles, convert, 0)
        for back in range(QUEUE, 0, -1):
            for cp in copies(n_tiles - back, lax.rem(n_tiles - back, QUEUE)):
                cp.wait()


def route_specs(top_k, n_blocks, first=0):
    def spec(r):
        return pl.BlockSpec((BT,), lambda i: (r * n_blocks + jnp.clip(i - first, 0, n_blocks - 1),), memory_space=pltpu.SMEM)

    return [spec(r) for r in range(top_k)]


def gate_spec(top_k, n_blocks, first=0, skip=0):
    return pl.BlockSpec((top_k, BT), lambda i: (0, skip + jnp.clip(i - first, 0, n_blocks - 1)))


def pre_bwd(pos, tab, gates, x, g, w1, w2, rows, n_exp, top_k):
    n_tok, hid = x.shape
    n_blocks = n_tok // BT
    smem = pl.BlockSpec(memory_space=pltpu.SMEM)
    blk = pl.BlockSpec((BT, hid), lambda i: (i, 0))
    whole = pl.BlockSpec((hid, hid), lambda i: (0, 0))
    return pl.pallas_call(
        functools.partial(pre_bwd_kernel, n_blocks=n_blocks, top_k=top_k, n_exp=n_exp),
        grid=(n_blocks,),
        in_specs=[*route_specs(top_k, n_blocks), smem, gate_spec(top_k, n_blocks), blk, blk, whole, whole],
        out_specs=[blk, pl.BlockSpec(memory_space=pl.ANY), pl.BlockSpec(memory_space=pl.ANY)],
        out_shape=(
            jax.ShapeDtypeStruct((n_tok, hid), BF16),
            jax.ShapeDtypeStruct((rows, hid), BF16),
            jax.ShapeDtypeStruct((rows, hid), BF16),
        ),
        scratch_shapes=[
            pltpu.VMEM((4 * rows + 8, hid // 2), F32),
            pltpu.VMEM((top_k, 4 * BT, hid // 2), F32),
            pltpu.VMEM((QUEUE, TM, hid), BF16),
            pltpu.VMEM((QUEUE, TM, hid), BF16),
            pltpu.SemaphoreType.DMA((2, QUEUE)),
        ],
        compiler_params=pltpu.CompilerParams(vmem_limit_bytes=VMEM_LIMIT),
        cost_estimate=pl.CostEstimate(flops=30_000_000_000, bytes_accessed=30_000_000, transcendentals=0),
        name="pre_bwd",
    )(*[pos] * top_k, tab, gates, x, g, w1, w2)


def exp_bwd_kernel(first_ref, tab_ref, xs_hbm, qs_hbm, *refs, n_parts, has_init):
    w_hbm, refs = refs[:n_parts], refs[n_parts:]
    init_hbm, refs = (refs[:1], refs[1:]) if has_init else ((), refs)
    per = w_hbm[0].shape[0]
    n_loc = n_parts * per
    rs_hbm, dw_hbm, wb, dwb, xb, qb, rb, mid, sems, wsems, dsems, isems = refs
    first = first_ref[0]
    begin = tab_ref[0, first]
    end = tab_ref[0, first + n_loc]

    def rows_of(t):
        return pl.ds(pl.multiple_of(t * TM, TM), TM)

    def loads(t):
        slot = lax.rem(t, DEPTH)
        return (
            pltpu.make_async_copy(xs_hbm.at[rows_of(t)], xb.at[slot], sems.at[0, slot]),
            pltpu.make_async_copy(qs_hbm.at[rows_of(t)], qb.at[slot], sems.at[1, slot]),
        )

    def save(t):
        slot = lax.rem(t, DEPTH)
        return pltpu.make_async_copy(rb.at[slot], rs_hbm.at[rows_of(t)], sems.at[2, slot])

    def w_loads(e, part=0, at=0):
        copies = [pltpu.make_async_copy(w_hbm[part].at[at], wb.at[e], wsems.at[e])]
        return copies + [pltpu.make_async_copy(ref.at[:, e], dwb.at[:, e], isems.at[e]) for ref in init_hbm]

    def dw_save(e):
        return pltpu.make_async_copy(dwb.at[:, e], dw_hbm.at[:, e], dsems.at[e])

    def first_half(t, e):
        slot = lax.rem(t, DEPTH)
        x = xb[slot]
        pre = dot(x, wb[e, 0])
        up = dot(x, wb[e, 1])
        da = dot_nt(qb[slot], wb[e, 2]).astype(BF16).astype(F32)
        sig = jax.nn.sigmoid(pre)
        sil = pre * sig
        return (
            (sil * up).astype(BF16),
            (da * up * (sig * (1.0 + pre * (1.0 - sig)))).astype(BF16),
            (da * sil).astype(BF16),
        )

    def keep(t, vals):
        for i, v in enumerate(vals):
            mid[lax.rem(t, 2), i] = v

    for cp in w_loads(0):
        cp.start()
    for ahead in range(DEPTH - 1):
        for cp in loads(begin + ahead):
            cp.start()
    for e in range(1, n_loc):
        for cp in w_loads(e, e // per, e % per):
            cp.start()
    if not has_init:
        def clear(e, c):
            for i in range(3):
                dwb[i, e] = jnp.zeros(dwb.shape[2:], F32)
            return c

        lax.fori_loop(0, n_loc, clear, 0)
    for cp in w_loads(0):
        cp.wait()
    for cp in loads(begin):
        cp.wait()
    keep(begin, first_half(begin, 0))

    def body(t, e):
        slot = lax.rem(t, DEPTH)
        more = t + 1 < end
        changes = t + 1 >= tab_ref[0, first + e + 1]
        then = jnp.where(changes & more, e + 1, e)

        @pl.when(changes & more)
        def _():
            for cp in w_loads(then):
                cp.wait()

        @pl.when(t + (DEPTH - 1) < end)
        def _():
            for cp in loads(t + (DEPTH - 1)):
                cp.start()

        @pl.when(more)
        def _():
            for cp in loads(t + 1):
                cp.wait()

        @pl.when(t >= begin + DEPTH)
        def _():
            save(t - DEPTH).wait()

        act, dpre, dup = mid[lax.rem(t, 2), 0], mid[lax.rem(t, 2), 1], mid[lax.rem(t, 2), 2]
        x = xb[slot]
        rows = (dot_nt(dpre, wb[e, 0]) + dot_nt(dup, wb[e, 1])).astype(BF16)
        upcoming = first_half(jnp.minimum(t + 1, end - 1), then)
        grads = (dot_tn(x, dpre), dot_tn(x, dup), dot_tn(act, qb[slot]))
        rb[slot] = rows
        for i, grad in enumerate(grads):
            dwb[i, e] += grad
        keep(t + 1, upcoming)
        save(t).start()

        @pl.when(changes)
        def _():
            dw_save(e).start()

        return then

    lax.fori_loop(begin, end, body, 0)
    for back in range(DEPTH, 0, -1):
        save(end - back).wait()
    for e in range(n_loc):
        dw_save(e).wait()


def exp_bwd(first, tab, weights, xs, qs, init=()):
    per, _, hid, ff = weights[0].shape
    n_loc = per * len(weights)
    smem = pl.BlockSpec(memory_space=pltpu.SMEM)
    hbm = pl.BlockSpec(memory_space=pl.ANY)
    return pl.pallas_call(
        functools.partial(exp_bwd_kernel, n_parts=len(weights), has_init=bool(init)),
        in_specs=[smem, smem] + [hbm] * (2 + len(weights) + len(init)),
        out_specs=[hbm, hbm],
        out_shape=(jax.ShapeDtypeStruct(xs.shape, BF16), jax.ShapeDtypeStruct((3, n_loc, hid, ff), F32)),
        input_output_aliases={2: 0},
        scratch_shapes=[
            pltpu.VMEM((n_loc, 3, hid, ff), BF16),
            pltpu.VMEM((3, n_loc, hid, ff), F32),
            pltpu.VMEM((DEPTH, TM, hid), BF16),
            pltpu.VMEM((DEPTH, TM, hid), BF16),
            pltpu.VMEM((DEPTH, TM, hid), BF16),
            pltpu.VMEM((2, 3, TM, ff), BF16),
            pltpu.SemaphoreType.DMA((3, DEPTH)),
            pltpu.SemaphoreType.DMA((n_loc,)),
            pltpu.SemaphoreType.DMA((n_loc,)),
            pltpu.SemaphoreType.DMA((n_loc,)),
        ],
        compiler_params=pltpu.CompilerParams(vmem_limit_bytes=VMEM_LIMIT),
        cost_estimate=pl.CostEstimate(flops=8_000_000_000, bytes_accessed=20_000_000, transcendentals=0),
        name="exp_bwd",
    )(first, tab, xs, qs, *weights, *init)


def post_bwd_kernel(*refs, n_blocks, top_k, n_exp, rows):
    pos_refs, refs = refs[:top_k], refs[top_k:]
    tab_ref, x_ref, g_ref, h_ref, w1_ref, w2_ref, rs_hbm, dx_ref, rbuf, acc, st, sems = refs

    @pl.when(pl.program_id(0) == 0)
    def _():
        n_tiles = tab_ref[0, n_exp]

        def load(t):
            slot = lax.rem(t, (2 * QUEUE))
            return pltpu.make_async_copy(rs_hbm.at[pl.ds(pl.multiple_of(t * TM, TM), TM)], st.at[slot], sems.at[slot])

        for ahead in range((2 * QUEUE) - 1):
            load(ahead).start()
        rbuf[2 * rows : 2 * rows + 8, :] = jnp.zeros((8, rbuf.shape[1]), F32)

        def expand(t, c):
            @pl.when(t + ((2 * QUEUE) - 1) < n_tiles)
            def _():
                load(t + ((2 * QUEUE) - 1)).start()

            load(t).wait()
            put_rows(rbuf, pl.multiple_of(t * (2 * TM), 2 * TM), st[lax.rem(t, (2 * QUEUE))].astype(F32))
            return c

        lax.fori_loop(0, n_tiles, expand, 0)

    gather_rows(rbuf, acc, pos_refs)
    dn = get_rows(acc.at[0], 0, BT)
    for r in range(1, top_k):
        dn = dn + get_rows(acc.at[r], 0, BT)
    xf = x_ref[...].astype(F32)
    u = dot((xf * rms_scale(xf)).astype(BF16), w1_ref[...])
    dh = g_ref[...].astype(F32) + rms_back(h_ref[...].astype(F32), dn)
    sig = jax.nn.sigmoid(u)
    du = (dot_nt(dh.astype(BF16), w2_ref[...]) * (sig * (1.0 + u * (1.0 - sig)))).astype(BF16)
    dx_ref[...] = (dh + rms_back(xf, dot_nt(du, w1_ref[...]))).astype(BF16)


def post_bwd(pos, tab, x, g, h, w1, w2, rs, n_exp, top_k):
    n_tok, hid = x.shape
    rows = rs.shape[0]
    n_blocks = n_tok // BT
    smem = pl.BlockSpec(memory_space=pltpu.SMEM)
    blk = pl.BlockSpec((BT, hid), lambda i: (i, 0))
    whole = pl.BlockSpec((hid, hid), lambda i: (0, 0))
    return pl.pallas_call(
        functools.partial(post_bwd_kernel, n_blocks=n_blocks, top_k=top_k, n_exp=n_exp, rows=rows),
        grid=(n_blocks,),
        in_specs=[*route_specs(top_k, n_blocks), smem, blk, blk, blk, whole, whole, pl.BlockSpec(memory_space=pl.ANY)],
        out_specs=blk,
        out_shape=jax.ShapeDtypeStruct((n_tok, hid), BF16),
        scratch_shapes=[
            pltpu.VMEM((2 * rows + 8, hid // 2), F32),
            pltpu.VMEM((top_k, 2 * BT, hid // 2), F32),
            pltpu.VMEM(((2 * QUEUE), TM, hid), BF16),
            pltpu.SemaphoreType.DMA(((2 * QUEUE),)),
        ],
        compiler_params=pltpu.CompilerParams(vmem_limit_bytes=VMEM_LIMIT),
        cost_estimate=pl.CostEstimate(flops=30_000_000_000, bytes_accessed=30_000_000, transcendentals=0),
        name="post_bwd",
    )(*[pos] * top_k, tab, x, g, h, w1, w2, rs)


def fwd_kernel(*refs, n_blocks, top_k, n_exp, n_groups, rows):
    pos_refs, pos_out_refs, refs = refs[:top_k], refs[top_k : 2 * top_k], refs[2 * top_k :]
    firsts_ref, tab_ref, gate_ref, x_ref, w1_ref, w2_ref, *rest = refs
    w_hbm = rest[:n_groups]
    y_ref, buf, acc, hsc, wsc, mid, sems = rest[n_groups:]
    nsc = acc.at[0]
    step = pl.program_id(0)

    def w_copy(i):
        return pltpu.make_async_copy(w_hbm[i], wsc.at[pl.ds(firsts_ref[i], w_hbm[i].shape[0])], sems.at[i])

    @pl.when(step == 0)
    def _():
        for i in range(n_groups):
            w_copy(i).start()
        zero_tails(buf, tab_ref, n_exp, 2)

    @pl.when(step < n_blocks)
    def _():
        h = dense_forward(x_ref[...].astype(F32), w1_ref[...], w2_ref[...])
        base = step * BT
        hsc[pl.ds(pl.multiple_of(base, BT), BT), :] = h
        hf = h.astype(F32)
        put_rows(nsc, 0, (hf * rms_scale(hf)).astype(BF16).astype(F32))

        scatter_rows(nsc, buf, pos_refs, 2, True)

    @pl.when(step == n_blocks)
    def _():
        buf[2 * rows : 2 * rows + 8, :] = jnp.zeros((8, buf.shape[1]), F32)
        for i in range(n_groups):
            w_copy(i).wait()
        end = tab_ref[0, n_exp]

        def rows_of(t):
            return get_rows(buf, pl.multiple_of(t * (2 * TM), 2 * TM), TM).astype(BF16)

        def first_half(x, e):
            pre = dot(x, wsc[e, 0])
            up = dot(x, wsc[e, 1])
            return (pre * jax.nn.sigmoid(pre) * up).astype(BF16)

        def expert_of(t, e):
            return jnp.where((t >= tab_ref[0, e + 1]) & (t < end), e + 1, e)

        def second(t):
            return jnp.minimum(t, end - 1)

        spare = 2 * rows + 8
        mid[0, 0] = first_half(rows_of(0), 0)
        mid[0, 1] = first_half(rows_of(second(1)), expert_of(1, 0))

        def body(i, experts):
            t = 2 * i
            slot = lax.rem(i, 2)
            e2 = expert_of(t + 2, experts[1])
            e3 = expert_of(t + 3, e2)
            x2, x3 = rows_of(second(t + 2)), rows_of(second(t + 3))
            outs = [dot(mid[slot, k], wsc[experts[k], 2]).astype(BF16).astype(F32) for k in range(2)]
            acts = [first_half(x2, e2), first_half(x3, e3)]
            put_rows(buf, pl.multiple_of(t * (2 * TM), 2 * TM), outs[0])
            put_rows(buf, pl.multiple_of(jnp.where(t + 1 < end, (t + 1) * (2 * TM), spare), 8), outs[1])
            for k in range(2):
                mid[1 - slot, k] = acts[k]
            return e2, e3

        lax.fori_loop(0, lax.div(end + 1, 2), body, (jnp.int32(0), expert_of(1, 0)))

    @pl.when(step > n_blocks)
    def _():
        base = (step - n_blocks - 1) * BT

        gather_rows(buf, acc, pos_out_refs)
        gates = gate_ref[...].astype(F32).T
        h = hsc[pl.ds(pl.multiple_of(base, BT), BT), :]
        mix = get_rows(acc.at[0], 0, BT) * gates[:, 0:1]
        for r in range(1, top_k):
            mix = mix + get_rows(acc.at[r], 0, BT) * gates[:, r : r + 1]
        y_ref[...] = (h.astype(F32) + mix).astype(BF16)


def fwd(n_blocks, skip, firsts, tab, pos, gates, x, w1, w2, weights, rows, n_exp, top_k):
    n_tok, hid = n_blocks * BT, x.shape[1]
    n_groups = len(weights)
    smem = pl.BlockSpec(memory_space=pltpu.SMEM)
    whole = pl.BlockSpec((hid, hid), lambda i: (0, 0))
    return pl.pallas_call(
        functools.partial(fwd_kernel, n_blocks=n_blocks, top_k=top_k, n_exp=n_exp, n_groups=n_groups, rows=rows),
        grid=(2 * n_blocks + 1,),
        in_specs=[*route_specs(top_k, n_blocks), *route_specs(top_k, n_blocks, n_blocks + 1), smem, smem, gate_spec(top_k, n_blocks, n_blocks + 1, skip)]
        + [pl.BlockSpec((BT, hid), lambda i: (skip + jnp.minimum(i, n_blocks - 1), 0)), whole, whole]
        + [pl.BlockSpec(memory_space=pl.ANY)] * n_groups,
        out_specs=pl.BlockSpec((BT, hid), lambda i: (jnp.maximum(i - n_blocks - 1, 0), 0)),
        out_shape=jax.ShapeDtypeStruct((n_tok, hid), BF16),
        scratch_shapes=[
            pltpu.VMEM((2 * rows + 8 + 2 * TM, hid // 2), F32),
            pltpu.VMEM((top_k, 2 * BT, hid // 2), F32),
            pltpu.VMEM((n_tok, hid), BF16),
            pltpu.VMEM((n_exp, 3, hid, hid), BF16),
            pltpu.VMEM((2, 2, TM, hid), BF16),
            pltpu.SemaphoreType.DMA((n_groups,)),
        ],
        compiler_params=pltpu.CompilerParams(vmem_limit_bytes=VMEM_LIMIT),
        cost_estimate=pl.CostEstimate(flops=80_000_000_000, bytes_accessed=30_000_000, transcendentals=0),
        name="fwd",
    )(*[pos] * (2 * top_k), firsts, tab, gates, x, w1, w2, *weights)


def solution(mesh):
    stages = mesh.shape["pp"]
    ep_size = mesh.shape["ep"]
    next_perm = [(i, (i + 1) % stages) for i in range(stages)]
    prev_perm = [(i, (i - 1) % stages) for i in range(stages)]
    mate_perm = [(i, i ^ 1) for i in range(ep_size)]
    chip_perm = [(i, i ^ 2) for i in range(ep_size)]
    tok_spec = P("pp", "ep", None)
    dense_spec = P("pp", None, None)
    expert_spec = P("pp", "ep", None, None)

    def mate(a):
        return lax.ppermute(a, "ep", mate_perm)

    def chip(a):
        return lax.ppermute(a, "ep", chip_perm)

    def slot(x_fwd, ids_fwd, slots_fwd, gates_fwd, x_saved, grad_in, ids_bwd, slots_bwd, gates_bwd, w_one, w_two, w_gate, w_up, w_down):
        x_fwd, ids_fwd, slots_fwd, gates_fwd = x_fwd[0], ids_fwd[0], slots_fwd[0], gates_fwd[0]
        x_saved, grad_in, ids_bwd, slots_bwd, gates_bwd = x_saved[0], grad_in[0], ids_bwd[0], slots_bwd[0], gates_bwd[0]
        w1, w2, w_gate, w_up, w_down = w_one[0], w_two[0], w_gate[0], w_up[0], w_down[0]
        top_k = ids_fwd.shape[1]
        n_loc = w_gate.shape[0]
        n_exp = n_loc * ep_size
        rows = TM * (ids_fwd.size // TM + n_exp)
        rows_f = [TM * (blocks * BT * top_k // TM + n_exp) for blocks in FWD_BLOCKS]
        me = lax.axis_index("ep")

        half = n_loc // 2
        halves = [slice(0, half), slice(half, n_loc)]
        own = [jnp.stack([w[at] for w in (w_gate, w_up, w_down)], axis=1) for at in halves]
        far = [chip(w) for w in own]
        near = [mate(w) for w in own]
        relay = [mate(w) for w in far]
        groups = {
            "own": (me * n_loc, own),
            "near": ((me ^ 1) * n_loc, near),
            "far0": ((me ^ 2) * n_loc, far[:1]),
            "far1": ((me ^ 2) * n_loc + half, far[1:]),
            "relay0": ((me ^ 3) * n_loc, relay[:1]),
            "relay1": ((me ^ 3) * n_loc + half, relay[1:]),
        }

        tab_b, pos4_b, pos2_b, tab_f, pos2_f = route_ranks(ids_bwd, slots_bwd, ids_fwd, slots_fwd, n_exp, rows, rows_f)
        gates_b = gates_bwd.T
        gates_f = gates_fwd.T

        h_bwd, xs, qs = pre_bwd(pos4_b, tab_b, gates_b, x_saved, grad_in, w1, w2, rows, n_exp, top_k)

        def experts(name, xs, init=()):
            first, weights = groups[name]
            return exp_bwd(first.reshape(1), tab_b, weights, xs, qs, init)

        xs, part = experts("relay0", xs)
        far_sum = mate(part)
        xs, part = experts("near", xs)
        near_sum = mate(part)
        xs, part = experts("far0", xs, (far_sum,))
        there = [chip(part)]
        xs, part = experts("relay1", xs)
        far_sum = mate(part)
        xs, dw_own = experts("own", xs, (near_sum,))
        xs, part = experts("far1", xs, (far_sum,))
        there.append(chip(part))
        grad_x = post_bwd(pos2_b, tab_b, x_saved, grad_in, h_bwd, w1, w2, xs, n_exp, top_k)
        x_fwd, grad_x = lax.optimization_barrier((x_fwd, grad_x))
        dx_prev = lax.ppermute(grad_x[None], "pp", prev_perm)

        parts = []
        firsts = jnp.stack([first + i * half for first, ws in groups.values() for i in range(len(ws))])
        weights = [w for _, ws in groups.values() for w in ws]
        skip = 0
        for h, blocks in enumerate(FWD_BLOCKS):
            y_half = fwd(blocks, skip, firsts, tab_f[h], pos2_f[h], gates_f, x_fwd, w1, w2, weights, rows_f[h], n_exp, top_k)
            skip += blocks
            if h + 1 < len(FWD_BLOCKS):
                x_fwd, y_half = lax.optimization_barrier((x_fwd, y_half))
            parts.append(lax.ppermute(y_half, "pp", next_perm))
        y_next = jnp.concatenate(parts, axis=0)[None]
        dws = [jnp.concatenate([dw_own[i, at] + sums[i] for at, sums in zip(halves, there)], axis=0)[None] for i in range(3)]
        dx_prev = jnp.where(me >= 0, dx_prev, jnp.zeros_like(dx_prev))
        return y_next, dx_prev, *dws

    in_specs = (tok_spec,) * 9 + (dense_spec, dense_spec, expert_spec, expert_spec, expert_spec)
    out_specs = (tok_spec, tok_spec, expert_spec, expert_spec, expert_spec)
    return jax.shard_map(slot, mesh=mesh, in_specs=in_specs, out_specs=out_specs, check_vma=False)
```

```python
import functools

import jax
import jax.numpy as jnp
from jax import lax
from jax.experimental import pallas as pl
from jax.experimental.pallas import tpu as pltpu
from jax.sharding import PartitionSpec as P


NORM_EPS = 1e-6
TM = 256
BT = 512
DEPTH = 4
QUEUE = 8
FWD_BLOCKS = (5, 3)
POST_BLOCKS = (4, 4)
F32 = jnp.float32
BF16 = jnp.bfloat16
VMEM_LIMIT = 60 * 1024 * 1024


def dot(a, b):
    return jnp.dot(a, b, preferred_element_type=F32)


def dot_nt(a, b):
    return lax.dot_general(a, b, (((1,), (1,)), ((), ())), preferred_element_type=F32)


def dot_tn(a, b):
    return lax.dot_general(a, b, (((0,), (0,)), ((), ())), preferred_element_type=F32)


def rms_scale(v):
    return lax.rsqrt(jnp.mean(v * v, axis=-1, keepdims=True) + NORM_EPS)


def rms_back(v, dy):
    r = rms_scale(v)
    return r * dy - v * (r * r * r * jnp.mean(dy * v, axis=-1, keepdims=True))


def dense_forward(xf, w1, w2):
    u = dot((xf * rms_scale(xf)).astype(BF16), w1)
    act = (u * jax.nn.sigmoid(u)).astype(BF16)
    return (xf + dot(act, w2)).astype(BF16)


def rank_routes(ids, slots, n_exp, dump):
    ids = jnp.where(slots >= 0, ids, -1)
    n, lanes = ids.shape
    row = lax.broadcasted_iota(jnp.int32, (lanes, lanes), 0)
    col = lax.broadcasted_iota(jnp.int32, (lanes, lanes), 1)
    upper = jnp.where(row < col, 1.0, 0.0).astype(BF16)
    right = jnp.concatenate([upper, jnp.ones((lanes, lanes), BF16)], axis=1)
    row = lax.broadcasted_iota(jnp.int32, (n + 8, n), 0)
    col = lax.broadcasted_iota(jnp.int32, (n + 8, n), 1)
    left = jnp.where((col < row) | (row >= n), 1.0, 0.0).astype(BF16)
    lane = lax.broadcasted_iota(jnp.int32, (n, lanes), 1)
    both = dot(jnp.concatenate([jnp.where(ids == e, 1.0, 0.0).astype(BF16) for e in range(n_exp)], axis=0), right)
    totals = jnp.zeros((n, lanes), F32)
    for e in range(n_exp):
        totals = jnp.where(lane == e, both[e * n : (e + 1) * n, lanes:], totals)
    pre = dot(left, totals.astype(BF16))
    tiles = jnp.maximum(jnp.floor((pre[n:] + (TM - 1.0)) * (1.0 / TM)), 1.0)
    tab = dot(tiles.astype(BF16), upper)
    base = pre[:n] + TM * tab[0:1]
    pos = jnp.full((n, lanes), float(dump), F32)
    for e in range(n_exp):
        pos = jnp.where(ids == e, both[e * n : (e + 1) * n, :lanes] + base[:, e : e + 1], pos)
    return pos, tab.astype(jnp.int32)


def chunks(ref, first, last):
    return jnp.concatenate([ref[r : r + 1, c * 128 : (c + 1) * 128] for r in range(ref.shape[0]) for c in range(first, last)], axis=0)


def rank_kernel(n_exp, rows_b, rows_f, ids_b, slots_b, ids_f, slots_f, tab_b, pos4_b, pos2_b, tab_f, *pos2_f):
    n = ids_b.shape[1] // 128
    pos, tab_b[...] = rank_routes(chunks(ids_b, 0, n), chunks(slots_b, 0, n), n_exp, rows_b)
    pos4_b[...] = (pos * 4.0).astype(jnp.int32)
    pos2_b[...] = (pos * 2.0).astype(jnp.int32)
    first = 0
    for h, (blocks, dump) in enumerate(zip(FWD_BLOCKS, rows_f)):
        last = first + blocks * (BT // 128)
        pos, tab_f[h] = rank_routes(chunks(ids_f, first, last), chunks(slots_f, first, last), n_exp, dump)
        pos2_f[h][...] = (pos * 2.0).astype(jnp.int32)
        first = last


def route_ranks(ids_b, slots_b, ids_f, slots_f, n_exp, rows_b, rows_f):
    def table(n_tok):
        return jax.ShapeDtypeStruct((n_tok * ids_b.shape[1] // 128, 128), jnp.int32)

    n_tok = ids_b.shape[0]
    tab_b, pos4_b, pos2_b, tab_f, *pos2_f = pl.pallas_call(
        functools.partial(rank_kernel, n_exp, rows_b, rows_f),
        out_shape=(
            jax.ShapeDtypeStruct((8, 128), jnp.int32),
            table(n_tok),
            table(n_tok),
            jax.ShapeDtypeStruct((len(FWD_BLOCKS), 8, 128), jnp.int32),
            *[table(blocks * BT) for blocks in FWD_BLOCKS],
        ),
        name="rank",
    )(ids_b.T, slots_b.T, ids_f.T, slots_f.T)
    return tab_b, pos4_b.reshape(-1), pos2_b.reshape(-1), tab_f, [p.reshape(-1) for p in pos2_f]


def put_rows(ref, at, vals, pitch=2, off=0):
    n = vals.shape[0]
    half = vals.shape[1] // 2
    ref[pl.ds(at + off, n, stride=pitch), :] = vals[:, :half]
    ref[pl.ds(at + off + 1, n, stride=pitch), :] = vals[:, half:]


def get_rows(ref, at, n, pitch=2, off=0):
    return jnp.concatenate([ref[pl.ds(at + off + i, n, stride=pitch), :] for i in range(2)], axis=1)


def rows_at(p, n):
    return pl.ds(pl.multiple_of(p, n), n)


def gather_rows(buf, acc, pos_refs):
    unroll = 32

    def body(j, c):
        base = j * unroll
        at = pl.multiple_of(j * (2 * unroll), 2 * unroll)
        for k in range(unroll):
            i = base + k
            for r, pos_ref in enumerate(pos_refs):
                acc[r, pl.ds(at + 2 * k, 2), :] = buf[rows_at(pos_ref[i], 2), :]
        return c

    lax.fori_loop(0, BT // unroll, body, 0)


def scatter_rows(src, buf, pos_refs, n, shared):
    unroll = 32

    def body(j, c):
        base = j * unroll
        at = pl.multiple_of(j * (n * unroll), n * unroll)
        for k in range(unroll):
            i = base + k
            v = src[pl.ds(at + n * k, n), :] if shared else None
            for r, pos_ref in enumerate(pos_refs):
                buf[rows_at(pos_ref[i], n), :] = v if shared else src[r, pl.ds(at + n * k, n), :]
        return c

    lax.fori_loop(0, BT // unroll, body, 0)


def zero_tails(buf, tab_ref, n_exp, pitch):
    def body(e, c):
        at = pl.multiple_of((tab_ref[0, e + 1] - 1) * (pitch * TM), pitch * TM)
        buf[pl.ds(at, pitch * TM), :] = jnp.zeros((pitch * TM, buf.shape[1]), F32)
        return c

    lax.fori_loop(0, n_exp, body, 0)


def pre_bwd_kernel(*refs, n_blocks, top_k, n_exp):
    pos_refs, refs = refs[:top_k], refs[top_k:]
    tab_ref, gate_ref, x_ref, g_ref, w1_ref, w2_ref, h_ref, xs_hbm, qs_hbm, buf, src, xst, qst, sems = refs
    step = pl.program_id(0)

    @pl.when(step == 0)
    def _():
        zero_tails(buf, tab_ref, n_exp, 4)

    h = dense_forward(x_ref[...].astype(F32), w1_ref[...], w2_ref[...])
    h_ref[...] = h
    hf = h.astype(F32)
    n = (hf * rms_scale(hf)).astype(BF16).astype(F32)
    g = g_ref[...].astype(F32)
    gates = gate_ref[...].astype(F32).T
    for r in range(top_k):
        put_rows(src.at[r], 0, n, 4, 0)
        put_rows(src.at[r], 0, g * gates[:, r : r + 1], 4, 2)
    scatter_rows(src, buf, pos_refs, 4, False)

    @pl.when(step == n_blocks - 1)
    def _():
        n_tiles = tab_ref[0, n_exp]

        def copies(t, slot):
            rows = pl.ds(pl.multiple_of(t * TM, TM), TM)
            return (
                pltpu.make_async_copy(xst.at[slot], xs_hbm.at[rows], sems.at[0, slot]),
                pltpu.make_async_copy(qst.at[slot], qs_hbm.at[rows], sems.at[1, slot]),
            )

        def convert(t, c):
            slot = lax.rem(t, QUEUE)

            @pl.when(t >= QUEUE)
            def _():
                for cp in copies(t - QUEUE, slot):
                    cp.wait()

            rows = pl.multiple_of(t * (4 * TM), 4 * TM)
            xst[slot] = get_rows(buf, rows, TM, 4, 0).astype(BF16)
            qst[slot] = get_rows(buf, rows, TM, 4, 2).astype(BF16)
            for cp in copies(t, slot):
                cp.start()
            return c

        lax.fori_loop(0, n_tiles, convert, 0)
        for back in range(QUEUE, 0, -1):
            for cp in copies(n_tiles - back, lax.rem(n_tiles - back, QUEUE)):
                cp.wait()


def route_specs(top_k, n_blocks, first=0, skip=0, total=None):
    def spec(r):
        start = r * (total or n_blocks) + skip
        return pl.BlockSpec((BT,), lambda i: (start + jnp.clip(i - first, 0, n_blocks - 1),), memory_space=pltpu.SMEM)

    return [spec(r) for r in range(top_k)]


def gate_spec(top_k, n_blocks, first=0, skip=0):
    return pl.BlockSpec((top_k, BT), lambda i: (0, skip + jnp.clip(i - first, 0, n_blocks - 1)))


def pre_bwd(pos, tab, gates, x, g, w1, w2, rows, n_exp, top_k):
    n_tok, hid = x.shape
    n_blocks = n_tok // BT
    smem = pl.BlockSpec(memory_space=pltpu.SMEM)
    blk = pl.BlockSpec((BT, hid), lambda i: (i, 0))
    whole = pl.BlockSpec((hid, hid), lambda i: (0, 0))
    return pl.pallas_call(
        functools.partial(pre_bwd_kernel, n_blocks=n_blocks, top_k=top_k, n_exp=n_exp),
        grid=(n_blocks,),
        in_specs=[*route_specs(top_k, n_blocks), smem, gate_spec(top_k, n_blocks), blk, blk, whole, whole],
        out_specs=[blk, pl.BlockSpec(memory_space=pl.ANY), pl.BlockSpec(memory_space=pl.ANY)],
        out_shape=(
            jax.ShapeDtypeStruct((n_tok, hid), BF16),
            jax.ShapeDtypeStruct((rows, hid), BF16),
            jax.ShapeDtypeStruct((rows, hid), BF16),
        ),
        scratch_shapes=[
            pltpu.VMEM((4 * rows + 8, hid // 2), F32),
            pltpu.VMEM((top_k, 4 * BT, hid // 2), F32),
            pltpu.VMEM((QUEUE, TM, hid), BF16),
            pltpu.VMEM((QUEUE, TM, hid), BF16),
            pltpu.SemaphoreType.DMA((2, QUEUE)),
        ],
        compiler_params=pltpu.CompilerParams(vmem_limit_bytes=VMEM_LIMIT),
        cost_estimate=pl.CostEstimate(flops=30_000_000_000, bytes_accessed=30_000_000, transcendentals=0),
        name="pre_bwd",
    )(*[pos] * top_k, tab, gates, x, g, w1, w2)


def exp_bwd_kernel(first_ref, tab_ref, xs_hbm, qs_hbm, *refs, n_parts, has_init):
    w_hbm, refs = refs[:n_parts], refs[n_parts:]
    init_hbm, refs = (refs[:1], refs[1:]) if has_init else ((), refs)
    per = w_hbm[0].shape[0]
    n_loc = n_parts * per
    rs_hbm, dw_hbm, wb, dwb, xb, qb, rb, mid, sems, wsems, dsems, isems = refs
    first = first_ref[0]
    begin = tab_ref[0, first]
    end = tab_ref[0, first + n_loc]

    def rows_of(t):
        return pl.ds(pl.multiple_of(t * TM, TM), TM)

    def loads(t):
        slot = lax.rem(t, DEPTH)
        return (
            pltpu.make_async_copy(xs_hbm.at[rows_of(t)], xb.at[slot], sems.at[0, slot]),
            pltpu.make_async_copy(qs_hbm.at[rows_of(t)], qb.at[slot], sems.at[1, slot]),
        )

    def save(t):
        slot = lax.rem(t, DEPTH)
        return pltpu.make_async_copy(rb.at[slot], rs_hbm.at[rows_of(t)], sems.at[2, slot])

    def w_loads(e, part=0, at=0):
        copies = [pltpu.make_async_copy(w_hbm[part].at[at], wb.at[e], wsems.at[e])]
        return copies + [pltpu.make_async_copy(ref.at[:, e], dwb.at[:, e], isems.at[e]) for ref in init_hbm]

    def dw_save(e):
        return pltpu.make_async_copy(dwb.at[:, e], dw_hbm.at[:, e], dsems.at[e])

    def first_half(t, e):
        slot = lax.rem(t, DEPTH)
        x = xb[slot]
        pre = dot(x, wb[e, 0])
        up = dot(x, wb[e, 1])
        da = dot_nt(qb[slot], wb[e, 2]).astype(BF16).astype(F32)
        sig = jax.nn.sigmoid(pre)
        sil = pre * sig
        return (
            (sil * up).astype(BF16),
            (da * up * (sig * (1.0 + pre * (1.0 - sig)))).astype(BF16),
            (da * sil).astype(BF16),
        )

    def keep(t, vals):
        for i, v in enumerate(vals):
            mid[lax.rem(t, 2), i] = v

    for cp in w_loads(0):
        cp.start()
    for ahead in range(DEPTH - 1):
        for cp in loads(begin + ahead):
            cp.start()
    for e in range(1, n_loc):
        for cp in w_loads(e, e // per, e % per):
            cp.start()
    if not has_init:
        def clear(e, c):
            for i in range(3):
                dwb[i, e] = jnp.zeros(dwb.shape[2:], F32)
            return c

        lax.fori_loop(0, n_loc, clear, 0)
    for cp in w_loads(0):
        cp.wait()
    for cp in loads(begin):
        cp.wait()
    keep(begin, first_half(begin, 0))

    def body(t, e):
        slot = lax.rem(t, DEPTH)
        more = t + 1 < end
        changes = t + 1 >= tab_ref[0, first + e + 1]
        then = jnp.where(changes & more, e + 1, e)

        @pl.when(changes & more)
        def _():
            for cp in w_loads(then):
                cp.wait()

        @pl.when(t + (DEPTH - 1) < end)
        def _():
            for cp in loads(t + (DEPTH - 1)):
                cp.start()

        @pl.when(more)
        def _():
            for cp in loads(t + 1):
                cp.wait()

        @pl.when(t >= begin + DEPTH)
        def _():
            save(t - DEPTH).wait()

        act, dpre, dup = mid[lax.rem(t, 2), 0], mid[lax.rem(t, 2), 1], mid[lax.rem(t, 2), 2]
        x = xb[slot]
        rows = (dot_nt(dpre, wb[e, 0]) + dot_nt(dup, wb[e, 1])).astype(BF16)
        upcoming = first_half(jnp.minimum(t + 1, end - 1), then)
        grads = (dot_tn(x, dpre), dot_tn(x, dup), dot_tn(act, qb[slot]))
        rb[slot] = rows
        for i, grad in enumerate(grads):
            dwb[i, e] += grad
        keep(t + 1, upcoming)
        save(t).start()

        @pl.when(changes)
        def _():
            dw_save(e).start()

        return then

    lax.fori_loop(begin, end, body, 0)
    for back in range(DEPTH, 0, -1):
        save(end - back).wait()
    for e in range(n_loc):
        dw_save(e).wait()


def exp_bwd(first, tab, weights, xs, qs, init=()):
    per, _, hid, ff = weights[0].shape
    n_loc = per * len(weights)
    smem = pl.BlockSpec(memory_space=pltpu.SMEM)
    hbm = pl.BlockSpec(memory_space=pl.ANY)
    return pl.pallas_call(
        functools.partial(exp_bwd_kernel, n_parts=len(weights), has_init=bool(init)),
        in_specs=[smem, smem] + [hbm] * (2 + len(weights) + len(init)),
        out_specs=[hbm, hbm],
        out_shape=(jax.ShapeDtypeStruct(xs.shape, BF16), jax.ShapeDtypeStruct((3, n_loc, hid, ff), F32)),
        input_output_aliases={2: 0},
        scratch_shapes=[
            pltpu.VMEM((n_loc, 3, hid, ff), BF16),
            pltpu.VMEM((3, n_loc, hid, ff), F32),
            pltpu.VMEM((DEPTH, TM, hid), BF16),
            pltpu.VMEM((DEPTH, TM, hid), BF16),
            pltpu.VMEM((DEPTH, TM, hid), BF16),
            pltpu.VMEM((2, 3, TM, ff), BF16),
            pltpu.SemaphoreType.DMA((3, DEPTH)),
            pltpu.SemaphoreType.DMA((n_loc,)),
            pltpu.SemaphoreType.DMA((n_loc,)),
            pltpu.SemaphoreType.DMA((n_loc,)),
        ],
        compiler_params=pltpu.CompilerParams(vmem_limit_bytes=VMEM_LIMIT),
        cost_estimate=pl.CostEstimate(flops=8_000_000_000, bytes_accessed=20_000_000, transcendentals=0),
        name="exp_bwd",
    )(first, tab, xs, qs, *weights, *init)


def post_bwd_kernel(*refs, n_blocks, top_k, n_exp, rows):
    pos_refs, refs = refs[:top_k], refs[top_k:]
    tab_ref, x_ref, g_ref, h_ref, w1_ref, w2_ref, rs_hbm, dx_ref, rbuf, acc, st, sems = refs

    @pl.when(pl.program_id(0) == 0)
    def _():
        n_tiles = tab_ref[0, n_exp]

        def load(t):
            slot = lax.rem(t, (2 * QUEUE))
            return pltpu.make_async_copy(rs_hbm.at[pl.ds(pl.multiple_of(t * TM, TM), TM)], st.at[slot], sems.at[slot])

        for ahead in range((2 * QUEUE) - 1):
            load(ahead).start()
        rbuf[2 * rows : 2 * rows + 8, :] = jnp.zeros((8, rbuf.shape[1]), F32)

        def expand(t, c):
            @pl.when(t + ((2 * QUEUE) - 1) < n_tiles)
            def _():
                load(t + ((2 * QUEUE) - 1)).start()

            load(t).wait()
            put_rows(rbuf, pl.multiple_of(t * (2 * TM), 2 * TM), st[lax.rem(t, (2 * QUEUE))].astype(F32))
            return c

        lax.fori_loop(0, n_tiles, expand, 0)

    gather_rows(rbuf, acc, pos_refs)
    dn = get_rows(acc.at[0], 0, BT)
    for r in range(1, top_k):
        dn = dn + get_rows(acc.at[r], 0, BT)
    xf = x_ref[...].astype(F32)
    u = dot((xf * rms_scale(xf)).astype(BF16), w1_ref[...])
    dh = g_ref[...].astype(F32) + rms_back(h_ref[...].astype(F32), dn)
    sig = jax.nn.sigmoid(u)
    du = (dot_nt(dh.astype(BF16), w2_ref[...]) * (sig * (1.0 + u * (1.0 - sig)))).astype(BF16)
    dx_ref[...] = (dh + rms_back(xf, dot_nt(du, w1_ref[...]))).astype(BF16)


def post_bwd(n_blocks, skip, pos, tab, x, g, h, w1, w2, rs, n_exp, top_k):
    total, hid = x.shape[0] // BT, x.shape[1]
    rows = rs.shape[0]
    smem = pl.BlockSpec(memory_space=pltpu.SMEM)
    blk = pl.BlockSpec((BT, hid), lambda i: (skip + i, 0))
    whole = pl.BlockSpec((hid, hid), lambda i: (0, 0))
    return pl.pallas_call(
        functools.partial(post_bwd_kernel, n_blocks=n_blocks, top_k=top_k, n_exp=n_exp, rows=rows),
        grid=(n_blocks,),
        in_specs=[*route_specs(top_k, n_blocks, 0, skip, total), smem, blk, blk, blk, whole, whole, pl.BlockSpec(memory_space=pl.ANY)],
        out_specs=pl.BlockSpec((BT, hid), lambda i: (i, 0)),
        out_shape=jax.ShapeDtypeStruct((n_blocks * BT, hid), BF16),
        scratch_shapes=[
            pltpu.VMEM((2 * rows + 8, hid // 2), F32),
            pltpu.VMEM((top_k, 2 * BT, hid // 2), F32),
            pltpu.VMEM(((2 * QUEUE), TM, hid), BF16),
            pltpu.SemaphoreType.DMA(((2 * QUEUE),)),
        ],
        compiler_params=pltpu.CompilerParams(vmem_limit_bytes=VMEM_LIMIT),
        cost_estimate=pl.CostEstimate(flops=30_000_000_000, bytes_accessed=30_000_000, transcendentals=0),
        name="post_bwd",
    )(*[pos] * top_k, tab, x, g, h, w1, w2, rs)


def fwd_kernel(*refs, n_blocks, top_k, n_exp, n_groups, rows):
    pos_refs, pos_out_refs, refs = refs[:top_k], refs[top_k : 2 * top_k], refs[2 * top_k :]
    firsts_ref, tab_ref, gate_ref, x_ref, w1_ref, w2_ref, *rest = refs
    w_hbm = rest[:n_groups]
    y_ref, buf, acc, hsc, wsc, mid, sems = rest[n_groups:]
    nsc = acc.at[0]
    step = pl.program_id(0)

    def w_copy(i):
        return pltpu.make_async_copy(w_hbm[i], wsc.at[pl.ds(firsts_ref[i], w_hbm[i].shape[0])], sems.at[i])

    @pl.when(step == 0)
    def _():
        for i in range(n_groups):
            w_copy(i).start()
        zero_tails(buf, tab_ref, n_exp, 2)

    @pl.when(step < n_blocks)
    def _():
        h = dense_forward(x_ref[...].astype(F32), w1_ref[...], w2_ref[...])
        base = step * BT
        hsc[pl.ds(pl.multiple_of(base, BT), BT), :] = h
        hf = h.astype(F32)
        put_rows(nsc, 0, (hf * rms_scale(hf)).astype(BF16).astype(F32))

        scatter_rows(nsc, buf, pos_refs, 2, True)

    @pl.when(step == n_blocks)
    def _():
        buf[2 * rows : 2 * rows + 8, :] = jnp.zeros((8, buf.shape[1]), F32)
        for i in range(n_groups):
            w_copy(i).wait()
        end = tab_ref[0, n_exp]

        def rows_of(t):
            return get_rows(buf, pl.multiple_of(t * (2 * TM), 2 * TM), TM).astype(BF16)

        def first_half(x, e):
            pre = dot(x, wsc[e, 0])
            up = dot(x, wsc[e, 1])
            return (pre * jax.nn.sigmoid(pre) * up).astype(BF16)

        def expert_of(t, e):
            return jnp.where((t >= tab_ref[0, e + 1]) & (t < end), e + 1, e)

        def second(t):
            return jnp.minimum(t, end - 1)

        spare = 2 * rows + 8
        mid[0, 0] = first_half(rows_of(0), 0)
        mid[0, 1] = first_half(rows_of(second(1)), expert_of(1, 0))

        def body(i, experts):
            t = 2 * i
            slot = lax.rem(i, 2)
            e2 = expert_of(t + 2, experts[1])
            e3 = expert_of(t + 3, e2)
            x2, x3 = rows_of(second(t + 2)), rows_of(second(t + 3))
            outs = [dot(mid[slot, k], wsc[experts[k], 2]).astype(BF16).astype(F32) for k in range(2)]
            acts = [first_half(x2, e2), first_half(x3, e3)]
            put_rows(buf, pl.multiple_of(t * (2 * TM), 2 * TM), outs[0])
            put_rows(buf, pl.multiple_of(jnp.where(t + 1 < end, (t + 1) * (2 * TM), spare), 8), outs[1])
            for k in range(2):
                mid[1 - slot, k] = acts[k]
            return e2, e3

        lax.fori_loop(0, lax.div(end + 1, 2), body, (jnp.int32(0), expert_of(1, 0)))

    @pl.when(step > n_blocks)
    def _():
        base = (step - n_blocks - 1) * BT

        gather_rows(buf, acc, pos_out_refs)
        gates = gate_ref[...].astype(F32).T
        h = hsc[pl.ds(pl.multiple_of(base, BT), BT), :]
        mix = get_rows(acc.at[0], 0, BT) * gates[:, 0:1]
        for r in range(1, top_k):
            mix = mix + get_rows(acc.at[r], 0, BT) * gates[:, r : r + 1]
        y_ref[...] = (h.astype(F32) + mix).astype(BF16)


def fwd(n_blocks, skip, firsts, tab, pos, gates, x, w1, w2, weights, rows, n_exp, top_k):
    n_tok, hid = n_blocks * BT, x.shape[1]
    n_groups = len(weights)
    smem = pl.BlockSpec(memory_space=pltpu.SMEM)
    whole = pl.BlockSpec((hid, hid), lambda i: (0, 0))
    return pl.pallas_call(
        functools.partial(fwd_kernel, n_blocks=n_blocks, top_k=top_k, n_exp=n_exp, n_groups=n_groups, rows=rows),
        grid=(2 * n_blocks + 1,),
        in_specs=[*route_specs(top_k, n_blocks), *route_specs(top_k, n_blocks, n_blocks + 1), smem, smem, gate_spec(top_k, n_blocks, n_blocks + 1, skip)]
        + [pl.BlockSpec((BT, hid), lambda i: (skip + jnp.minimum(i, n_blocks - 1), 0)), whole, whole]
        + [pl.BlockSpec(memory_space=pl.ANY)] * n_groups,
        out_specs=pl.BlockSpec((BT, hid), lambda i: (jnp.maximum(i - n_blocks - 1, 0), 0)),
        out_shape=jax.ShapeDtypeStruct((n_tok, hid), BF16),
        scratch_shapes=[
            pltpu.VMEM((2 * rows + 8 + 2 * TM, hid // 2), F32),
            pltpu.VMEM((top_k, 2 * BT, hid // 2), F32),
            pltpu.VMEM((n_tok, hid), BF16),
            pltpu.VMEM((n_exp, 3, hid, hid), BF16),
            pltpu.VMEM((2, 2, TM, hid), BF16),
            pltpu.SemaphoreType.DMA((n_groups,)),
        ],
        compiler_params=pltpu.CompilerParams(vmem_limit_bytes=VMEM_LIMIT),
        cost_estimate=pl.CostEstimate(flops=80_000_000_000, bytes_accessed=30_000_000, transcendentals=0),
        name="fwd",
    )(*[pos] * (2 * top_k), firsts, tab, gates, x, w1, w2, *weights)


def solution(mesh):
    stages = mesh.shape["pp"]
    ep_size = mesh.shape["ep"]
    next_perm = [(i, (i + 1) % stages) for i in range(stages)]
    prev_perm = [(i, (i - 1) % stages) for i in range(stages)]
    mate_perm = [(i, i ^ 1) for i in range(ep_size)]
    chip_perm = [(i, i ^ 2) for i in range(ep_size)]
    tok_spec = P("pp", "ep", None)
    dense_spec = P("pp", None, None)
    expert_spec = P("pp", "ep", None, None)

    def mate(a):
        return lax.ppermute(a, "ep", mate_perm)

    def chip(a):
        return lax.ppermute(a, "ep", chip_perm)

    def slot(x_fwd, ids_fwd, slots_fwd, gates_fwd, x_saved, grad_in, ids_bwd, slots_bwd, gates_bwd, w_one, w_two, w_gate, w_up, w_down):
        x_fwd, ids_fwd, slots_fwd, gates_fwd = x_fwd[0], ids_fwd[0], slots_fwd[0], gates_fwd[0]
        x_saved, grad_in, ids_bwd, slots_bwd, gates_bwd = x_saved[0], grad_in[0], ids_bwd[0], slots_bwd[0], gates_bwd[0]
        w1, w2, w_gate, w_up, w_down = w_one[0], w_two[0], w_gate[0], w_up[0], w_down[0]
        top_k = ids_fwd.shape[1]
        n_loc = w_gate.shape[0]
        n_exp = n_loc * ep_size
        rows = TM * (ids_fwd.size // TM + n_exp)
        rows_f = [TM * (blocks * BT * top_k // TM + n_exp) for blocks in FWD_BLOCKS]
        me = lax.axis_index("ep")

        half = n_loc // 2
        halves = [slice(0, half), slice(half, n_loc)]
        own = [jnp.stack([w[at] for w in (w_gate, w_up, w_down)], axis=1) for at in halves]
        far = [chip(w) for w in own]
        near = [mate(w) for w in own]
        relay = [mate(w) for w in far]
        groups = {
            "own": (me * n_loc, own),
            "near": ((me ^ 1) * n_loc, near),
            "far0": ((me ^ 2) * n_loc, far[:1]),
            "far1": ((me ^ 2) * n_loc + half, far[1:]),
            "relay0": ((me ^ 3) * n_loc, relay[:1]),
            "relay1": ((me ^ 3) * n_loc + half, relay[1:]),
        }

        tab_b, pos4_b, pos2_b, tab_f, pos2_f = route_ranks(ids_bwd, slots_bwd, ids_fwd, slots_fwd, n_exp, rows, rows_f)
        gates_b = gates_bwd.T
        gates_f = gates_fwd.T

        h_bwd, xs, qs = pre_bwd(pos4_b, tab_b, gates_b, x_saved, grad_in, w1, w2, rows, n_exp, top_k)

        def experts(name, xs, init=()):
            first, weights = groups[name]
            return exp_bwd(first.reshape(1), tab_b, weights, xs, qs, init)

        xs, part = experts("relay0", xs)
        far_sum = mate(part)
        xs, part = experts("near", xs)
        near_sum = mate(part)
        xs, part = experts("far0", xs, (far_sum,))
        there = [chip(part)]
        xs, part = experts("relay1", xs)
        far_sum = mate(part)
        xs, dw_own = experts("own", xs, (near_sum,))
        xs, part = experts("far1", xs, (far_sum,))
        there.append(chip(part))

        def chained(calls, perm, blocks_of, x_in):
            pieces, skip = [], 0
            for h, blocks in enumerate(blocks_of):
                piece = calls(h, blocks, skip, x_in)
                skip += blocks
                x_in, piece = lax.optimization_barrier((x_in, piece))
                pieces.append(lax.ppermute(piece, "pp", perm))
            return pieces, x_in

        def post_part(h, blocks, skip, x_in):
            return post_bwd(blocks, skip, pos2_b, tab_b, x_saved, grad_in, h_bwd, w1, w2, x_in, n_exp, top_k)

        dx_parts, xs = chained(post_part, prev_perm, POST_BLOCKS, xs)
        x_fwd, xs = lax.optimization_barrier((x_fwd, xs))

        firsts = jnp.stack([first + i * half for first, ws in groups.values() for i in range(len(ws))])
        weights = [w for _, ws in groups.values() for w in ws]

        def fwd_part(h, blocks, skip, x_in):
            return fwd(blocks, skip, firsts, tab_f[h], pos2_f[h], gates_f, x_in, w1, w2, weights, rows_f[h], n_exp, top_k)

        parts, _ = chained(fwd_part, next_perm, FWD_BLOCKS, x_fwd)
        y_next = jnp.concatenate(parts, axis=0)[None]
        dws = [jnp.concatenate([dw_own[i, at] + sums[i] for at, sums in zip(halves, there)], axis=0)[None] for i in range(3)]
        dx_prev = jnp.concatenate(dx_parts, axis=0)[None]
        return y_next, dx_prev, *dws

    in_specs = (tok_spec,) * 9 + (dense_spec, dense_spec, expert_spec, expert_spec, expert_spec)
    out_specs = (tok_spec, tok_spec, expert_spec, expert_spec, expert_spec)
    return jax.shard_map(slot, mesh=mesh, in_specs=in_specs, out_specs=out_specs, check_vma=False)
```

```python
import functools

import jax
import jax.numpy as jnp
from jax import lax
from jax.experimental import pallas as pl
from jax.experimental.pallas import tpu as pltpu
from jax.sharding import PartitionSpec as P


NORM_EPS = 1e-6
TM = 256
BT = 512
DEPTH = 4
QUEUE = 8
FWD_BLOCKS = (4, 4)
POST_BLOCKS = (6, 2)
F32 = jnp.float32
BF16 = jnp.bfloat16
VMEM_LIMIT = 60 * 1024 * 1024


def dot(a, b):
    return jnp.dot(a, b, preferred_element_type=F32)


def dot_nt(a, b):
    return lax.dot_general(a, b, (((1,), (1,)), ((), ())), preferred_element_type=F32)


def dot_tn(a, b):
    return lax.dot_general(a, b, (((0,), (0,)), ((), ())), preferred_element_type=F32)


def rms_scale(v):
    return lax.rsqrt(jnp.mean(v * v, axis=-1, keepdims=True) + NORM_EPS)


def rms_back(v, dy):
    r = rms_scale(v)
    return r * dy - v * (r * r * r * jnp.mean(dy * v, axis=-1, keepdims=True))


def dense_forward(xf, w1, w2):
    u = dot((xf * rms_scale(xf)).astype(BF16), w1)
    act = (u * jax.nn.sigmoid(u)).astype(BF16)
    return (xf + dot(act, w2)).astype(BF16)


def rank_routes(ids, slots, n_exp, dump):
    ids = jnp.where(slots >= 0, ids, -1)
    n, lanes = ids.shape
    row = lax.broadcasted_iota(jnp.int32, (lanes, lanes), 0)
    col = lax.broadcasted_iota(jnp.int32, (lanes, lanes), 1)
    upper = jnp.where(row < col, 1.0, 0.0).astype(BF16)
    right = jnp.concatenate([upper, jnp.ones((lanes, lanes), BF16)], axis=1)
    row = lax.broadcasted_iota(jnp.int32, (n + 8, n), 0)
    col = lax.broadcasted_iota(jnp.int32, (n + 8, n), 1)
    left = jnp.where((col < row) | (row >= n), 1.0, 0.0).astype(BF16)
    lane = lax.broadcasted_iota(jnp.int32, (n, lanes), 1)
    both = dot(jnp.concatenate([jnp.where(ids == e, 1.0, 0.0).astype(BF16) for e in range(n_exp)], axis=0), right)
    totals = jnp.zeros((n, lanes), F32)
    for e in range(n_exp):
        totals = jnp.where(lane == e, both[e * n : (e + 1) * n, lanes:], totals)
    pre = dot(left, totals.astype(BF16))
    tiles = jnp.maximum(jnp.floor((pre[n:] + (TM - 1.0)) * (1.0 / TM)), 1.0)
    tab = dot(tiles.astype(BF16), upper)
    base = pre[:n] + TM * tab[0:1]
    pos = jnp.full((n, lanes), float(dump), F32)
    for e in range(n_exp):
        pos = jnp.where(ids == e, both[e * n : (e + 1) * n, :lanes] + base[:, e : e + 1], pos)
    return pos, tab.astype(jnp.int32)


def chunks(ref, first, last):
    return jnp.concatenate([ref[r : r + 1, c * 128 : (c + 1) * 128] for r in range(ref.shape[0]) for c in range(first, last)], axis=0)


def rank_kernel(n_exp, blocks_of, dumps, scales, ids, slots, tab, *tables):
    first = 0
    for h, (blocks, dump) in enumerate(zip(blocks_of, dumps)):
        last = first + blocks * (BT // 128)
        pos, tab[h] = rank_routes(chunks(ids, first, last), chunks(slots, first, last), n_exp, dump)
        for k, scale in enumerate(scales):
            tables[h * len(scales) + k][...] = (pos * scale).astype(jnp.int32)
        first = last


def route_ranks(ids, slots, n_exp, blocks_of, dumps, scales):
    tables = [jax.ShapeDtypeStruct((blocks * BT * ids.shape[1] // 128, 128), jnp.int32) for blocks in blocks_of for _ in scales]
    tab, *pos = pl.pallas_call(
        functools.partial(rank_kernel, n_exp, blocks_of, dumps, scales),
        out_shape=(jax.ShapeDtypeStruct((len(blocks_of), 8, 128), jnp.int32), *tables),
        name="rank",
    )(ids.T, slots.T)
    return tab, [p.reshape(-1) for p in pos]


def put_rows(ref, at, vals, pitch=2, off=0):
    n = vals.shape[0]
    half = vals.shape[1] // 2
    ref[pl.ds(at + off, n, stride=pitch), :] = vals[:, :half]
    ref[pl.ds(at + off + 1, n, stride=pitch), :] = vals[:, half:]


def get_rows(ref, at, n, pitch=2, off=0):
    return jnp.concatenate([ref[pl.ds(at + off + i, n, stride=pitch), :] for i in range(2)], axis=1)


def rows_at(p, n):
    return pl.ds(pl.multiple_of(p, n), n)


def gather_rows(buf, acc, pos_refs):
    unroll = 32

    def body(j, c):
        base = j * unroll
        at = pl.multiple_of(j * (2 * unroll), 2 * unroll)
        for k in range(unroll):
            i = base + k
            for r, pos_ref in enumerate(pos_refs):
                acc[r, pl.ds(at + 2 * k, 2), :] = buf[rows_at(pos_ref[i], 2), :]
        return c

    lax.fori_loop(0, BT // unroll, body, 0)


def scatter_rows(src, buf, pos_refs, n, shared):
    unroll = 32

    def body(j, c):
        base = j * unroll
        at = pl.multiple_of(j * (n * unroll), n * unroll)
        for k in range(unroll):
            i = base + k
            v = src[pl.ds(at + n * k, n), :] if shared else None
            for r, pos_ref in enumerate(pos_refs):
                buf[rows_at(pos_ref[i], n), :] = v if shared else src[r, pl.ds(at + n * k, n), :]
        return c

    lax.fori_loop(0, BT // unroll, body, 0)


def zero_tails(buf, tab_ref, n_exp, pitch):
    def body(e, c):
        at = pl.multiple_of((tab_ref[0, e + 1] - 1) * (pitch * TM), pitch * TM)
        buf[pl.ds(at, pitch * TM), :] = jnp.zeros((pitch * TM, buf.shape[1]), F32)
        return c

    lax.fori_loop(0, n_exp, body, 0)


def pre_bwd_kernel(*refs, n_blocks, top_k, n_exp):
    pos_refs, refs = refs[:top_k], refs[top_k:]
    tab_ref, gate_ref, x_ref, g_ref, w1_ref, w2_ref, h_ref, xs_hbm, qs_hbm, buf, src, xst, qst, sems = refs
    step = pl.program_id(0)

    @pl.when(step == 0)
    def _():
        zero_tails(buf, tab_ref, n_exp, 4)

    h = dense_forward(x_ref[...].astype(F32), w1_ref[...], w2_ref[...])
    h_ref[...] = h
    hf = h.astype(F32)
    n = (hf * rms_scale(hf)).astype(BF16).astype(F32)
    g = g_ref[...].astype(F32)
    gates = gate_ref[...].astype(F32).T
    for r in range(top_k):
        put_rows(src.at[r], 0, n, 4, 0)
        put_rows(src.at[r], 0, g * gates[:, r : r + 1], 4, 2)
    scatter_rows(src, buf, pos_refs, 4, False)

    @pl.when(step == n_blocks - 1)
    def _():
        n_tiles = tab_ref[0, n_exp]

        def copies(t, slot):
            rows = pl.ds(pl.multiple_of(t * TM, TM), TM)
            return (
                pltpu.make_async_copy(xst.at[slot], xs_hbm.at[rows], sems.at[0, slot]),
                pltpu.make_async_copy(qst.at[slot], qs_hbm.at[rows], sems.at[1, slot]),
            )

        def convert(t, c):
            slot = lax.rem(t, QUEUE)

            @pl.when(t >= QUEUE)
            def _():
                for cp in copies(t - QUEUE, slot):
                    cp.wait()

            rows = pl.multiple_of(t * (4 * TM), 4 * TM)
            xst[slot] = get_rows(buf, rows, TM, 4, 0).astype(BF16)
            qst[slot] = get_rows(buf, rows, TM, 4, 2).astype(BF16)
            for cp in copies(t, slot):
                cp.start()
            return c

        lax.fori_loop(0, n_tiles, convert, 0)
        for back in range(QUEUE, 0, -1):
            for cp in copies(n_tiles - back, lax.rem(n_tiles - back, QUEUE)):
                cp.wait()


def route_specs(top_k, n_blocks, first=0, skip=0, total=None):
    def spec(r):
        start = r * (total or n_blocks) + skip
        return pl.BlockSpec((BT,), lambda i: (start + jnp.clip(i - first, 0, n_blocks - 1),), memory_space=pltpu.SMEM)

    return [spec(r) for r in range(top_k)]


def gate_spec(top_k, n_blocks, first=0, skip=0):
    return pl.BlockSpec((top_k, BT), lambda i: (0, skip + jnp.clip(i - first, 0, n_blocks - 1)))


def pre_bwd(pos, tab, gates, x, g, w1, w2, rows, n_exp, top_k):
    n_tok, hid = x.shape
    n_blocks = n_tok // BT
    smem = pl.BlockSpec(memory_space=pltpu.SMEM)
    blk = pl.BlockSpec((BT, hid), lambda i: (i, 0))
    whole = pl.BlockSpec((hid, hid), lambda i: (0, 0))
    return pl.pallas_call(
        functools.partial(pre_bwd_kernel, n_blocks=n_blocks, top_k=top_k, n_exp=n_exp),
        grid=(n_blocks,),
        in_specs=[*route_specs(top_k, n_blocks), smem, gate_spec(top_k, n_blocks), blk, blk, whole, whole],
        out_specs=[blk, pl.BlockSpec(memory_space=pl.ANY), pl.BlockSpec(memory_space=pl.ANY)],
        out_shape=(
            jax.ShapeDtypeStruct((n_tok, hid), BF16),
            jax.ShapeDtypeStruct((rows, hid), BF16),
            jax.ShapeDtypeStruct((rows, hid), BF16),
        ),
        scratch_shapes=[
            pltpu.VMEM((4 * rows + 8, hid // 2), F32),
            pltpu.VMEM((top_k, 4 * BT, hid // 2), F32),
            pltpu.VMEM((QUEUE, TM, hid), BF16),
            pltpu.VMEM((QUEUE, TM, hid), BF16),
            pltpu.SemaphoreType.DMA((2, QUEUE)),
        ],
        compiler_params=pltpu.CompilerParams(vmem_limit_bytes=VMEM_LIMIT),
        cost_estimate=pl.CostEstimate(flops=30_000_000_000, bytes_accessed=30_000_000, transcendentals=0),
        name="pre_bwd",
    )(*[pos] * top_k, tab, gates, x, g, w1, w2)


def exp_bwd_kernel(first_ref, tab_ref, xs_hbm, qs_hbm, *refs, n_parts, has_init):
    w_hbm, refs = refs[:n_parts], refs[n_parts:]
    init_hbm, refs = (refs[:1], refs[1:]) if has_init else ((), refs)
    per = w_hbm[0].shape[0]
    n_loc = n_parts * per
    rs_hbm, dw_hbm, wb, dwb, xb, qb, rb, mid, sems, wsems, dsems, isems = refs
    first = first_ref[0]
    begin = tab_ref[0, first]
    end = tab_ref[0, first + n_loc]

    def rows_of(t):
        return pl.ds(pl.multiple_of(t * TM, TM), TM)

    def loads(t):
        slot = lax.rem(t, DEPTH)
        return (
            pltpu.make_async_copy(xs_hbm.at[rows_of(t)], xb.at[slot], sems.at[0, slot]),
            pltpu.make_async_copy(qs_hbm.at[rows_of(t)], qb.at[slot], sems.at[1, slot]),
        )

    def save(t):
        slot = lax.rem(t, DEPTH)
        return pltpu.make_async_copy(rb.at[slot], rs_hbm.at[rows_of(t)], sems.at[2, slot])

    def w_loads(e, part=0, at=0):
        copies = [pltpu.make_async_copy(w_hbm[part].at[at], wb.at[e], wsems.at[e])]
        return copies + [pltpu.make_async_copy(ref.at[:, e], dwb.at[:, e], isems.at[e]) for ref in init_hbm]

    def dw_save(e):
        return pltpu.make_async_copy(dwb.at[:, e], dw_hbm.at[:, e], dsems.at[e])

    def first_half(t, e):
        slot = lax.rem(t, DEPTH)
        x = xb[slot]
        pre = dot(x, wb[e, 0])
        up = dot(x, wb[e, 1])
        da = dot_nt(qb[slot], wb[e, 2]).astype(BF16).astype(F32)
        sig = jax.nn.sigmoid(pre)
        sil = pre * sig
        return (
            (sil * up).astype(BF16),
            (da * up * (sig * (1.0 + pre * (1.0 - sig)))).astype(BF16),
            (da * sil).astype(BF16),
        )

    def keep(t, vals):
        for i, v in enumerate(vals):
            mid[lax.rem(t, 2), i] = v

    for cp in w_loads(0):
        cp.start()
    for ahead in range(DEPTH - 1):
        for cp in loads(begin + ahead):
            cp.start()
    for e in range(1, n_loc):
        for cp in w_loads(e, e // per, e % per):
            cp.start()
    if not has_init:
        def clear(e, c):
            for i in range(3):
                dwb[i, e] = jnp.zeros(dwb.shape[2:], F32)
            return c

        lax.fori_loop(0, n_loc, clear, 0)
    for cp in w_loads(0):
        cp.wait()
    for cp in loads(begin):
        cp.wait()
    keep(begin, first_half(begin, 0))

    def body(t, e):
        slot = lax.rem(t, DEPTH)
        more = t + 1 < end
        changes = t + 1 >= tab_ref[0, first + e + 1]
        then = jnp.where(changes & more, e + 1, e)

        @pl.when(changes & more)
        def _():
            for cp in w_loads(then):
                cp.wait()

        @pl.when(t + (DEPTH - 1) < end)
        def _():
            for cp in loads(t + (DEPTH - 1)):
                cp.start()

        @pl.when(more)
        def _():
            for cp in loads(t + 1):
                cp.wait()

        @pl.when(t >= begin + DEPTH)
        def _():
            save(t - DEPTH).wait()

        act, dpre, dup = mid[lax.rem(t, 2), 0], mid[lax.rem(t, 2), 1], mid[lax.rem(t, 2), 2]
        x = xb[slot]
        rows = (dot_nt(dpre, wb[e, 0]) + dot_nt(dup, wb[e, 1])).astype(BF16)
        upcoming = first_half(jnp.minimum(t + 1, end - 1), then)
        grads = (dot_tn(x, dpre), dot_tn(x, dup), dot_tn(act, qb[slot]))
        rb[slot] = rows
        for i, grad in enumerate(grads):
            dwb[i, e] += grad
        keep(t + 1, upcoming)
        save(t).start()

        @pl.when(changes)
        def _():
            dw_save(e).start()

        return then

    lax.fori_loop(begin, end, body, 0)
    for back in range(DEPTH, 0, -1):
        save(end - back).wait()
    for e in range(n_loc):
        dw_save(e).wait()


def exp_bwd(first, tab, weights, xs, qs, init=()):
    per, _, hid, ff = weights[0].shape
    n_loc = per * len(weights)
    smem = pl.BlockSpec(memory_space=pltpu.SMEM)
    hbm = pl.BlockSpec(memory_space=pl.ANY)
    return pl.pallas_call(
        functools.partial(exp_bwd_kernel, n_parts=len(weights), has_init=bool(init)),
        in_specs=[smem, smem] + [hbm] * (2 + len(weights) + len(init)),
        out_specs=[hbm, hbm],
        out_shape=(jax.ShapeDtypeStruct(xs.shape, BF16), jax.ShapeDtypeStruct((3, n_loc, hid, ff), F32)),
        input_output_aliases={2: 0},
        scratch_shapes=[
            pltpu.VMEM((n_loc, 3, hid, ff), BF16),
            pltpu.VMEM((3, n_loc, hid, ff), F32),
            pltpu.VMEM((DEPTH, TM, hid), BF16),
            pltpu.VMEM((DEPTH, TM, hid), BF16),
            pltpu.VMEM((DEPTH, TM, hid), BF16),
            pltpu.VMEM((2, 3, TM, ff), BF16),
            pltpu.SemaphoreType.DMA((3, DEPTH)),
            pltpu.SemaphoreType.DMA((n_loc,)),
            pltpu.SemaphoreType.DMA((n_loc,)),
            pltpu.SemaphoreType.DMA((n_loc,)),
        ],
        compiler_params=pltpu.CompilerParams(vmem_limit_bytes=VMEM_LIMIT),
        cost_estimate=pl.CostEstimate(flops=8_000_000_000, bytes_accessed=20_000_000, transcendentals=0),
        name="exp_bwd",
    )(first, tab, xs, qs, *weights, *init)


def post_bwd_kernel(*refs, n_blocks, top_k, n_exp, rows):
    pos_refs, refs = refs[:top_k], refs[top_k:]
    tab_ref, x_ref, g_ref, h_ref, w1_ref, w2_ref, rs_hbm, dx_ref, rbuf, acc, st, sems = refs

    @pl.when(pl.program_id(0) == 0)
    def _():
        n_tiles = tab_ref[0, n_exp]

        def load(t):
            slot = lax.rem(t, (2 * QUEUE))
            return pltpu.make_async_copy(rs_hbm.at[pl.ds(pl.multiple_of(t * TM, TM), TM)], st.at[slot], sems.at[slot])

        for ahead in range((2 * QUEUE) - 1):
            load(ahead).start()
        rbuf[2 * rows : 2 * rows + 8, :] = jnp.zeros((8, rbuf.shape[1]), F32)

        def expand(t, c):
            @pl.when(t + ((2 * QUEUE) - 1) < n_tiles)
            def _():
                load(t + ((2 * QUEUE) - 1)).start()

            load(t).wait()
            put_rows(rbuf, pl.multiple_of(t * (2 * TM), 2 * TM), st[lax.rem(t, (2 * QUEUE))].astype(F32))
            return c

        lax.fori_loop(0, n_tiles, expand, 0)

    gather_rows(rbuf, acc, pos_refs)
    dn = get_rows(acc.at[0], 0, BT)
    for r in range(1, top_k):
        dn = dn + get_rows(acc.at[r], 0, BT)
    xf = x_ref[...].astype(F32)
    u = dot((xf * rms_scale(xf)).astype(BF16), w1_ref[...])
    dh = g_ref[...].astype(F32) + rms_back(h_ref[...].astype(F32), dn)
    sig = jax.nn.sigmoid(u)
    du = (dot_nt(dh.astype(BF16), w2_ref[...]) * (sig * (1.0 + u * (1.0 - sig)))).astype(BF16)
    dx_ref[...] = (dh + rms_back(xf, dot_nt(du, w1_ref[...]))).astype(BF16)


def post_bwd(n_blocks, skip, pos, tab, x, g, h, w1, w2, rs, n_exp, top_k):
    total, hid = x.shape[0] // BT, x.shape[1]
    rows = rs.shape[0]
    smem = pl.BlockSpec(memory_space=pltpu.SMEM)
    blk = pl.BlockSpec((BT, hid), lambda i: (skip + i, 0))
    whole = pl.BlockSpec((hid, hid), lambda i: (0, 0))
    return pl.pallas_call(
        functools.partial(post_bwd_kernel, n_blocks=n_blocks, top_k=top_k, n_exp=n_exp, rows=rows),
        grid=(n_blocks,),
        in_specs=[*route_specs(top_k, n_blocks, 0, skip, total), smem, blk, blk, blk, whole, whole, pl.BlockSpec(memory_space=pl.ANY)],
        out_specs=pl.BlockSpec((BT, hid), lambda i: (i, 0)),
        out_shape=jax.ShapeDtypeStruct((n_blocks * BT, hid), BF16),
        scratch_shapes=[
            pltpu.VMEM((2 * rows + 8, hid // 2), F32),
            pltpu.VMEM((top_k, 2 * BT, hid // 2), F32),
            pltpu.VMEM(((2 * QUEUE), TM, hid), BF16),
            pltpu.SemaphoreType.DMA(((2 * QUEUE),)),
        ],
        compiler_params=pltpu.CompilerParams(vmem_limit_bytes=VMEM_LIMIT),
        cost_estimate=pl.CostEstimate(flops=30_000_000_000, bytes_accessed=30_000_000, transcendentals=0),
        name="post_bwd",
    )(*[pos] * top_k, tab, x, g, h, w1, w2, rs)


def fwd_kernel(*refs, n_blocks, top_k, n_exp, n_groups, rows):
    pos_refs, pos_out_refs, refs = refs[:top_k], refs[top_k : 2 * top_k], refs[2 * top_k :]
    firsts_ref, tab_ref, gate_ref, x_ref, w1_ref, w2_ref, *rest = refs
    w_hbm = rest[:n_groups]
    y_ref, buf, acc, hsc, wsc, mid, sems = rest[n_groups:]
    nsc = acc.at[0]
    step = pl.program_id(0)

    def w_copy(i):
        return pltpu.make_async_copy(w_hbm[i], wsc.at[pl.ds(firsts_ref[i], w_hbm[i].shape[0])], sems.at[i])

    @pl.when(step == 0)
    def _():
        for i in range(n_groups):
            w_copy(i).start()
        zero_tails(buf, tab_ref, n_exp, 2)

    @pl.when(step < n_blocks)
    def _():
        h = dense_forward(x_ref[...].astype(F32), w1_ref[...], w2_ref[...])
        base = step * BT
        hsc[pl.ds(pl.multiple_of(base, BT), BT), :] = h
        hf = h.astype(F32)
        put_rows(nsc, 0, (hf * rms_scale(hf)).astype(BF16).astype(F32))

        scatter_rows(nsc, buf, pos_refs, 2, True)

    @pl.when(step == n_blocks)
    def _():
        buf[2 * rows : 2 * rows + 8, :] = jnp.zeros((8, buf.shape[1]), F32)
        for i in range(n_groups):
            w_copy(i).wait()
        end = tab_ref[0, n_exp]

        def rows_of(t):
            return get_rows(buf, pl.multiple_of(t * (2 * TM), 2 * TM), TM).astype(BF16)

        def first_half(x, e):
            pre = dot(x, wsc[e, 0])
            up = dot(x, wsc[e, 1])
            return (pre * jax.nn.sigmoid(pre) * up).astype(BF16)

        def expert_of(t, e):
            return jnp.where((t >= tab_ref[0, e + 1]) & (t < end), e + 1, e)

        def second(t):
            return jnp.minimum(t, end - 1)

        spare = 2 * rows + 8
        mid[0, 0] = first_half(rows_of(0), 0)
        mid[0, 1] = first_half(rows_of(second(1)), expert_of(1, 0))

        def body(i, experts):
            t = 2 * i
            slot = lax.rem(i, 2)
            e2 = expert_of(t + 2, experts[1])
            e3 = expert_of(t + 3, e2)
            x2, x3 = rows_of(second(t + 2)), rows_of(second(t + 3))
            outs = [dot(mid[slot, k], wsc[experts[k], 2]).astype(BF16).astype(F32) for k in range(2)]
            acts = [first_half(x2, e2), first_half(x3, e3)]
            put_rows(buf, pl.multiple_of(t * (2 * TM), 2 * TM), outs[0])
            put_rows(buf, pl.multiple_of(jnp.where(t + 1 < end, (t + 1) * (2 * TM), spare), 8), outs[1])
            for k in range(2):
                mid[1 - slot, k] = acts[k]
            return e2, e3

        lax.fori_loop(0, lax.div(end + 1, 2), body, (jnp.int32(0), expert_of(1, 0)))

    @pl.when(step > n_blocks)
    def _():
        base = (step - n_blocks - 1) * BT

        gather_rows(buf, acc, pos_out_refs)
        gates = gate_ref[...].astype(F32).T
        h = hsc[pl.ds(pl.multiple_of(base, BT), BT), :]
        mix = get_rows(acc.at[0], 0, BT) * gates[:, 0:1]
        for r in range(1, top_k):
            mix = mix + get_rows(acc.at[r], 0, BT) * gates[:, r : r + 1]
        y_ref[...] = (h.astype(F32) + mix).astype(BF16)


def fwd(n_blocks, skip, firsts, tab, pos, gates, x, w1, w2, weights, rows, n_exp, top_k):
    n_tok, hid = n_blocks * BT, x.shape[1]
    n_groups = len(weights)
    smem = pl.BlockSpec(memory_space=pltpu.SMEM)
    whole = pl.BlockSpec((hid, hid), lambda i: (0, 0))
    return pl.pallas_call(
        functools.partial(fwd_kernel, n_blocks=n_blocks, top_k=top_k, n_exp=n_exp, n_groups=n_groups, rows=rows),
        grid=(2 * n_blocks + 1,),
        in_specs=[*route_specs(top_k, n_blocks), *route_specs(top_k, n_blocks, n_blocks + 1), smem, smem, gate_spec(top_k, n_blocks, n_blocks + 1, skip)]
        + [pl.BlockSpec((BT, hid), lambda i: (skip + jnp.minimum(i, n_blocks - 1), 0)), whole, whole]
        + [pl.BlockSpec(memory_space=pl.ANY)] * n_groups,
        out_specs=pl.BlockSpec((BT, hid), lambda i: (jnp.maximum(i - n_blocks - 1, 0), 0)),
        out_shape=jax.ShapeDtypeStruct((n_tok, hid), BF16),
        scratch_shapes=[
            pltpu.VMEM((2 * rows + 8 + 2 * TM, hid // 2), F32),
            pltpu.VMEM((top_k, 2 * BT, hid // 2), F32),
            pltpu.VMEM((n_tok, hid), BF16),
            pltpu.VMEM((n_exp, 3, hid, hid), BF16),
            pltpu.VMEM((2, 2, TM, hid), BF16),
            pltpu.SemaphoreType.DMA((n_groups,)),
        ],
        compiler_params=pltpu.CompilerParams(vmem_limit_bytes=VMEM_LIMIT),
        cost_estimate=pl.CostEstimate(flops=80_000_000_000, bytes_accessed=30_000_000, transcendentals=0),
        name="fwd",
    )(*[pos] * (2 * top_k), firsts, tab, gates, x, w1, w2, *weights)


def solution(mesh):
    stages = mesh.shape["pp"]
    ep_size = mesh.shape["ep"]
    next_perm = [(i, (i + 1) % stages) for i in range(stages)]
    prev_perm = [(i, (i - 1) % stages) for i in range(stages)]
    mate_perm = [(i, i ^ 1) for i in range(ep_size)]
    chip_perm = [(i, i ^ 2) for i in range(ep_size)]
    tok_spec = P("pp", "ep", None)
    dense_spec = P("pp", None, None)
    expert_spec = P("pp", "ep", None, None)

    def mate(a):
        return lax.ppermute(a, "ep", mate_perm)

    def chip(a):
        return lax.ppermute(a, "ep", chip_perm)

    def slot(x_fwd, ids_fwd, slots_fwd, gates_fwd, x_saved, grad_in, ids_bwd, slots_bwd, gates_bwd, w_one, w_two, w_gate, w_up, w_down):
        x_fwd, ids_fwd, slots_fwd, gates_fwd = x_fwd[0], ids_fwd[0], slots_fwd[0], gates_fwd[0]
        x_saved, grad_in, ids_bwd, slots_bwd, gates_bwd = x_saved[0], grad_in[0], ids_bwd[0], slots_bwd[0], gates_bwd[0]
        w1, w2, w_gate, w_up, w_down = w_one[0], w_two[0], w_gate[0], w_up[0], w_down[0]
        top_k = ids_fwd.shape[1]
        n_loc = w_gate.shape[0]
        n_exp = n_loc * ep_size
        rows = TM * (ids_fwd.size // TM + n_exp)
        rows_f = [TM * (blocks * BT * top_k // TM + n_exp) for blocks in FWD_BLOCKS]
        me = lax.axis_index("ep")

        half = n_loc // 2
        halves = [slice(0, half), slice(half, n_loc)]
        own = [jnp.stack([w[at] for w in (w_gate, w_up, w_down)], axis=1) for at in halves]
        far = [chip(w) for w in own]
        near = [mate(w) for w in own]
        relay = [mate(w) for w in far]
        groups = {
            "own": (me * n_loc, own),
            "near": ((me ^ 1) * n_loc, near),
            "far0": ((me ^ 2) * n_loc, far[:1]),
            "far1": ((me ^ 2) * n_loc + half, far[1:]),
            "relay0": ((me ^ 3) * n_loc, relay[:1]),
            "relay1": ((me ^ 3) * n_loc + half, relay[1:]),
        }

        tab_b, (pos4_b, pos2_b) = route_ranks(ids_bwd, slots_bwd, n_exp, (ids_bwd.shape[0] // BT,), (rows,), (4.0, 2.0))
        tab_b = tab_b[0]
        tab_f, pos2_f = route_ranks(ids_fwd, slots_fwd, n_exp, FWD_BLOCKS, rows_f, (2.0,))
        gates_b = gates_bwd.T
        gates_f = gates_fwd.T

        h_bwd, xs, qs = pre_bwd(pos4_b, tab_b, gates_b, x_saved, grad_in, w1, w2, rows, n_exp, top_k)

        def experts(name, xs, init=()):
            first, weights = groups[name]
            return exp_bwd(first.reshape(1), tab_b, weights, xs, qs, init)

        xs, part = experts("relay0", xs)
        far_sum = mate(part)
        xs, part = experts("near", xs)
        near_sum = mate(part)
        xs, part = experts("far0", xs, (far_sum,))
        there = [chip(part)]
        xs, part = experts("relay1", xs)
        far_sum = mate(part)
        xs, dw_own = experts("own", xs, (near_sum,))
        xs, part = experts("far1", xs, (far_sum,))
        there.append(chip(part))
        firsts = jnp.stack([first + i * half for first, ws in groups.values() for i in range(len(ws))])
        weights = [w for _, ws in groups.values() for w in ws]

        def post_part(h, rs):
            blocks, skip = POST_BLOCKS[h], sum(POST_BLOCKS[:h])
            return post_bwd(blocks, skip, pos2_b, tab_b, x_saved, grad_in, h_bwd, w1, w2, rs, n_exp, top_k)

        def fwd_part(h, x_in):
            blocks, skip = FWD_BLOCKS[h], sum(FWD_BLOCKS[:h])
            return fwd(blocks, skip, firsts, tab_f[h], pos2_f[h], gates_f, x_in, w1, w2, weights, rows_f[h], n_exp, top_k)

        def send(piece, perm):
            return lax.ppermute(piece, "pp", perm)

        dx_parts, parts = [], []
        piece = post_part(0, xs)
        x_fwd, piece = lax.optimization_barrier((x_fwd, piece))
        dx_parts.append(send(piece, prev_perm))
        for h in range(len(FWD_BLOCKS)):
            piece = fwd_part(h, x_fwd)
            x_fwd, xs, piece = lax.optimization_barrier((x_fwd, xs, piece))
            parts.append(send(piece, next_perm))
        dx_parts.append(send(post_part(1, xs), prev_perm))
        y_next = jnp.concatenate(parts, axis=0)[None]
        dws = [(dw_own[i] + jnp.concatenate([sums[i] for sums in there], axis=0))[None] for i in range(3)]
        dx_prev = jnp.concatenate(dx_parts, axis=0)[None]
        return y_next, dx_prev, *dws

    in_specs = (tok_spec,) * 9 + (dense_spec, dense_spec, expert_spec, expert_spec, expert_spec)
    out_specs = (tok_spec, tok_spec, expert_spec, expert_spec, expert_spec)
    return jax.shard_map(slot, mesh=mesh, in_specs=in_specs, out_specs=out_specs, check_vma=False)
```

```python
import functools

import jax
import jax.numpy as jnp
from jax import lax
from jax.experimental import pallas as pl
from jax.experimental.pallas import tpu as pltpu
from jax.sharding import PartitionSpec as P


NORM_EPS = 1e-6
TM = 256
BT = 512
DEPTH = 4
QUEUE = 8
FWD_BLOCKS = (5, 3)
POST_BLOCKS = (4, 4)
F32 = jnp.float32
BF16 = jnp.bfloat16
VMEM_LIMIT = 60 * 1024 * 1024


def dot(a, b):
    return jnp.dot(a, b, preferred_element_type=F32)


def dot_nt(a, b):
    return lax.dot_general(a, b, (((1,), (1,)), ((), ())), preferred_element_type=F32)


def dot_tn(a, b):
    return lax.dot_general(a, b, (((0,), (0,)), ((), ())), preferred_element_type=F32)


def rms_scale(v):
    return lax.rsqrt(jnp.mean(v * v, axis=-1, keepdims=True) + NORM_EPS)


def rms_back(v, dy):
    r = rms_scale(v)
    return r * dy - v * (r * r * r * jnp.mean(dy * v, axis=-1, keepdims=True))


def dense_forward(xf, w1, w2):
    u = dot((xf * rms_scale(xf)).astype(BF16), w1)
    act = (u * jax.nn.sigmoid(u)).astype(BF16)
    return (xf + dot(act, w2)).astype(BF16)


def rank_routes(ids, slots, n_exp, dump):
    ids = jnp.where(slots >= 0, ids, -1)
    n, lanes = ids.shape
    row = lax.broadcasted_iota(jnp.int32, (lanes, lanes), 0)
    col = lax.broadcasted_iota(jnp.int32, (lanes, lanes), 1)
    upper = jnp.where(row < col, 1.0, 0.0).astype(BF16)
    right = jnp.concatenate([upper, jnp.ones((lanes, lanes), BF16)], axis=1)
    row = lax.broadcasted_iota(jnp.int32, (n + 8, n), 0)
    col = lax.broadcasted_iota(jnp.int32, (n + 8, n), 1)
    left = jnp.where((col < row) | (row >= n), 1.0, 0.0).astype(BF16)
    lane = lax.broadcasted_iota(jnp.int32, (n, lanes), 1)
    both = dot(jnp.concatenate([jnp.where(ids == e, 1.0, 0.0).astype(BF16) for e in range(n_exp)], axis=0), right)
    totals = jnp.zeros((n, lanes), F32)
    for e in range(n_exp):
        totals = jnp.where(lane == e, both[e * n : (e + 1) * n, lanes:], totals)
    pre = dot(left, totals.astype(BF16))
    tiles = jnp.maximum(jnp.floor((pre[n:] + (TM - 1.0)) * (1.0 / TM)), 1.0)
    tab = dot(tiles.astype(BF16), upper)
    base = pre[:n] + TM * tab[0:1]
    pos = jnp.full((n, lanes), float(dump), F32)
    for e in range(n_exp):
        pos = jnp.where(ids == e, both[e * n : (e + 1) * n, :lanes] + base[:, e : e + 1], pos)
    return pos, tab.astype(jnp.int32)


def chunks(ref, first, last):
    return jnp.concatenate([ref[r : r + 1, c * 128 : (c + 1) * 128] for r in range(ref.shape[0]) for c in range(first, last)], axis=0)


def rank_kernel(n_exp, blocks_of, dumps, scales, ids, slots, tab, *tables):
    first = 0
    for h, (blocks, dump) in enumerate(zip(blocks_of, dumps)):
        last = first + blocks * (BT // 128)
        pos, tab[h] = rank_routes(chunks(ids, first, last), chunks(slots, first, last), n_exp, dump)
        for k, scale in enumerate(scales):
            tables[h * len(scales) + k][...] = (pos * scale).astype(jnp.int32)
        first = last


def route_ranks(ids, slots, n_exp, blocks_of, dumps, scales):
    tables = [jax.ShapeDtypeStruct((blocks * BT * ids.shape[1] // 128, 128), jnp.int32) for blocks in blocks_of for _ in scales]
    tab, *pos = pl.pallas_call(
        functools.partial(rank_kernel, n_exp, blocks_of, dumps, scales),
        out_shape=(jax.ShapeDtypeStruct((len(blocks_of), 8, 128), jnp.int32), *tables),
        name="rank",
    )(ids.T, slots.T)
    return tab, [p.reshape(-1) for p in pos]


def put_rows(ref, at, vals, pitch=2, off=0):
    n = vals.shape[0]
    half = vals.shape[1] // 2
    ref[pl.ds(at + off, n, stride=pitch), :] = vals[:, :half]
    ref[pl.ds(at + off + 1, n, stride=pitch), :] = vals[:, half:]


def get_rows(ref, at, n, pitch=2, off=0):
    return jnp.concatenate([ref[pl.ds(at + off + i, n, stride=pitch), :] for i in range(2)], axis=1)


def rows_at(p, n):
    return pl.ds(pl.multiple_of(p, n), n)


def gather_rows(buf, acc, pos_refs):
    unroll = 32

    def body(j, c):
        base = j * unroll
        at = pl.multiple_of(j * (2 * unroll), 2 * unroll)
        for k in range(unroll):
            i = base + k
            for r, pos_ref in enumerate(pos_refs):
                acc[r, pl.ds(at + 2 * k, 2), :] = buf[rows_at(pos_ref[i], 2), :]
        return c

    lax.fori_loop(0, BT // unroll, body, 0)


def scatter_rows(src, buf, pos_refs, n, shared):
    unroll = 32

    def body(j, c):
        base = j * unroll
        at = pl.multiple_of(j * (n * unroll), n * unroll)
        for k in range(unroll):
            i = base + k
            v = src[pl.ds(at + n * k, n), :] if shared else None
            for r, pos_ref in enumerate(pos_refs):
                buf[rows_at(pos_ref[i], n), :] = v if shared else src[r, pl.ds(at + n * k, n), :]
        return c

    lax.fori_loop(0, BT // unroll, body, 0)


def zero_tails(buf, tab_ref, n_exp, pitch):
    def body(e, c):
        at = pl.multiple_of((tab_ref[0, e + 1] - 1) * (pitch * TM), pitch * TM)
        buf[pl.ds(at, pitch * TM), :] = jnp.zeros((pitch * TM, buf.shape[1]), F32)
        return c

    lax.fori_loop(0, n_exp, body, 0)


def pre_bwd_kernel(*refs, n_blocks, top_k, n_exp):
    pos_refs, refs = refs[:top_k], refs[top_k:]
    tab_ref, gate_ref, x_ref, g_ref, w1_ref, w2_ref, h_ref, xs_hbm, qs_hbm, buf, src, xst, qst, sems = refs
    step = pl.program_id(0)

    @pl.when(step == 0)
    def _():
        zero_tails(buf, tab_ref, n_exp, 4)

    h = dense_forward(x_ref[...].astype(F32), w1_ref[...], w2_ref[...])
    h_ref[...] = h
    hf = h.astype(F32)
    n = (hf * rms_scale(hf)).astype(BF16).astype(F32)
    g = g_ref[...].astype(F32)
    gates = gate_ref[...].astype(F32).T
    for r in range(top_k):
        put_rows(src.at[r], 0, n, 4, 0)
        put_rows(src.at[r], 0, g * gates[:, r : r + 1], 4, 2)
    scatter_rows(src, buf, pos_refs, 4, False)

    @pl.when(step == n_blocks - 1)
    def _():
        n_tiles = tab_ref[0, n_exp]

        def copies(t, slot):
            rows = pl.ds(pl.multiple_of(t * TM, TM), TM)
            return (
                pltpu.make_async_copy(xst.at[slot], xs_hbm.at[rows], sems.at[0, slot]),
                pltpu.make_async_copy(qst.at[slot], qs_hbm.at[rows], sems.at[1, slot]),
            )

        def convert(t, c):
            slot = lax.rem(t, QUEUE)

            @pl.when(t >= QUEUE)
            def _():
                for cp in copies(t - QUEUE, slot):
                    cp.wait()

            rows = pl.multiple_of(t * (4 * TM), 4 * TM)
            xst[slot] = get_rows(buf, rows, TM, 4, 0).astype(BF16)
            qst[slot] = get_rows(buf, rows, TM, 4, 2).astype(BF16)
            for cp in copies(t, slot):
                cp.start()
            return c

        lax.fori_loop(0, n_tiles, convert, 0)
        for back in range(QUEUE, 0, -1):
            for cp in copies(n_tiles - back, lax.rem(n_tiles - back, QUEUE)):
                cp.wait()


def route_specs(top_k, n_blocks, first=0, skip=0, total=None):
    def spec(r):
        start = r * (total or n_blocks) + skip
        return pl.BlockSpec((BT,), lambda i: (start + jnp.clip(i - first, 0, n_blocks - 1),), memory_space=pltpu.SMEM)

    return [spec(r) for r in range(top_k)]


def gate_spec(top_k, n_blocks, first=0, skip=0):
    return pl.BlockSpec((top_k, BT), lambda i: (0, skip + jnp.clip(i - first, 0, n_blocks - 1)))


def pre_bwd(pos, tab, gates, x, g, w1, w2, rows, n_exp, top_k):
    n_tok, hid = x.shape
    n_blocks = n_tok // BT
    smem = pl.BlockSpec(memory_space=pltpu.SMEM)
    blk = pl.BlockSpec((BT, hid), lambda i: (i, 0))
    whole = pl.BlockSpec((hid, hid), lambda i: (0, 0))
    return pl.pallas_call(
        functools.partial(pre_bwd_kernel, n_blocks=n_blocks, top_k=top_k, n_exp=n_exp),
        grid=(n_blocks,),
        in_specs=[*route_specs(top_k, n_blocks), smem, gate_spec(top_k, n_blocks), blk, blk, whole, whole],
        out_specs=[blk, pl.BlockSpec(memory_space=pl.ANY), pl.BlockSpec(memory_space=pl.ANY)],
        out_shape=(
            jax.ShapeDtypeStruct((n_tok, hid), BF16),
            jax.ShapeDtypeStruct((rows, hid), BF16),
            jax.ShapeDtypeStruct((rows, hid), BF16),
        ),
        scratch_shapes=[
            pltpu.VMEM((4 * rows + 8, hid // 2), F32),
            pltpu.VMEM((top_k, 4 * BT, hid // 2), F32),
            pltpu.VMEM((QUEUE, TM, hid), BF16),
            pltpu.VMEM((QUEUE, TM, hid), BF16),
            pltpu.SemaphoreType.DMA((2, QUEUE)),
        ],
        compiler_params=pltpu.CompilerParams(vmem_limit_bytes=VMEM_LIMIT),
        cost_estimate=pl.CostEstimate(flops=30_000_000_000, bytes_accessed=30_000_000, transcendentals=0),
        name="pre_bwd",
    )(*[pos] * top_k, tab, gates, x, g, w1, w2)


def exp_bwd_kernel(first_ref, tab_ref, xs_hbm, qs_hbm, *refs, n_parts, has_init):
    w_hbm, refs = refs[:n_parts], refs[n_parts:]
    init_hbm, refs = (refs[:1], refs[1:]) if has_init else ((), refs)
    per = w_hbm[0].shape[0]
    n_loc = n_parts * per
    rs_hbm, dw_hbm, wb, dwb, xb, qb, rb, mid, sems, wsems, dsems, isems = refs
    first = first_ref[0]
    begin = tab_ref[0, first]
    end = tab_ref[0, first + n_loc]

    def rows_of(t):
        return pl.ds(pl.multiple_of(t * TM, TM), TM)

    def loads(t):
        slot = lax.rem(t, DEPTH)
        return (
            pltpu.make_async_copy(xs_hbm.at[rows_of(t)], xb.at[slot], sems.at[0, slot]),
            pltpu.make_async_copy(qs_hbm.at[rows_of(t)], qb.at[slot], sems.at[1, slot]),
        )

    def save(t):
        slot = lax.rem(t, DEPTH)
        return pltpu.make_async_copy(rb.at[slot], rs_hbm.at[rows_of(t)], sems.at[2, slot])

    def w_loads(e, part=0, at=0):
        copies = [pltpu.make_async_copy(w_hbm[part].at[at], wb.at[e], wsems.at[e])]
        return copies + [pltpu.make_async_copy(ref.at[:, e], dwb.at[:, e], isems.at[e]) for ref in init_hbm]

    def dw_save(e):
        return pltpu.make_async_copy(dwb.at[:, e], dw_hbm.at[:, e], dsems.at[e])

    def first_half(t, e):
        slot = lax.rem(t, DEPTH)
        x = xb[slot]
        pre = dot(x, wb[e, 0])
        up = dot(x, wb[e, 1])
        da = dot_nt(qb[slot], wb[e, 2]).astype(BF16).astype(F32)
        sig = jax.nn.sigmoid(pre)
        sil = pre * sig
        return (
            (sil * up).astype(BF16),
            (da * up * (sig * (1.0 + pre * (1.0 - sig)))).astype(BF16),
            (da * sil).astype(BF16),
        )

    def keep(t, vals):
        for i, v in enumerate(vals):
            mid[lax.rem(t, 2), i] = v

    for cp in w_loads(0):
        cp.start()
    for ahead in range(DEPTH - 1):
        for cp in loads(begin + ahead):
            cp.start()
    for e in range(1, n_loc):
        for cp in w_loads(e, e // per, e % per):
            cp.start()
    if not has_init:
        def clear(e, c):
            for i in range(3):
                dwb[i, e] = jnp.zeros(dwb.shape[2:], F32)
            return c

        lax.fori_loop(0, n_loc, clear, 0)
    for cp in w_loads(0):
        cp.wait()
    for cp in loads(begin):
        cp.wait()
    keep(begin, first_half(begin, 0))

    def body(t, e):
        slot = lax.rem(t, DEPTH)
        more = t + 1 < end
        changes = t + 1 >= tab_ref[0, first + e + 1]
        then = jnp.where(changes & more, e + 1, e)

        @pl.when(changes & more)
        def _():
            for cp in w_loads(then):
                cp.wait()

        @pl.when(t + (DEPTH - 1) < end)
        def _():
            for cp in loads(t + (DEPTH - 1)):
                cp.start()

        @pl.when(more)
        def _():
            for cp in loads(t + 1):
                cp.wait()

        @pl.when(t >= begin + DEPTH)
        def _():
            save(t - DEPTH).wait()

        act, dpre, dup = mid[lax.rem(t, 2), 0], mid[lax.rem(t, 2), 1], mid[lax.rem(t, 2), 2]
        x = xb[slot]
        rows = (dot_nt(dpre, wb[e, 0]) + dot_nt(dup, wb[e, 1])).astype(BF16)
        upcoming = first_half(jnp.minimum(t + 1, end - 1), then)
        grads = (dot_tn(x, dpre), dot_tn(x, dup), dot_tn(act, qb[slot]))
        rb[slot] = rows
        for i, grad in enumerate(grads):
            dwb[i, e] += grad
        keep(t + 1, upcoming)
        save(t).start()

        @pl.when(changes)
        def _():
            dw_save(e).start()

        return then

    lax.fori_loop(begin, end, body, 0)
    for back in range(DEPTH, 0, -1):
        save(end - back).wait()
    for e in range(n_loc):
        dw_save(e).wait()


def exp_bwd(first, tab, weights, xs, qs, init=()):
    per, _, hid, ff = weights[0].shape
    n_loc = per * len(weights)
    smem = pl.BlockSpec(memory_space=pltpu.SMEM)
    hbm = pl.BlockSpec(memory_space=pl.ANY)
    return pl.pallas_call(
        functools.partial(exp_bwd_kernel, n_parts=len(weights), has_init=bool(init)),
        in_specs=[smem, smem] + [hbm] * (2 + len(weights) + len(init)),
        out_specs=[hbm, hbm],
        out_shape=(jax.ShapeDtypeStruct(xs.shape, BF16), jax.ShapeDtypeStruct((3, n_loc, hid, ff), F32)),
        input_output_aliases={2: 0},
        scratch_shapes=[
            pltpu.VMEM((n_loc, 3, hid, ff), BF16),
            pltpu.VMEM((3, n_loc, hid, ff), F32),
            pltpu.VMEM((DEPTH, TM, hid), BF16),
            pltpu.VMEM((DEPTH, TM, hid), BF16),
            pltpu.VMEM((DEPTH, TM, hid), BF16),
            pltpu.VMEM((2, 3, TM, ff), BF16),
            pltpu.SemaphoreType.DMA((3, DEPTH)),
            pltpu.SemaphoreType.DMA((n_loc,)),
            pltpu.SemaphoreType.DMA((n_loc,)),
            pltpu.SemaphoreType.DMA((n_loc,)),
        ],
        compiler_params=pltpu.CompilerParams(vmem_limit_bytes=VMEM_LIMIT),
        cost_estimate=pl.CostEstimate(flops=8_000_000_000, bytes_accessed=20_000_000, transcendentals=0),
        name="exp_bwd",
    )(first, tab, xs, qs, *weights, *init)


def post_bwd_kernel(*refs, n_blocks, top_k, n_exp, rows):
    pos_refs, refs = refs[:top_k], refs[top_k:]
    tab_ref, x_ref, g_ref, h_ref, w1_ref, w2_ref, rs_hbm, dx_ref, rbuf, acc, st, sems = refs

    @pl.when(pl.program_id(0) == 0)
    def _():
        n_tiles = tab_ref[0, n_exp]

        def load(t):
            slot = lax.rem(t, (2 * QUEUE))
            return pltpu.make_async_copy(rs_hbm.at[pl.ds(pl.multiple_of(t * TM, TM), TM)], st.at[slot], sems.at[slot])

        for ahead in range((2 * QUEUE) - 1):
            load(ahead).start()
        rbuf[2 * rows : 2 * rows + 8, :] = jnp.zeros((8, rbuf.shape[1]), F32)

        def expand(t, c):
            @pl.when(t + ((2 * QUEUE) - 1) < n_tiles)
            def _():
                load(t + ((2 * QUEUE) - 1)).start()

            load(t).wait()
            put_rows(rbuf, pl.multiple_of(t * (2 * TM), 2 * TM), st[lax.rem(t, (2 * QUEUE))].astype(F32))
            return c

        lax.fori_loop(0, n_tiles, expand, 0)

    gather_rows(rbuf, acc, pos_refs)
    dn = get_rows(acc.at[0], 0, BT)
    for r in range(1, top_k):
        dn = dn + get_rows(acc.at[r], 0, BT)
    xf = x_ref[...].astype(F32)
    u = dot((xf * rms_scale(xf)).astype(BF16), w1_ref[...])
    dh = g_ref[...].astype(F32) + rms_back(h_ref[...].astype(F32), dn)
    sig = jax.nn.sigmoid(u)
    du = (dot_nt(dh.astype(BF16), w2_ref[...]) * (sig * (1.0 + u * (1.0 - sig)))).astype(BF16)
    dx_ref[...] = (dh + rms_back(xf, dot_nt(du, w1_ref[...]))).astype(BF16)


def post_bwd(n_blocks, skip, pos, tab, x, g, h, w1, w2, rs, n_exp, top_k):
    total, hid = x.shape[0] // BT, x.shape[1]
    rows = rs.shape[0]
    smem = pl.BlockSpec(memory_space=pltpu.SMEM)
    blk = pl.BlockSpec((BT, hid), lambda i: (skip + i, 0))
    whole = pl.BlockSpec((hid, hid), lambda i: (0, 0))
    return pl.pallas_call(
        functools.partial(post_bwd_kernel, n_blocks=n_blocks, top_k=top_k, n_exp=n_exp, rows=rows),
        grid=(n_blocks,),
        in_specs=[*route_specs(top_k, n_blocks, 0, skip, total), smem, blk, blk, blk, whole, whole, pl.BlockSpec(memory_space=pl.ANY)],
        out_specs=pl.BlockSpec((BT, hid), lambda i: (i, 0)),
        out_shape=jax.ShapeDtypeStruct((n_blocks * BT, hid), BF16),
        scratch_shapes=[
            pltpu.VMEM((2 * rows + 8, hid // 2), F32),
            pltpu.VMEM((top_k, 2 * BT, hid // 2), F32),
            pltpu.VMEM(((2 * QUEUE), TM, hid), BF16),
            pltpu.SemaphoreType.DMA(((2 * QUEUE),)),
        ],
        compiler_params=pltpu.CompilerParams(vmem_limit_bytes=VMEM_LIMIT),
        cost_estimate=pl.CostEstimate(flops=30_000_000_000, bytes_accessed=30_000_000, transcendentals=0),
        name="post_bwd",
    )(*[pos] * top_k, tab, x, g, h, w1, w2, rs)


def fwd_kernel(*refs, n_blocks, top_k, n_exp, n_groups, rows):
    pos_refs, pos_out_refs, refs = refs[:top_k], refs[top_k : 2 * top_k], refs[2 * top_k :]
    firsts_ref, tab_ref, gate_ref, x_ref, w1_ref, w2_ref, *rest = refs
    w_hbm = rest[:n_groups]
    y_ref, buf, acc, hsc, wsc, mid, sems = rest[n_groups:]
    nsc = acc.at[0]
    step = pl.program_id(0)

    def w_copy(i):
        return pltpu.make_async_copy(w_hbm[i], wsc.at[pl.ds(firsts_ref[i], w_hbm[i].shape[0])], sems.at[i])

    @pl.when(step == 0)
    def _():
        for i in range(n_groups):
            w_copy(i).start()
        zero_tails(buf, tab_ref, n_exp, 2)

    @pl.when(step < n_blocks)
    def _():
        h = dense_forward(x_ref[...].astype(F32), w1_ref[...], w2_ref[...])
        base = step * BT
        hsc[pl.ds(pl.multiple_of(base, BT), BT), :] = h
        hf = h.astype(F32)
        put_rows(nsc, 0, (hf * rms_scale(hf)).astype(BF16).astype(F32))

        scatter_rows(nsc, buf, pos_refs, 2, True)

    @pl.when(step == n_blocks)
    def _():
        buf[2 * rows : 2 * rows + 8, :] = jnp.zeros((8, buf.shape[1]), F32)
        for i in range(n_groups):
            w_copy(i).wait()
        end = tab_ref[0, n_exp]

        def rows_of(t):
            return get_rows(buf, pl.multiple_of(t * (2 * TM), 2 * TM), TM).astype(BF16)

        def first_half(x, e):
            pre = dot(x, wsc[e, 0])
            up = dot(x, wsc[e, 1])
            return (pre * jax.nn.sigmoid(pre) * up).astype(BF16)

        def expert_of(t, e):
            return jnp.where((t >= tab_ref[0, e + 1]) & (t < end), e + 1, e)

        def second(t):
            return jnp.minimum(t, end - 1)

        spare = 2 * rows + 8
        mid[0, 0] = first_half(rows_of(0), 0)
        mid[0, 1] = first_half(rows_of(second(1)), expert_of(1, 0))

        def body(i, experts):
            t = 2 * i
            slot = lax.rem(i, 2)
            e2 = expert_of(t + 2, experts[1])
            e3 = expert_of(t + 3, e2)
            x2, x3 = rows_of(second(t + 2)), rows_of(second(t + 3))
            outs = [dot(mid[slot, k], wsc[experts[k], 2]).astype(BF16).astype(F32) for k in range(2)]
            acts = [first_half(x2, e2), first_half(x3, e3)]
            put_rows(buf, pl.multiple_of(t * (2 * TM), 2 * TM), outs[0])
            put_rows(buf, pl.multiple_of(jnp.where(t + 1 < end, (t + 1) * (2 * TM), spare), 8), outs[1])
            for k in range(2):
                mid[1 - slot, k] = acts[k]
            return e2, e3

        lax.fori_loop(0, lax.div(end + 1, 2), body, (jnp.int32(0), expert_of(1, 0)))

    @pl.when(step > n_blocks)
    def _():
        base = (step - n_blocks - 1) * BT

        gather_rows(buf, acc, pos_out_refs)
        gates = gate_ref[...].astype(F32).T
        h = hsc[pl.ds(pl.multiple_of(base, BT), BT), :]
        mix = get_rows(acc.at[0], 0, BT) * gates[:, 0:1]
        for r in range(1, top_k):
            mix = mix + get_rows(acc.at[r], 0, BT) * gates[:, r : r + 1]
        y_ref[...] = (h.astype(F32) + mix).astype(BF16)


def fwd(n_blocks, skip, firsts, tab, pos, gates, x, w1, w2, weights, rows, n_exp, top_k):
    n_tok, hid = n_blocks * BT, x.shape[1]
    n_groups = len(weights)
    smem = pl.BlockSpec(memory_space=pltpu.SMEM)
    whole = pl.BlockSpec((hid, hid), lambda i: (0, 0))
    return pl.pallas_call(
        functools.partial(fwd_kernel, n_blocks=n_blocks, top_k=top_k, n_exp=n_exp, n_groups=n_groups, rows=rows),
        grid=(2 * n_blocks + 1,),
        in_specs=[*route_specs(top_k, n_blocks), *route_specs(top_k, n_blocks, n_blocks + 1), smem, smem, gate_spec(top_k, n_blocks, n_blocks + 1, skip)]
        + [pl.BlockSpec((BT, hid), lambda i: (skip + jnp.minimum(i, n_blocks - 1), 0)), whole, whole]
        + [pl.BlockSpec(memory_space=pl.ANY)] * n_groups,
        out_specs=pl.BlockSpec((BT, hid), lambda i: (jnp.maximum(i - n_blocks - 1, 0), 0)),
        out_shape=jax.ShapeDtypeStruct((n_tok, hid), BF16),
        scratch_shapes=[
            pltpu.VMEM((2 * rows + 8 + 2 * TM, hid // 2), F32),
            pltpu.VMEM((top_k, 2 * BT, hid // 2), F32),
            pltpu.VMEM((n_tok, hid), BF16),
            pltpu.VMEM((n_exp, 3, hid, hid), BF16),
            pltpu.VMEM((2, 2, TM, hid), BF16),
            pltpu.SemaphoreType.DMA((n_groups,)),
        ],
        compiler_params=pltpu.CompilerParams(vmem_limit_bytes=VMEM_LIMIT),
        cost_estimate=pl.CostEstimate(flops=80_000_000_000, bytes_accessed=30_000_000, transcendentals=0),
        name="fwd",
    )(*[pos] * (2 * top_k), firsts, tab, gates, x, w1, w2, *weights)


def solution(mesh):
    stages = mesh.shape["pp"]
    ep_size = mesh.shape["ep"]
    next_perm = [(i, (i + 1) % stages) for i in range(stages)]
    prev_perm = [(i, (i - 1) % stages) for i in range(stages)]
    mate_perm = [(i, i ^ 1) for i in range(ep_size)]
    chip_perm = [(i, i ^ 2) for i in range(ep_size)]
    tok_spec = P("pp", "ep", None)
    dense_spec = P("pp", None, None)
    expert_spec = P("pp", "ep", None, None)

    def mate(a):
        return lax.ppermute(a, "ep", mate_perm)

    def chip(a):
        return lax.ppermute(a, "ep", chip_perm)

    def slot(x_fwd, ids_fwd, slots_fwd, gates_fwd, x_saved, grad_in, ids_bwd, slots_bwd, gates_bwd, w_one, w_two, w_gate, w_up, w_down):
        x_fwd, ids_fwd, slots_fwd, gates_fwd = x_fwd[0], ids_fwd[0], slots_fwd[0], gates_fwd[0]
        x_saved, grad_in, ids_bwd, slots_bwd, gates_bwd = x_saved[0], grad_in[0], ids_bwd[0], slots_bwd[0], gates_bwd[0]
        w1, w2, w_gate, w_up, w_down = w_one[0], w_two[0], w_gate[0], w_up[0], w_down[0]
        top_k = ids_fwd.shape[1]
        n_loc = w_gate.shape[0]
        n_exp = n_loc * ep_size
        rows = TM * (ids_fwd.size // TM + n_exp)
        rows_f = [TM * (blocks * BT * top_k // TM + n_exp) for blocks in FWD_BLOCKS]
        me = lax.axis_index("ep")

        half = n_loc // 2
        halves = [slice(0, half), slice(half, n_loc)]
        own = [jnp.stack([w[at] for w in (w_gate, w_up, w_down)], axis=1) for at in halves]
        far = [chip(w) for w in own]
        near = [mate(w) for w in own]
        relay = [mate(w) for w in far]
        groups = {
            "own": (me * n_loc, own),
            "near": ((me ^ 1) * n_loc, near),
            "far0": ((me ^ 2) * n_loc, far[:1]),
            "far1": ((me ^ 2) * n_loc + half, far[1:]),
            "relay0": ((me ^ 3) * n_loc, relay[:1]),
            "relay1": ((me ^ 3) * n_loc + half, relay[1:]),
        }

        tab_b, (pos4_b, pos2_b) = route_ranks(ids_bwd, slots_bwd, n_exp, (ids_bwd.shape[0] // BT,), (rows,), (4.0, 2.0))
        tab_b = tab_b[0]
        tab_f, pos2_f = route_ranks(ids_fwd, slots_fwd, n_exp, FWD_BLOCKS, rows_f, (2.0,))
        gates_b = gates_bwd.T
        gates_f = gates_fwd.T

        h_bwd, xs, qs = pre_bwd(pos4_b, tab_b, gates_b, x_saved, grad_in, w1, w2, rows, n_exp, top_k)

        def experts(name, xs, init=()):
            first, weights = groups[name]
            return exp_bwd(first.reshape(1), tab_b, weights, xs, qs, init)

        xs, part = experts("relay0", xs)
        far_sum = mate(part)
        xs, part = experts("near", xs)
        near_sum = mate(part)
        xs, part = experts("far0", xs, (far_sum,))
        there = [chip(part)]
        xs, part = experts("relay1", xs)
        far_sum = mate(part)
        xs, dw_own = experts("own", xs, (near_sum,))
        xs, part = experts("far1", xs, (far_sum,))
        there.append(chip(part))

        def chained(calls, perm, blocks_of, x_in):
            pieces, skip = [], 0
            for h, blocks in enumerate(blocks_of):
                piece = calls(h, blocks, skip, x_in)
                skip += blocks
                x_in, piece = lax.optimization_barrier((x_in, piece))
                pieces.append(lax.ppermute(piece, "pp", perm))
            return pieces, x_in

        def post_part(h, blocks, skip, x_in):
            return post_bwd(blocks, skip, pos2_b, tab_b, x_saved, grad_in, h_bwd, w1, w2, x_in, n_exp, top_k)

        dx_parts, xs = chained(post_part, prev_perm, POST_BLOCKS, xs)
        x_fwd, xs = lax.optimization_barrier((x_fwd, xs))

        firsts = jnp.stack([first + i * half for first, ws in groups.values() for i in range(len(ws))])
        weights = [w for _, ws in groups.values() for w in ws]

        def fwd_part(h, blocks, skip, x_in):
            return fwd(blocks, skip, firsts, tab_f[h], pos2_f[h], gates_f, x_in, w1, w2, weights, rows_f[h], n_exp, top_k)

        parts, _ = chained(fwd_part, next_perm, FWD_BLOCKS, x_fwd)
        y_next = jnp.concatenate(parts, axis=0)[None]
        dws = [(dw_own[i] + jnp.concatenate([sums[i] for sums in there], axis=0))[None] for i in range(3)]
        dx_prev = jnp.concatenate(dx_parts, axis=0)[None]
        return y_next, dx_prev, *dws

    in_specs = (tok_spec,) * 9 + (dense_spec, dense_spec, expert_spec, expert_spec, expert_spec)
    out_specs = (tok_spec, tok_spec, expert_spec, expert_spec, expert_spec)
    return jax.shard_map(slot, mesh=mesh, in_specs=in_specs, out_specs=out_specs, check_vma=False)
```
